64 devices in a mesh: dp: 4 (over x, y), dap: 16 (over z, core).
Axes of the slice: x: 2, y: 2, z: 8, core: 2. Of those that a mesh axis runs over, the one named last changes fastest.
The devices are a block of a 4x4x8 slice.
Arguments:
- z: bfloat16 [512, 128, 128], P(('dp', 'dap')), parts along dimension 0
- pair_mask: int32 [512, 128], P(('dp', 'dap')), parts along dimension 0
- dz_out: bfloat16 [512, 128, 128], P(('dp', 'dap')), parts along dimension 0
- ln_scale: float32 [2, 128], replicated
- ln_shift: float32 [2, 128], replicated
- w_proj: bfloat16 [2, 128, 512], replicated
- w_bias: bfloat16 [2, 128, 4], replicated
- b_gate: float32 [2, 128], replicated
- w_out: bfloat16 [2, 128, 128], replicated
- b_out: float32 [2, 128], replicated
Outputs:
- output 1: bfloat16 [512, 128, 128], P(('dp', 'dap')), parts along dimension 0
- output 2: bfloat16 [512, 128, 128], P(('dp', 'dap')), parts along dimension 0
- output 3: float32 [8, 128], P('dp'), parts along dimension 0
- output 4: float32 [8, 128], P('dp'), parts along dimension 0
- output 5: float32 [8, 128, 512], P('dp'), parts along dimension 0
- output 6: float32 [8, 128, 4], P('dp'), parts along dimension 0
- output 7: float32 [8, 128], P('dp'), parts along dimension 0
- output 8: float32 [8, 128, 128], P('dp'), parts along dimension 0
- output 9: float32 [8, 128], P('dp'), parts along dimension 0
There are 4 independent parts. The reference program is written for one: setup_inputs(seed, part) draws one part's arguments, and reference() takes and returns one part's arrays. A program takes and returns all parts, laid end to end along the dimension named above; an argument that names none is the same for every part.
All inputs are finite; a program needn't handle non-finite values.
Results may differ from the reference program's by a relative error of at most 0.02.
Values are sent between devices in bfloat16 or wider.
A program may use at most 768 MiB of HBM per device.

```python
import jax
import jax.numpy as jnp
from jax import lax

N = 128
C = 128
H = 4
D = 32
HD = H * D
EPS = 1e-5
MASK_FILL = 1e9


def snap_bf16(values):
    return values + lax.stop_gradient(values.astype(jnp.bfloat16).astype(jnp.float32) - values)


def setup_inputs(seed: int = 0, part: int = 0) -> dict:
    base_key = jax.random.key(seed)
    shared = jax.random.split(base_key, 7)
    part_keys = jax.random.split(jax.random.fold_in(base_key, part), 3)
    z = jax.random.normal(part_keys[0], (N, N, C), jnp.float32).astype(jnp.bfloat16)
    dz_out = jax.random.normal(part_keys[1], (N, N, C), jnp.float32).astype(jnp.bfloat16)
    length = jax.random.randint(part_keys[2], (), N // 2, N - N // 8 + 1)
    positions = jnp.arange(N)
    is_valid = positions < length
    pair_mask = ((is_valid[:, None] & is_valid[None, :]) | (positions[:, None] == positions[None, :])).astype(jnp.int32)
    ln_scale = 1.0 + 0.3 * jax.random.normal(shared[0], (2, C), jnp.float32)
    ln_shift = 0.3 * jax.random.normal(shared[1], (2, C), jnp.float32)
    w_proj = (jax.random.normal(shared[2], (2, C, 4 * HD), jnp.float32) * C ** -0.5).astype(jnp.bfloat16)
    w_bias = (jax.random.normal(shared[3], (2, C, H), jnp.float32) * (2.0 * C ** -0.5)).astype(jnp.bfloat16)
    b_gate = jax.random.normal(shared[4], (2, HD), jnp.float32)
    w_out = (jax.random.normal(shared[5], (2, HD, C), jnp.float32) * (2.0 * HD ** -0.5)).astype(jnp.bfloat16)
    b_out = 0.2 * jax.random.normal(shared[6], (2, C), jnp.float32)
    return dict(z=z, pair_mask=pair_mask, dz_out=dz_out, ln_scale=ln_scale, ln_shift=ln_shift, w_proj=w_proj, w_bias=w_bias, b_gate=b_gate, w_out=w_out, b_out=b_out)


def node_block(pair_in, mask, weights, block_idx):
    ln_gain, ln_bias, w_proj, w_bias, b_gate, w_out, b_out = [stack_arr[block_idx] for stack_arr in weights]
    centred = pair_in - jnp.mean(pair_in, axis=-1, keepdims=True)
    inv_std = lax.rsqrt(jnp.mean(centred * centred, axis=-1, keepdims=True) + EPS)
    normed = snap_bf16(centred * inv_std * ln_gain + ln_bias)
    projected = snap_bf16(jnp.einsum('ijc,ce->ije', normed, w_proj))
    tri_bias = snap_bf16(jnp.einsum('jkc,ch->hjk', normed, w_bias))
    qkvg = projected.reshape(N, N, 4, H, D)
    gate_val = jax.nn.sigmoid(projected[:, :, 3 * HD:] + b_gate)
    mask_bias = (mask.astype(jnp.float32) - 1.0) * MASK_FILL
    logit_scale = D ** -0.5

    def one_row(row_args):
        q_row, k_row, v_row, mask_row = row_args
        logits = jnp.einsum('jhd,khd->hjk', q_row, k_row) * logit_scale + tri_bias + mask_row
        att_probs = jax.nn.softmax(logits, axis=-1)
        return jnp.einsum('hjk,khd->jhd', snap_bf16(att_probs), v_row)

    attended = lax.map(jax.checkpoint(one_row), (qkvg[:, :, 0], qkvg[:, :, 1], qkvg[:, :, 2], mask_bias))
    gated_out = snap_bf16(attended.reshape(N, N, HD) * gate_val)
    return snap_bf16(pair_in + jnp.einsum('ije,ec->ijc', gated_out, w_out) + b_out)


def reference(z, pair_mask, dz_out, ln_scale, ln_shift, w_proj, w_bias, b_gate, w_out, b_out):
    mask_flip = pair_mask.T

    def forward(pair_grid, gain_all, shift_all, proj_all, bias_all, gate_all, out_all, outb_all):
        weights = (gain_all, shift_all, proj_all, bias_all, gate_all, out_all, outb_all)
        mid_grid = node_block(pair_grid, pair_mask, weights, 0)
        flipped = node_block(jnp.swapaxes(mid_grid, 0, 1), mask_flip, weights, 1)
        return jnp.swapaxes(flipped, 0, 1)

    z_out, pullback = jax.vjp(forward, z.astype(jnp.float32), ln_scale, ln_shift, w_proj.astype(jnp.float32), w_bias.astype(jnp.float32), b_gate, w_out.astype(jnp.float32), b_out)
    grads = pullback(dz_out.astype(jnp.float32))
    return (z_out.astype(jnp.bfloat16), grads[0].astype(jnp.bfloat16), grads[1], grads[2], grads[3], grads[4], grads[5], grads[6], grads[7])
```

```python
import functools

import jax
import jax.numpy as jnp
from jax import lax
from jax.experimental import pallas as pl
from jax.experimental.pallas import tpu as pltpu
from jax.sharding import PartitionSpec as P

EPS = 1e-5
MASK_FILL = 1e9
LOG2E = 1.4426950408889634
F32 = jnp.float32
BF16 = jnp.bfloat16
NN = (((1,), (0,)), ((), ()))
NT = (((1,), (1,)), ((), ()))


def dot(a, b, dims=NN):
    return lax.dot_general(a, b, dims, preferred_element_type=F32)


class Exchange:
    def __init__(self, group, axis, send, recv, send_sem, recv_sem, same=False):
        self.group, self.axis, self.send, self.recv = group, axis, send, recv
        self.send_sem, self.recv_sem, self.same = send_sem, recv_sem, same

    def start(self):
        me = lax.axis_index(self.axis)
        half = self.group // 2
        order = [half]
        for hop in range(half - 1, 0, -2):
            order += [hop, self.group - hop]
        for hop in range(half - 2, 0, -2):
            order += [hop, self.group - hop]
        for hop in order:
            peer = lax.rem(me + hop, self.group)
            pltpu.make_async_remote_copy(
                src_ref=self.send if self.same else self.send.at[peer],
                dst_ref=self.recv.at[me],
                send_sem=self.send_sem,
                recv_sem=self.recv_sem,
                device_id={self.axis: peer},
                device_id_type=pl.DeviceIdType.MESH,
            ).start()
        self.recv[me] = self.send[...] if self.same else self.send[me]

    def _all(self):
        some = self.recv.at[pl.ds(0, self.group - 1)]
        return pltpu.make_async_remote_copy(
            src_ref=some,
            dst_ref=some,
            send_sem=self.send_sem,
            recv_sem=self.recv_sem,
            device_id={self.axis: lax.axis_index(self.axis)},
            device_id_type=pl.DeviceIdType.MESH,
        )

    def wait_recv(self):
        self._all().wait_recv()

    def wait_send(self):
        self._all().wait_send()


def kernel(dims, *refs):
    rows, n, ch, heads, hd, group, axis = dims
    hdim = hd // heads
    scale = hdim ** -0.5
    pairs = rows // 2
    two = 2 * n
    wide = heads * n
    (z_ref, mask_ref, dz_ref, lns_ref, lnb_ref, wp_ref, wb_ref, bg_ref, wo_ref, bo_ref,
     zo_out, zg_out, lns_out, lnb_out, wp_out, wb_out, bg_out, wo_out, bo_out,
     wpt, wot, wbt, wbp, col,
     xt, xh, inv, a_s, qt, kt, vt, kv, g_s, ot, ut, btmp, qbd, dbd, dot_s, dgt, dpt, dnt, pf, bias, db, maskb, stage,
     wacc, small, shard,
     b_send, b_recv, mid_send, mid_recv, dz_send, dz_recv, mk_send, mk_recv, zo_send, zo_recv, dm_send, dm_recv,
     db_send, db_recv, w_send, w_recv, w_part, w_full, sm_send, sm_recv,
     send_sems, recv_sems) = refs
    me = lax.axis_index(axis)

    def exchange(slot, send, recv, same=False):
        return Exchange(group, axis, send, recv, send_sems.at[slot], recv_sems.at[slot], same)

    ex_b = [exchange(s, b_send.at[s], b_recv.at[s], True) for s in range(2)]
    ex_mid = exchange(2, mid_send, mid_recv)
    ex_dz = exchange(3, dz_send, dz_recv)
    ex_mask = exchange(4, mk_send, mk_recv, True)
    ex_zo = exchange(5, zo_send, zo_recv)
    ex_dm = exchange(6, dm_send, dm_recv)
    ex_db = [exchange(7 + s, db_send.at[s], db_recv.at[s]) for s in range(2)]
    ex_w = [exchange(9 + s, w_send.at[s], w_recv.at[s]) for s in range(2)]
    ex_wf = [exchange(11 + s, w_part.at[s], w_full.at[s], True) for s in range(2)]
    ex_small = exchange(13, sm_send, sm_recv, True)

    barrier = pltpu.get_barrier_semaphore()
    for hop in range(1, group):
        pl.semaphore_signal(barrier, inc=1, device_id={axis: lax.rem(me + hop, group)},
                            device_id_type=pl.DeviceIdType.MESH)

    head_pick = (lax.broadcasted_iota(jnp.int32, (16, heads), 0) == lax.broadcasted_iota(jnp.int32, (16, heads), 1)).astype(BF16)
    for s in range(2):
        wpt[s] = wp_ref[s].T
        wot[s] = wo_ref[s].T
        wbt[s] = dot(head_pick, wb_ref[s], NT).astype(BF16)
        wbp[s] = dot(wb_ref[s], head_pick, NT).astype(BF16)
        for place, ref in enumerate((lns_ref, lnb_ref, bg_ref, bo_ref)):
            col[s, place] = jnp.broadcast_to(ref[s:s + 1, :], (n, ch)).T

    def zero_diag(i, carry):
        qbd[i] = jnp.zeros((hd, wide), BF16)
        dbd[i] = jnp.zeros((hd, wide), BF16)
        return carry
    lax.fori_loop(0, rows, zero_diag, 0)

    def column(s, place):
        one = col[s, place]
        return jnp.concatenate([one, one], axis=1)

    def store_diag(ref, t, value):
        for r in range(2):
            for h in range(heads):
                ref[2 * t + r, h * hdim:(h + 1) * hdim, h * n:(h + 1) * n] = value[h * hdim:(h + 1) * hdim, r * n:(r + 1) * n]

    def staged(t):
        return [stage[pl.ds(2 * t + r, n, stride=rows), :] for r in range(2)]

    def unpack(recv):
        stage[...] = recv[...].astype(F32).reshape(group * rows * rows, ch)

    def pack(send, t, value):
        parts = [value[r * n:(r + 1) * n].reshape(group, n // group, ch) for r in range(2)]
        send[:, pl.ds(pl.multiple_of(t * 16, 16), 16), :] = jnp.concatenate(parts, axis=1).astype(BF16)

    def project(s, t, x):
        centred = x - jnp.mean(x, axis=0, keepdims=True)
        inv_std = lax.rsqrt(jnp.mean(centred * centred, axis=0, keepdims=True) + EPS)
        x_hat = centred * inv_std
        a_t = (x_hat * column(s, 0) + column(s, 1)).astype(BF16)
        xt[s, t] = x
        xh[s, t] = x_hat
        inv[s, t] = jnp.broadcast_to(inv_std, (8, two))
        a = a_t.T
        a_s[s, t] = a
        p = dot(wpt[s], a_t).astype(BF16)
        qt[s, t] = p[:hd]
        kt[s, t] = p[hd:2 * hd]
        vt[s, t] = p[2 * hd:3 * hd]
        store_diag(qbd, t, p[:hd])
        g_s[s, t] = jax.nn.sigmoid(p[3 * hd:].astype(F32) + column(s, 2))
        kv[s, t] = dot(a, wp_ref[s, :, hd:3 * hd]).astype(BF16)
        b_t = dot(wbt[s], a_t)
        btmp[pl.ds(pl.multiple_of(t * 32, 32), 32), :] = jnp.concatenate([b_t[:, :n], b_t[:, n:]], axis=0)

    def send_bias(s):
        for h in range(0, heads, 2):
            some = [btmp[pl.ds(h + r, rows, stride=16), :] for r in range(2)]
            b_send[s, h * rows:(h + 2) * rows, :] = jnp.concatenate(some, axis=0).astype(BF16)
        ex_b[s].start()

    def take_bias(s):
        ex_b[s].wait_recv()
        got = b_recv[s].astype(F32).reshape(group, heads, rows, n)
        for h in range(heads):
            bias[:, h * n:(h + 1) * n] = got[:, h].reshape(n, n).T * LOG2E

    def probs(s, t, r):
        i = 2 * t + r
        logits = dot(kv[s, t, r * n:(r + 1) * n, :hd], qbd[i])
        fill = maskb[s, i]
        logits = logits * (scale * LOG2E) + bias[...] + jnp.concatenate([fill] * heads, axis=1)
        e = jnp.exp2(logits - jnp.max(logits, axis=0, keepdims=True))
        return e * (1.0 / jnp.sum(e, axis=0, keepdims=True))

    def attend(s, t, r, p_low):
        v = vt[s, t]
        return jnp.concatenate(
            [dot(v[h * hdim:(h + 1) * hdim, r * n:(r + 1) * n], p_low[:, h * n:(h + 1) * n]) for h in range(heads)], axis=0)

    def block_out(s, t):
        u = ut[s, t]
        y = xt[s, t] + dot(wot[s], u) + column(s, 3)
        return y.T

    def attend_bwd(s, t, r, p, p_low):
        i = 2 * t + r
        d_p = dot(kv[s, t, r * n:(r + 1) * n, hd:], dbd[i])
        d_l = p * (d_p - jnp.sum(d_p * p, axis=0, keepdims=True))
        db[...] += d_l
        d_s = (d_l * scale).astype(BF16)
        at = slice(r * n, (r + 1) * n)
        for h in range(heads):
            hs = slice(h * hdim, (h + 1) * hdim)
            d_sh = d_s[:, h * n:(h + 1) * n]
            d_q = dot(kt[s, t, hs, at], d_sh)
            d_k = dot(qt[s, t, hs, at], d_sh, NT)
            d_v = dot(dot_s[t, hs, at], p_low[:, h * n:(h + 1) * n], NT)
            dpt[t, h * hdim:(h + 1) * hdim, at] = d_q.astype(BF16)
            dpt[t, hd + h * hdim:hd + (h + 1) * hdim, at] = d_k.astype(BF16)
            dpt[t, 2 * hd + h * hdim:2 * hd + (h + 1) * hdim, at] = d_v.astype(BF16)

    def gate_bwd(s, t, b_out_sum):
        d_y = jnp.concatenate(staged(t), axis=0)
        d_low = d_y.astype(BF16)
        d_gated = dot(wo_ref[s], d_low, NT)
        dgt[t] = d_gated
        d_o = (d_gated * g_s[s, t]).astype(BF16)
        dot_s[t] = d_o
        store_diag(dbd, t, d_o)
        return b_out_sum + jnp.sum(d_y, axis=0, keepdims=True)

    def after_attention(s, t, gate_sum):
        g = g_s[s, t]
        d_lin = dgt[t] * ot[s, t] * g * (1.0 - g)
        dpt[t, 3 * hd:, :] = d_lin.astype(BF16)
        dnt[t] = dot(wp_ref[s], dpt[t])
        return gate_sum + d_lin

    def add_weights(s, t):
        wacc[:4 * hd] += dot(dpt[t], a_s[s, t])
        d_low = jnp.concatenate(staged(t), axis=0).astype(BF16)
        wacc[4 * hd:] += dot(ut[s, t], d_low)

    def send_weights(s):
        top = wacc[:4 * hd].reshape(group, 4 * hd // group, ch)
        low = wacc[4 * hd:].reshape(group, hd // group, ch)
        w_send[s] = jnp.concatenate([top, low], axis=1).astype(BF16)
        ex_w[s].start()

    def send_bias_grad(s):
        for h in range(0, heads, 2):
            some = [db[:, (h + r) * n:(h + r + 1) * n].T.reshape(group, rows, n) for r in range(2)]
            db_send[s, :, h * rows:(h + 2) * rows, :] = jnp.concatenate(some, axis=1).astype(BF16)
        ex_db[s].start()

    def take_bias_grad(s):
        ex_db[s].wait_recv()
        return jnp.sum(db_recv[s].astype(F32), axis=0).astype(BF16)

    def norm_bwd(s, t, d_own, sums):
        at16 = lax.broadcasted_iota(jnp.int32, (16, heads * rows), 0)
        at32 = lax.broadcasted_iota(jnp.int32, (16, heads * rows), 1)
        rows_of = [dot((at32 == at16 * rows + (2 * t + r)).astype(BF16), d_own) for r in range(2)]
        d_b = jnp.concatenate(rows_of, axis=1).astype(BF16)
        d_n = dnt[t] + dot(wbp[s], d_b)
        x_hat = xh[s, t]
        d_hat = d_n * column(s, 0)
        along = jnp.mean(d_hat * x_hat, axis=0, keepdims=True)
        d_in = inv[s, t, 0:1, :] * (d_hat - jnp.mean(d_hat, axis=0, keepdims=True) - x_hat * along)
        gain_sum, shift_sum, wb_sum = sums
        d_x = d_in.T + jnp.concatenate(staged(t), axis=0)
        return d_x, (gain_sum + d_n * x_hat, shift_sum + d_n, wb_sum + dot(d_b, a_s[s, t]))

    def lanes_to_row(value):
        return jnp.sum((value[:, :n] + value[:, n:]).T, axis=0, keepdims=True)

    def store_small(s, sums, gate_sum, b_out_sum):
        gain_sum, shift_sum, wb_sum = sums
        small[8 * s:8 * s + 1, :] = lanes_to_row(gain_sum)
        small[8 * s + 1:8 * s + 2, :] = lanes_to_row(shift_sum)
        small[8 * s + 2:8 * s + 3, :] = lanes_to_row(gate_sum)
        small[8 * s + 3:8 * s + 4, :] = b_out_sum
        small[8 * s + 4:8 * s + 8, :] = wb_sum[:heads]

    zero_row = jnp.zeros((1, ch), F32)
    zero_tile = jnp.zeros((ch, two), F32)
    zero_sums = (zero_tile, zero_tile, jnp.zeros((16, ch), F32))

    def project_rows(t, carry):
        project(0, t, jnp.concatenate([z_ref[2 * t + r].astype(F32).T for r in range(2)], axis=1))
        return carry
    lax.fori_loop(0, pairs, project_rows, 0)
    pl.semaphore_wait(barrier, group - 1)
    send_bias(0)

    def pack_dz(t, carry):
        pack(dz_send, t, jnp.concatenate([dz_ref[2 * t + r].astype(F32) for r in range(2)], axis=0))
        return carry
    lax.fori_loop(0, pairs, pack_dz, 0)
    fill_rows = (mask_ref[...].astype(F32) - 1.0) * (MASK_FILL * LOG2E)
    for i in range(rows):
        maskb[0, i] = jnp.broadcast_to(fill_rows[i:i + 1, :], (n, n)).T
    mk_send[...] = jnp.concatenate([mask_ref[...].astype(F32)] * 2, axis=0).astype(BF16)
    take_bias(0)
    ex_dz.start()
    ex_mask.start()

    def forward_rows(t, carry):
        for r in range(2):
            p = probs(0, t, r)
            pf[2 * t + r] = p
            ot[0, t, :, r * n:(r + 1) * n] = attend(0, t, r, p.astype(BF16))
        ut[0, t] = (ot[0, t] * g_s[0, t]).astype(BF16)
        pack(mid_send, t, block_out(0, t))
        return carry
    lax.fori_loop(0, pairs, forward_rows, 0)
    ex_mid.start()

    ex_mid.wait_recv()
    unpack(mid_recv)

    def project_cols(t, carry):
        project(1, t, jnp.concatenate([x.T for x in staged(t)], axis=1))
        return carry
    lax.fori_loop(0, pairs, project_cols, 0)
    send_bias(1)

    ex_dz.wait_recv()
    unpack(dz_recv)
    ex_mask.wait_recv()
    whole = mk_recv[...].astype(F32).reshape(group, 2, rows, n)[:, 0].reshape(n, n).astype(BF16)
    for i in range(rows):
        pick = (lax.broadcasted_iota(jnp.int32, (n, n), 0) == me * rows + i).astype(BF16)
        maskb[1, i] = (dot(whole, pick) - 1.0) * (MASK_FILL * LOG2E)
    b_out_sum = lax.fori_loop(0, pairs, lambda t, acc: gate_bwd(1, t, acc), zero_row)
    db[...] = jnp.zeros((n, wide), F32)
    take_bias(1)

    def both_rows(t, carry):
        for r in range(2):
            p = probs(1, t, r)
            p_low = p.astype(BF16)
            ot[1, t, :, r * n:(r + 1) * n] = attend(1, t, r, p_low)
            attend_bwd(1, t, r, p, p_low)
        return carry
    lax.fori_loop(0, pairs, both_rows, 0)
    send_bias_grad(1)

    wacc[...] = jnp.zeros(wacc.shape, F32)

    def finish_cols(t, gate_sum):
        ut[1, t] = (ot[1, t] * g_s[1, t]).astype(BF16)
        pack(zo_send, t, block_out(1, t))
        gate_sum = after_attention(1, t, gate_sum)
        add_weights(1, t)
        return gate_sum
    gate_sum = lax.fori_loop(0, pairs, finish_cols, zero_tile)
    d_own = take_bias_grad(1)

    def norm_cols(t, sums):
        d_x, sums = norm_bwd(1, t, d_own, sums)
        pack(dm_send, t, d_x)
        return sums
    sums = lax.fori_loop(0, pairs, norm_cols, zero_sums)
    ex_dm.start()
    ex_zo.start()
    send_weights(1)
    store_small(1, sums, gate_sum, b_out_sum)

    db[...] = jnp.zeros((n, wide), F32)
    wacc[...] = jnp.zeros(wacc.shape, F32)
    ex_dm.wait_recv()
    unpack(dm_recv)
    b_out_sum = lax.fori_loop(0, pairs, lambda t, acc: gate_bwd(0, t, acc), zero_row)

    def backward_rows(t, carry):
        for r in range(2):
            p = pf[2 * t + r]
            attend_bwd(0, t, r, p, p.astype(BF16))
        return carry
    lax.fori_loop(0, pairs, backward_rows, 0)
    send_bias_grad(0)

    def finish_rows(t, gate_sum):
        gate_sum = after_attention(0, t, gate_sum)
        add_weights(0, t)
        return gate_sum
    gate_sum = lax.fori_loop(0, pairs, finish_rows, zero_tile)
    send_weights(0)
    d_own = take_bias_grad(0)

    def norm_rows(t, sums):
        d_x, sums = norm_bwd(0, t, d_own, sums)
        for r in range(2):
            zg_out[2 * t + r] = d_x[r * n:(r + 1) * n].astype(BF16)
        return sums
    sums = lax.fori_loop(0, pairs, norm_rows, zero_sums)
    store_small(0, sums, gate_sum, b_out_sum)
    sm_send[...] = small[...]
    ex_small.start()

    def reduce_weights(s):
        ex_w[s].wait_recv()
        shard[...] = jnp.sum(w_recv[s].astype(F32), axis=0)
        w_part[s] = shard[...].astype(BF16)
        ex_wf[s].start()
    reduce_weights(1)
    reduce_weights(0)

    ex_zo.wait_recv()
    unpack(zo_recv)

    def store_out(t, carry):
        for r, value in enumerate(staged(t)):
            zo_out[2 * t + r] = value.astype(BF16)
        return carry
    lax.fori_loop(0, pairs, store_out, 0)

    def store_weights(s):
        ex_wf[s].wait_recv()
        full = w_full[s].astype(F32)
        cut = 4 * hd // group
        wp_out[s] = full[:, :cut].reshape(4 * hd, ch).T
        wo_out[s] = full[:, cut:].reshape(hd, ch)
    store_weights(1)

    ex_small.wait_recv()
    total = jnp.sum(sm_recv[...], axis=0)
    for s in range(2):
        for place, ref in enumerate((lns_out, lnb_out, bg_out, bo_out)):
            ref[s:s + 1, :] = total[8 * s + place:8 * s + place + 1, :]
    small[...] = total
    turned = jnp.concatenate([small[...]] * (n // 16), axis=0).T
    for s in range(2):
        wb_out[s] = turned[:, 8 * s + 4:8 * s + 4 + heads]
    store_weights(0)

    for one in ex_b + [ex_mid, ex_dz, ex_mask, ex_zo, ex_dm] + ex_db + ex_w + ex_wf + [ex_small]:
        one.wait_send()


def solution(mesh):
    axis = 'dap'
    group = mesh.shape[axis]
    row_spec = P(('dp', axis), None, None)
    mask_spec = P(('dp', axis), None)
    grad_spec = P('dp')

    def per_device(z, pair_mask, dz_out, ln_scale, ln_shift, w_proj, w_bias, b_gate, w_out, b_out):
        rows, n, ch = z.shape
        heads = w_bias.shape[-1]
        hd = b_gate.shape[-1]
        pairs, two, wide = rows // 2, 2 * n, heads * n
        piece = (group, rows * rows, ch)
        w_rows = 5 * hd // group

        def vmem(shape, dtype):
            return pltpu.VMEM(shape, dtype)

        like = [z, z, ln_scale, ln_shift, w_proj, w_bias, b_gate, w_out, b_out]
        out_shape = [jax.ShapeDtypeStruct(a.shape, BF16 if k < 2 else F32) for k, a in enumerate(like)]
        scratch = [
            vmem((2, 4 * hd, ch), BF16), vmem((2, ch, hd), BF16), vmem((2, 16, ch), BF16), vmem((2, ch, 16), BF16), vmem((2, 4, ch, n), F32),
            vmem((2, pairs, ch, two), F32), vmem((2, pairs, ch, two), F32), vmem((2, pairs, 8, two), F32), vmem((2, pairs, two, ch), BF16),
            vmem((2, pairs, hd, two), BF16), vmem((2, pairs, hd, two), BF16), vmem((2, pairs, hd, two), BF16), vmem((2, pairs, two, 2 * hd), BF16),
            vmem((2, pairs, hd, two), F32), vmem((2, pairs, hd, two), F32), vmem((2, pairs, hd, two), BF16), vmem((rows * 16, n), F32),
            vmem((rows, hd, wide), BF16), vmem((rows, hd, wide), BF16), vmem((pairs, hd, two), BF16), vmem((pairs, hd, two), F32),
            vmem((pairs, 4 * hd, two), BF16), vmem((pairs, ch, two), F32), vmem((rows, n, wide), F32), vmem((n, wide), F32), vmem((n, wide), F32),
            vmem((2, rows, n, n), F32), vmem((group * rows * rows, ch), F32),
            vmem((5 * hd, ch), F32), vmem((16, ch), F32), vmem((w_rows, ch), F32),
            vmem((2, heads * rows, n), BF16), vmem((2, group, heads * rows, n), BF16), vmem(piece, BF16), vmem(piece, BF16), vmem(piece, BF16), vmem(piece, BF16),
            vmem((2 * rows, n), BF16), vmem((group, 2 * rows, n), BF16), vmem(piece, BF16), vmem(piece, BF16), vmem(piece, BF16), vmem(piece, BF16),
            vmem((2, group, heads * rows, n), BF16), vmem((2, group, heads * rows, n), BF16),
            vmem((2, group, w_rows, ch), BF16), vmem((2, group, w_rows, ch), BF16), vmem((2, w_rows, ch), BF16), vmem((2, group, w_rows, ch), BF16),
            vmem((16, ch), F32), vmem((group, 16, ch), F32),
            pltpu.SemaphoreType.DMA((14,)), pltpu.SemaphoreType.DMA((14,)),
        ]
        return pl.pallas_call(
            functools.partial(kernel, (rows, n, ch, heads, hd, group, axis)),
            out_shape=out_shape,
            in_specs=[pl.BlockSpec(memory_space=pltpu.VMEM)] * 10,
            out_specs=[pl.BlockSpec(memory_space=pltpu.VMEM)] * 9,
            scratch_shapes=scratch,
            compiler_params=pltpu.CompilerParams(collective_id=0, has_side_effects=True, vmem_limit_bytes=60 * 1024 * 1024),
        )(z, pair_mask, dz_out, ln_scale, ln_shift, w_proj, w_bias, b_gate, w_out, b_out)

    return jax.shard_map(per_device, mesh=mesh, in_specs=(row_spec, mask_spec, row_spec) + (P(),) * 7,
                         out_specs=(row_spec, row_spec) + (grad_spec,) * 7, check_vma=False)
```

```python
import functools

import jax
import jax.numpy as jnp
from jax import lax
from jax.experimental import pallas as pl
from jax.experimental.pallas import tpu as pltpu
from jax.sharding import PartitionSpec as P

EPS = 1e-5
MASK_FILL = 1e9
LOG2E = 1.4426950408889634
F32 = jnp.float32
BF16 = jnp.bfloat16
NN = (((1,), (0,)), ((), ()))
NT = (((1,), (1,)), ((), ()))


def dot(a, b, dims=NN):
    return lax.dot_general(a, b, dims, preferred_element_type=F32)


class Exchange:
    def __init__(self, group, axis, send, recv, send_sem, recv_sem, same=False):
        self.group, self.axis, self.send, self.recv = group, axis, send, recv
        self.send_sem, self.recv_sem, self.same = send_sem, recv_sem, same

    def start(self):
        me = lax.axis_index(self.axis)
        half = self.group // 2
        order = [half]
        for hop in range(half - 1, 0, -2):
            order += [hop, self.group - hop]
        for hop in range(half - 2, 0, -2):
            order += [hop, self.group - hop]
        for hop in order:
            peer = lax.rem(me + hop, self.group)
            pltpu.make_async_remote_copy(
                src_ref=self.send if self.same else self.send.at[peer],
                dst_ref=self.recv.at[me],
                send_sem=self.send_sem,
                recv_sem=self.recv_sem,
                device_id={self.axis: peer},
                device_id_type=pl.DeviceIdType.MESH,
            ).start()
        self.recv[me] = self.send[...] if self.same else self.send[me]

    def _all(self):
        some = self.recv.at[pl.ds(0, self.group - 1)]
        return pltpu.make_async_remote_copy(
            src_ref=some,
            dst_ref=some,
            send_sem=self.send_sem,
            recv_sem=self.recv_sem,
            device_id={self.axis: lax.axis_index(self.axis)},
            device_id_type=pl.DeviceIdType.MESH,
        )

    def wait_recv(self):
        self._all().wait_recv()

    def wait_send(self):
        self._all().wait_send()


def kernel(dims, *refs):
    rows, n, ch, heads, hd, group, axis = dims
    hdim = hd // heads
    scale = hdim ** -0.5
    pairs = rows // 2
    two = 2 * n
    wide = heads * n
    operands = refs[:10]
    local = refs[-11:-1]
    (z_ref, mask_ref, dz_ref, lns_ref, lnb_ref, wp_ref, wb_ref, bg_ref, wo_ref, bo_ref) = local
    load_sems, refs = refs[-1], refs[10:-11]
    (zo_recv, zg_out, w_full, sm_recv,
     wpt, wot, wbt, wbp, col,
     xt, xh, inv, a_s, qt, kt, vt, kv, g_s, ot, ut, btmp, qbd, dbd, dot_s, dgt, dpt, dnt, pf, bias, db, maskb, stage,
     wacc, small, shard,
     b_send, b_recv, mid_send, mid_recv, dz_send, dz_recv, mk_send, mk_recv, zo_send, dm_send, dm_recv,
     db_send, db_recv, w_send, w_recv, w_part, sm_send,
     send_sems, recv_sems) = refs
    me = lax.axis_index(axis)
    loads = [pltpu.make_async_copy(src, dst, load_sems.at[k]) for k, (src, dst) in enumerate(zip(operands, local))]
    for one in loads:
        one.start()

    def exchange(slot, send, recv, same=False):
        return Exchange(group, axis, send, recv, send_sems.at[slot], recv_sems.at[slot], same)

    ex_b = [exchange(s, b_send.at[s], b_recv.at[s], True) for s in range(2)]
    ex_mid = exchange(2, mid_send, mid_recv)
    ex_dz = exchange(3, dz_send, dz_recv)
    ex_mask = exchange(4, mk_send, mk_recv, True)
    ex_zo = exchange(5, zo_send, zo_recv)
    ex_dm = exchange(6, dm_send, dm_recv)
    ex_db = [exchange(7 + s, db_send.at[s], db_recv.at[s]) for s in range(2)]
    ex_w = [exchange(9 + s, w_send.at[s], w_recv.at[s]) for s in range(2)]
    ex_wf = [exchange(11 + s, w_part.at[s], w_full.at[s], True) for s in range(2)]
    ex_small = exchange(13, sm_send, sm_recv, True)

    barrier = pltpu.get_barrier_semaphore()
    for hop in range(1, group):
        pl.semaphore_signal(barrier, inc=1, device_id={axis: lax.rem(me + hop, group)},
                            device_id_type=pl.DeviceIdType.MESH)

    for k in (3, 4, 5, 6, 7, 8, 9):
        loads[k].wait()
    head_pick = (lax.broadcasted_iota(jnp.int32, (16, heads), 0) == lax.broadcasted_iota(jnp.int32, (16, heads), 1)).astype(BF16)
    eye = (lax.broadcasted_iota(jnp.int32, (ch, ch), 0) == lax.broadcasted_iota(jnp.int32, (ch, ch), 1)).astype(BF16)
    for s in range(2):
        wpt[s] = wp_ref[s].T
        wot[s] = wo_ref[s].T
        w_heads = dot(head_pick, wb_ref[s]).astype(BF16)
        wbt[s] = w_heads
        wbp[s] = dot(eye, w_heads, NT).astype(BF16)
        for place, ref in enumerate((lns_ref, lnb_ref, bg_ref, bo_ref)):
            col[s, place] = jnp.broadcast_to(ref[s:s + 1, :], (n, ch)).T

    def zero_diag(i, carry):
        qbd[i] = jnp.zeros((hd, wide), BF16)
        dbd[i] = jnp.zeros((hd, wide), BF16)
        return carry
    lax.fori_loop(0, rows, zero_diag, 0)

    def column(s, place):
        one = col[s, place]
        return jnp.concatenate([one, one], axis=1)

    def store_diag(ref, t, value):
        for r in range(2):
            for h in range(heads):
                ref[2 * t + r, h * hdim:(h + 1) * hdim, h * n:(h + 1) * n] = value[h * hdim:(h + 1) * hdim, r * n:(r + 1) * n]

    def staged(t):
        return [stage[pl.ds(2 * t + r, n, stride=rows), :] for r in range(2)]

    def unpack(recv):
        stage[...] = recv[...].astype(F32).reshape(group * rows * rows, ch)

    def pack(send, t, value):
        parts = [value[r * n:(r + 1) * n].reshape(group, n // group, ch) for r in range(2)]
        send[:, pl.ds(pl.multiple_of(t * 16, 16), 16), :] = jnp.concatenate(parts, axis=1).astype(BF16)

    def project(s, t, x):
        centred = x - jnp.mean(x, axis=0, keepdims=True)
        inv_std = lax.rsqrt(jnp.mean(centred * centred, axis=0, keepdims=True) + EPS)
        x_hat = centred * inv_std
        a_t = (x_hat * column(s, 0) + column(s, 1)).astype(BF16)
        xt[s, t] = x
        xh[s, t] = x_hat
        inv[s, t] = jnp.broadcast_to(inv_std, (8, two))
        a = a_t.T
        a_s[s, t] = a
        p = dot(wpt[s], a_t).astype(BF16)
        qt[s, t] = p[:hd]
        kt[s, t] = p[hd:2 * hd]
        vt[s, t] = p[2 * hd:3 * hd]
        store_diag(qbd, t, p[:hd])
        g_s[s, t] = jax.nn.sigmoid(p[3 * hd:].astype(F32) + column(s, 2))
        kv[s, t] = dot(a, wp_ref[s, :, hd:3 * hd]).astype(BF16)
        b_t = dot(wbt[s], a_t)
        btmp[pl.ds(pl.multiple_of(t * 32, 32), 32), :] = jnp.concatenate([b_t[:, :n], b_t[:, n:]], axis=0)

    def send_bias(s):
        for h in range(0, heads, 2):
            some = [btmp[pl.ds(h + r, rows, stride=16), :] for r in range(2)]
            b_send[s, h * rows:(h + 2) * rows, :] = jnp.concatenate(some, axis=0).astype(BF16)
        ex_b[s].start()

    def take_bias(s):
        ex_b[s].wait_recv()
        got = b_recv[s].astype(F32).reshape(group, heads, rows, n)
        for h in range(heads):
            bias[:, h * n:(h + 1) * n] = got[:, h].reshape(n, n).T * LOG2E

    def probs(s, t, r):
        i = 2 * t + r
        logits = dot(kv[s, t, r * n:(r + 1) * n, :hd], qbd[i])
        fill = maskb[s, i]
        logits = logits * (scale * LOG2E) + bias[...] + jnp.concatenate([fill] * heads, axis=1)
        e = jnp.exp2(logits - jnp.max(logits, axis=0, keepdims=True))
        return e * (1.0 / jnp.sum(e, axis=0, keepdims=True))

    def attend(s, t, r, p_low):
        v = vt[s, t]
        return jnp.concatenate(
            [dot(v[h * hdim:(h + 1) * hdim, r * n:(r + 1) * n], p_low[:, h * n:(h + 1) * n]) for h in range(heads)], axis=0)

    def block_out(s, t):
        u = ut[s, t]
        y = xt[s, t] + dot(wot[s], u) + column(s, 3)
        return y.T

    def attend_bwd(s, t, r, p, p_low):
        i = 2 * t + r
        d_p = dot(kv[s, t, r * n:(r + 1) * n, hd:], dbd[i])
        d_l = p * (d_p - jnp.sum(d_p * p, axis=0, keepdims=True))
        db[...] += d_l
        d_s = (d_l * scale).astype(BF16)
        at = slice(r * n, (r + 1) * n)
        for h in range(heads):
            hs = slice(h * hdim, (h + 1) * hdim)
            d_sh = d_s[:, h * n:(h + 1) * n]
            d_q = dot(kt[s, t, hs, at], d_sh)
            d_k = dot(qt[s, t, hs, at], d_sh, NT)
            d_v = dot(dot_s[t, hs, at], p_low[:, h * n:(h + 1) * n], NT)
            dpt[t, h * hdim:(h + 1) * hdim, at] = d_q.astype(BF16)
            dpt[t, hd + h * hdim:hd + (h + 1) * hdim, at] = d_k.astype(BF16)
            dpt[t, 2 * hd + h * hdim:2 * hd + (h + 1) * hdim, at] = d_v.astype(BF16)

    def gate_bwd(s, t, b_out_sum):
        d_y = jnp.concatenate(staged(t), axis=0)
        d_low = d_y.astype(BF16)
        d_gated = dot(wo_ref[s], d_low, NT)
        dgt[t] = d_gated
        d_o = (d_gated * g_s[s, t]).astype(BF16)
        dot_s[t] = d_o
        store_diag(dbd, t, d_o)
        return b_out_sum + jnp.sum(d_y, axis=0, keepdims=True)

    def after_attention(s, t, gate_sum):
        g = g_s[s, t]
        d_lin = dgt[t] * ot[s, t] * g * (1.0 - g)
        dpt[t, 3 * hd:, :] = d_lin.astype(BF16)
        dnt[t] = dot(wp_ref[s], dpt[t])
        return gate_sum + d_lin

    def add_weights(s, t):
        wacc[:4 * hd] += dot(dpt[t], a_s[s, t])
        d_low = jnp.concatenate(staged(t), axis=0).astype(BF16)
        wacc[4 * hd:] += dot(ut[s, t], d_low)

    def send_weights(s):
        top = wacc[:4 * hd].reshape(group, 4 * hd // group, ch)
        low = wacc[4 * hd:].reshape(group, hd // group, ch)
        w_send[s] = jnp.concatenate([top, low], axis=1).astype(BF16)
        ex_w[s].start()

    def send_bias_grad(s):
        for h in range(0, heads, 2):
            some = [db[:, (h + r) * n:(h + r + 1) * n].T.reshape(group, rows, n) for r in range(2)]
            db_send[s, :, h * rows:(h + 2) * rows, :] = jnp.concatenate(some, axis=1).astype(BF16)
        ex_db[s].start()

    def take_bias_grad(s):
        ex_db[s].wait_recv()
        return jnp.sum(db_recv[s].astype(F32), axis=0).astype(BF16)

    def norm_bwd(s, t, d_own, sums):
        at16 = lax.broadcasted_iota(jnp.int32, (16, heads * rows), 0)
        at32 = lax.broadcasted_iota(jnp.int32, (16, heads * rows), 1)
        rows_of = [dot((at32 == at16 * rows + (2 * t + r)).astype(BF16), d_own) for r in range(2)]
        d_b = jnp.concatenate(rows_of, axis=1).astype(BF16)
        d_n = dnt[t] + dot(wbp[s], d_b)
        x_hat = xh[s, t]
        d_hat = d_n * column(s, 0)
        along = jnp.mean(d_hat * x_hat, axis=0, keepdims=True)
        d_in = inv[s, t, 0:1, :] * (d_hat - jnp.mean(d_hat, axis=0, keepdims=True) - x_hat * along)
        gain_sum, shift_sum, wb_sum = sums
        d_x = d_in.T + jnp.concatenate(staged(t), axis=0)
        return d_x, (gain_sum + d_n * x_hat, shift_sum + d_n, wb_sum + dot(d_b, a_s[s, t]))

    def lanes_to_row(value):
        return jnp.sum((value[:, :n] + value[:, n:]).T, axis=0, keepdims=True)

    def store_small(s, sums, gate_sum, b_out_sum):
        gain_sum, shift_sum, wb_sum = sums
        small[8 * s:8 * s + 1, :] = lanes_to_row(gain_sum)
        small[8 * s + 1:8 * s + 2, :] = lanes_to_row(shift_sum)
        small[8 * s + 2:8 * s + 3, :] = lanes_to_row(gate_sum)
        small[8 * s + 3:8 * s + 4, :] = b_out_sum
        small[8 * s + 4:8 * s + 8, :] = wb_sum[:heads]

    zero_row = jnp.zeros((1, ch), F32)
    zero_tile = jnp.zeros((ch, two), F32)
    zero_sums = (zero_tile, zero_tile, jnp.zeros((16, ch), F32))

    loads[0].wait()

    def project_rows(t, carry):
        project(0, t, jnp.concatenate([z_ref[2 * t + r].astype(F32).T for r in range(2)], axis=1))
        return carry
    lax.fori_loop(0, pairs, project_rows, 0)
    pl.semaphore_wait(barrier, group - 1)
    send_bias(0)

    loads[1].wait()
    loads[2].wait()

    def pack_dz(t, carry):
        pack(dz_send, t, jnp.concatenate([dz_ref[2 * t + r].astype(F32) for r in range(2)], axis=0))
        return carry
    lax.fori_loop(0, pairs, pack_dz, 0)
    fill_rows = (mask_ref[...].astype(F32) - 1.0) * (MASK_FILL * LOG2E)
    for i in range(rows):
        maskb[0, i] = jnp.broadcast_to(fill_rows[i:i + 1, :], (n, n)).T
    mk_send[...] = jnp.concatenate([mask_ref[...].astype(F32)] * 2, axis=0).astype(BF16)
    take_bias(0)
    ex_dz.start()
    ex_mask.start()

    def forward_rows(t, carry):
        for r in range(2):
            p = probs(0, t, r)
            pf[2 * t + r] = p
            ot[0, t, :, r * n:(r + 1) * n] = attend(0, t, r, p.astype(BF16))
        ut[0, t] = (ot[0, t] * g_s[0, t]).astype(BF16)
        pack(mid_send, t, block_out(0, t))
        return carry
    lax.fori_loop(0, pairs, forward_rows, 0)
    ex_mid.start()

    ex_mid.wait_recv()
    unpack(mid_recv)

    def project_cols(t, carry):
        project(1, t, jnp.concatenate([x.T for x in staged(t)], axis=1))
        return carry
    lax.fori_loop(0, pairs, project_cols, 0)
    send_bias(1)

    ex_dz.wait_recv()
    unpack(dz_recv)
    ex_mask.wait_recv()
    whole = mk_recv[...].astype(F32).reshape(group, 2, rows, n)[:, 0].reshape(n, n).astype(BF16)
    for i in range(rows):
        pick = (lax.broadcasted_iota(jnp.int32, (n, n), 0) == me * rows + i).astype(BF16)
        maskb[1, i] = (dot(whole, pick) - 1.0) * (MASK_FILL * LOG2E)
    b_out_sum = lax.fori_loop(0, pairs, lambda t, acc: gate_bwd(1, t, acc), zero_row)
    db[...] = jnp.zeros((n, wide), F32)
    take_bias(1)

    def both_rows(t, carry):
        for r in range(2):
            p = probs(1, t, r)
            p_low = p.astype(BF16)
            ot[1, t, :, r * n:(r + 1) * n] = attend(1, t, r, p_low)
            attend_bwd(1, t, r, p, p_low)
        return carry
    lax.fori_loop(0, pairs, both_rows, 0)
    send_bias_grad(1)

    wacc[...] = jnp.zeros(wacc.shape, F32)

    def finish_cols(t, gate_sum):
        ut[1, t] = (ot[1, t] * g_s[1, t]).astype(BF16)
        pack(zo_send, t, block_out(1, t))
        gate_sum = after_attention(1, t, gate_sum)
        add_weights(1, t)
        return gate_sum
    gate_sum = lax.fori_loop(0, pairs, finish_cols, zero_tile)
    d_own = take_bias_grad(1)

    def norm_cols(t, sums):
        d_x, sums = norm_bwd(1, t, d_own, sums)
        pack(dm_send, t, d_x)
        return sums
    sums = lax.fori_loop(0, pairs, norm_cols, zero_sums)
    ex_dm.start()
    ex_zo.start()
    send_weights(1)
    store_small(1, sums, gate_sum, b_out_sum)

    db[...] = jnp.zeros((n, wide), F32)
    wacc[...] = jnp.zeros(wacc.shape, F32)
    ex_dm.wait_recv()
    unpack(dm_recv)
    b_out_sum = lax.fori_loop(0, pairs, lambda t, acc: gate_bwd(0, t, acc), zero_row)

    def backward_rows(t, carry):
        for r in range(2):
            p = pf[2 * t + r]
            attend_bwd(0, t, r, p, p.astype(BF16))
        return carry
    lax.fori_loop(0, pairs, backward_rows, 0)
    send_bias_grad(0)

    def finish_rows(t, gate_sum):
        gate_sum = after_attention(0, t, gate_sum)
        add_weights(0, t)
        return gate_sum
    gate_sum = lax.fori_loop(0, pairs, finish_rows, zero_tile)
    send_weights(0)
    d_own = take_bias_grad(0)

    def norm_rows(t, sums):
        d_x, sums = norm_bwd(0, t, d_own, sums)
        for r in range(2):
            zg_out[2 * t + r] = d_x[r * n:(r + 1) * n].astype(BF16)
        return sums
    sums = lax.fori_loop(0, pairs, norm_rows, zero_sums)
    store_small(0, sums, gate_sum, b_out_sum)
    sm_send[...] = small[...]
    ex_small.start()

    def reduce_weights(s):
        ex_w[s].wait_recv()
        shard[...] = jnp.sum(w_recv[s].astype(F32), axis=0)
        w_part[s] = shard[...].astype(BF16)
        ex_wf[s].start()
    reduce_weights(1)
    reduce_weights(0)

    for one in [ex_zo, ex_small] + ex_wf:
        one.wait_recv()
    for one in ex_b + [ex_mid, ex_dz, ex_mask, ex_zo, ex_dm] + ex_db + ex_w + ex_wf + [ex_small]:
        one.wait_send()


def finish(dims, zo_ref, zg_ref, w_ref, sm_ref,
           zo_out, zg_out, lns_out, lnb_out, wp_out, wb_out, bg_out, wo_out, bo_out, stage):
    rows, n, ch, heads, hd, group = dims
    zg_out[...] = zg_ref[...]
    stage[...] = zo_ref[...].astype(F32).reshape(group * rows * rows, ch)
    for i in range(rows):
        zo_out[i] = stage[pl.ds(i, n, stride=rows), :].astype(BF16)
    cut = 4 * hd // group
    for s in range(2):
        full = w_ref[s].astype(F32)
        wp_out[s] = full[:, :cut].reshape(4 * hd, ch).T
        wo_out[s] = full[:, cut:].reshape(hd, ch)
    total = jnp.sum(sm_ref[...], axis=0)
    for s in range(2):
        for place, ref in enumerate((lns_out, lnb_out, bg_out, bo_out)):
            ref[s:s + 1, :] = total[8 * s + place:8 * s + place + 1, :]
        wb_out[s] = total[8 * s + 4:8 * s + 4 + heads]


def solution(mesh):
    axis = 'dap'
    group = mesh.shape[axis]
    row_spec = P(('dp', axis), None, None)
    mask_spec = P(('dp', axis), None)
    grad_spec = P('dp')

    def per_device(z, pair_mask, dz_out, ln_scale, ln_shift, w_proj, w_bias, b_gate, w_out, b_out):
        rows, n, ch = z.shape
        heads = w_bias.shape[-1]
        hd = b_gate.shape[-1]
        pairs, two, wide = rows // 2, 2 * n, heads * n
        piece = (group, rows * rows, ch)
        w_rows = 5 * hd // group

        def vmem(shape, dtype):
            return pltpu.VMEM(shape, dtype)

        w_heads = jnp.swapaxes(w_bias, 1, 2)
        like = [z, z, ln_scale, ln_shift, w_proj, w_heads, b_gate, w_out, b_out]
        out_shape = [jax.ShapeDtypeStruct(a.shape, BF16 if k < 2 else F32) for k, a in enumerate(like)]
        mid_shape = [jax.ShapeDtypeStruct(piece, BF16), jax.ShapeDtypeStruct(z.shape, BF16),
                     jax.ShapeDtypeStruct((2, group, w_rows, ch), BF16), jax.ShapeDtypeStruct((group, 16, ch), F32)]
        scratch = [
            vmem((2, 4 * hd, ch), BF16), vmem((2, ch, hd), BF16), vmem((2, 16, ch), BF16), vmem((2, ch, 16), BF16), vmem((2, 4, ch, n), F32),
            vmem((2, pairs, ch, two), F32), vmem((2, pairs, ch, two), F32), vmem((2, pairs, 8, two), F32), vmem((2, pairs, two, ch), BF16),
            vmem((2, pairs, hd, two), BF16), vmem((2, pairs, hd, two), BF16), vmem((2, pairs, hd, two), BF16), vmem((2, pairs, two, 2 * hd), BF16),
            vmem((2, pairs, hd, two), F32), vmem((2, pairs, hd, two), F32), vmem((2, pairs, hd, two), BF16), vmem((rows * 16, n), F32),
            vmem((rows, hd, wide), BF16), vmem((rows, hd, wide), BF16), vmem((pairs, hd, two), BF16), vmem((pairs, hd, two), F32),
            vmem((pairs, 4 * hd, two), BF16), vmem((pairs, ch, two), F32), vmem((rows, n, wide), F32), vmem((n, wide), F32), vmem((n, wide), F32),
            vmem((2, rows, n, n), F32), vmem((group * rows * rows, ch), F32),
            vmem((5 * hd, ch), F32), vmem((16, ch), F32), vmem((w_rows, ch), F32),
            vmem((2, heads * rows, n), BF16), vmem((2, group, heads * rows, n), BF16), vmem(piece, BF16), vmem(piece, BF16), vmem(piece, BF16), vmem(piece, BF16),
            vmem((2 * rows, n), BF16), vmem((group, 2 * rows, n), BF16), vmem(piece, BF16), vmem(piece, BF16), vmem(piece, BF16),
            vmem((2, group, heads * rows, n), BF16), vmem((2, group, heads * rows, n), BF16),
            vmem((2, group, w_rows, ch), BF16), vmem((2, group, w_rows, ch), BF16), vmem((2, w_rows, ch), BF16), vmem((16, ch), F32),
            pltpu.SemaphoreType.DMA((14,)), pltpu.SemaphoreType.DMA((14,)),
        ]
        operands = (z, pair_mask, dz_out, ln_scale, ln_shift, w_proj, w_heads, b_gate, w_out, b_out)
        scratch += [vmem(a.shape, a.dtype) for a in operands] + [pltpu.SemaphoreType.DMA((10,))]
        in_vmem = pl.BlockSpec(memory_space=pltpu.VMEM)
        mid = pl.pallas_call(
            functools.partial(kernel, (rows, n, ch, heads, hd, group, axis)),
            out_shape=mid_shape,
            in_specs=[pl.BlockSpec(memory_space=pltpu.HBM)] * 10,
            out_specs=[in_vmem] * 4,
            scratch_shapes=scratch,
            compiler_params=pltpu.CompilerParams(collective_id=0, has_side_effects=True, vmem_limit_bytes=40 * 1024 * 1024),
        )(*[pltpu.with_memory_space_constraint(a, pltpu.HBM) for a in operands])
        out = pl.pallas_call(
            functools.partial(finish, (rows, n, ch, heads, hd, group)),
            out_shape=out_shape,
            in_specs=[in_vmem] * 4,
            out_specs=[in_vmem] * 9,
            scratch_shapes=[vmem((group * rows * rows, ch), F32)],
            compiler_params=pltpu.CompilerParams(vmem_limit_bytes=16 * 1024 * 1024),
        )(*mid)
        return tuple(out[:5]) + (jnp.swapaxes(out[5], 1, 2),) + tuple(out[6:])

    return jax.shard_map(per_device, mesh=mesh, in_specs=(row_spec, mask_spec, row_spec) + (P(),) * 7,
                         out_specs=(row_spec, row_spec) + (grad_spec,) * 7, check_vma=False)
```

```python
import functools

import jax
import jax.numpy as jnp
from jax import lax
from jax.experimental import pallas as pl
from jax.experimental.pallas import tpu as pltpu
from jax.sharding import PartitionSpec as P

EPS = 1e-5
MASK_FILL = 1e9
LOG2E = 1.4426950408889634
F32 = jnp.float32
BF16 = jnp.bfloat16
NN = (((1,), (0,)), ((), ()))
NT = (((1,), (1,)), ((), ()))


def dot(a, b, dims=NN):
    return lax.dot_general(a, b, dims, preferred_element_type=F32)


class Exchange:
    def __init__(self, group, axis, send, recv, send_sem, recv_sem, same=False):
        self.group, self.axis, self.send, self.recv = group, axis, send, recv
        self.send_sem, self.recv_sem, self.same = send_sem, recv_sem, same

    def start(self, part=None):
        me = lax.axis_index(self.axis)
        half = self.group // 2
        order = [half]
        for hop in range(half - 1, 0, -1):
            order += [hop, self.group - hop]
        for hop in order:
            peer = lax.rem(me + hop, self.group)
            source = self.send if self.same else self.send.at[peer] if part is None else self.send.at[peer, part]
            pltpu.make_async_remote_copy(
                src_ref=source,
                dst_ref=self.recv.at[me] if part is None else self.recv.at[me, part],
                send_sem=self.send_sem,
                recv_sem=self.recv_sem,
                device_id={self.axis: peer},
                device_id_type=pl.DeviceIdType.MESH,
            ).start()
        if part is None:
            self.recv[me] = self.send[...] if self.same else self.send[me]
        else:
            self.recv[me, part] = self.send[me, part]

    def _all(self):
        some = self.recv.at[pl.ds(0, self.group - 1)]
        return pltpu.make_async_remote_copy(
            src_ref=some,
            dst_ref=some,
            send_sem=self.send_sem,
            recv_sem=self.recv_sem,
            device_id={self.axis: lax.axis_index(self.axis)},
            device_id_type=pl.DeviceIdType.MESH,
        )

    def wait_recv(self):
        self._all().wait_recv()

    def wait_send(self):
        self._all().wait_send()


class ChipExchange:
    def __init__(self, chips, axis, send, recv, send_sem, recv_sem, same=False):
        self.chips, self.axis, self.send, self.recv = chips, axis, send, recv
        self.send_sem, self.recv_sem, self.same = send_sem, recv_sem, same

    def start(self):
        me = lax.axis_index(self.axis)
        chip, core = me // 2, me % 2
        order = [self.chips // 2]
        for hop in range(self.chips // 2 - 1, 0, -1):
            order += [hop, self.chips - hop]
        for hop in order:
            to = lax.rem(chip + hop, self.chips)
            pltpu.make_async_remote_copy(
                src_ref=self.send if self.same else self.send.at[to],
                dst_ref=self.recv.at[chip],
                send_sem=self.send_sem,
                recv_sem=self.recv_sem,
                device_id={self.axis: 2 * to + core},
                device_id_type=pl.DeviceIdType.MESH,
            ).start()
        self.recv[chip] = self.send[...] if self.same else self.send[chip]

    def _all(self):
        some = self.recv.at[pl.ds(0, self.chips - 1)]
        return pltpu.make_async_remote_copy(
            src_ref=some,
            dst_ref=some,
            send_sem=self.send_sem,
            recv_sem=self.recv_sem,
            device_id={self.axis: lax.axis_index(self.axis)},
            device_id_type=pl.DeviceIdType.MESH,
        )

    def wait_recv(self):
        self._all().wait_recv()

    def wait_send(self):
        self._all().wait_send()


def kernel(dims, *refs):
    rows, n, ch, heads, hd, group, axis = dims
    hdim = hd // heads
    scale = hdim ** -0.5
    pairs = rows // 2
    two = 2 * n
    wide = heads * n
    chips = group // 2
    operands = refs[:10]
    local = refs[-11:-1]
    (z_ref, mask_ref, dz_ref, lns_ref, lnb_ref, wp_ref, wb_ref, bg_ref, wo_ref, bo_ref) = local
    load_sems, refs = refs[-1], refs[10:-11]
    (zo_recv, zg_out, w_full, sm_recv,
     wpt, wot, wbt, wbp, col,
     xt, xh, inv, a_s, at1, qt, kt, vt, kv, g_s, ot, ut, btmp, qbd, dbd, dot_s, dgt, dpt, dnt, dzt, dmt, dlp, dlt, pf, bias, db, maskb, stage,
     wacc,
     b_send, b_recv, mid_send, mid_recv, dz_send, dz_recv, mk_send, mk_recv, zo_send, dm_send, dm_recv,
     db_send, db_recv, w_send, w_half, w_mid, w_recv, w_part, sm_send,
     send_sems, recv_sems) = refs
    me = lax.axis_index(axis)
    core = me % 2
    loads = [pltpu.make_async_copy(src, dst, load_sems.at[k]) for k, (src, dst) in enumerate(zip(operands, local))]
    for one in loads:
        one.start()

    def exchange(slot, send, recv, same=False):
        return Exchange(group, axis, send, recv, send_sems.at[slot], recv_sems.at[slot], same)

    def chip_exchange(slot, send, recv, same=False):
        return ChipExchange(chips, axis, send, recv, send_sems.at[slot], recv_sems.at[slot], same)

    def to_sibling(slot, send, recv):
        return pltpu.make_async_remote_copy(src_ref=send, dst_ref=recv, send_sem=send_sems.at[slot], recv_sem=recv_sems.at[slot],
                                            device_id={axis: me + 1 - 2 * core}, device_id_type=pl.DeviceIdType.MESH)

    ex_b = [exchange(s, b_send.at[s], b_recv.at[s], True) for s in range(2)]
    ex_mid = exchange(2, mid_send, mid_recv)
    ex_dz = exchange(3, dz_send, dz_recv)
    ex_mask = exchange(4, mk_send, mk_recv, True)
    ex_zo = exchange(5, zo_send, zo_recv)
    ex_dm = exchange(6, dm_send, dm_recv)
    ex_db = [exchange(7 + s, db_send.at[s], db_recv.at[s]) for s in range(2)]
    ex_small = [exchange(9 + s, sm_send.at[s], sm_recv.at[s], True) for s in range(2)]
    near_w = [to_sibling(11 + s, w_send.at[s, 1 - core], w_half.at[s]) for s in range(2)]
    ex_w = [chip_exchange(13 + s, w_mid.at[s], w_recv.at[s]) for s in range(2)]
    ex_wf = [chip_exchange(15 + s, w_part.at[s], w_full.at[s, core], True) for s in range(2)]
    near_wf = [to_sibling(17 + s, w_full.at[s, core], w_full.at[s, core]) for s in range(2)]

    barrier = pltpu.get_barrier_semaphore()
    for hop in range(1, group):
        pl.semaphore_signal(barrier, inc=1, device_id={axis: lax.rem(me + hop, group)},
                            device_id_type=pl.DeviceIdType.MESH)

    for k in (3, 4, 5, 6, 7, 8, 9):
        loads[k].wait()
    head_pick = (lax.broadcasted_iota(jnp.int32, (16, heads), 0) == lax.broadcasted_iota(jnp.int32, (16, heads), 1)).astype(BF16)
    eye = (lax.broadcasted_iota(jnp.int32, (ch, ch), 0) == lax.broadcasted_iota(jnp.int32, (ch, ch), 1)).astype(BF16)
    for s in range(2):
        wpt[s] = wp_ref[s].T
        wot[s] = wo_ref[s].T
        w_heads = dot(head_pick, wb_ref[s]).astype(BF16)
        wbt[s] = w_heads
        wbp[s] = dot(eye, w_heads, NT).astype(BF16)
        for place, ref in enumerate((lns_ref, lnb_ref, bg_ref, bo_ref)):
            col[s, place] = jnp.broadcast_to(ref[s:s + 1, :], (n, ch)).T

    def zero_diag(i, carry):
        qbd[i] = jnp.zeros((hd, wide), BF16)
        dbd[i] = jnp.zeros((hd, wide), BF16)
        return carry
    lax.fori_loop(0, rows, zero_diag, 0)

    def column(s, place):
        one = col[s, place]
        return jnp.concatenate([one, one], axis=1)

    def store_diag(ref, t, value):
        for r in range(2):
            for h in range(heads):
                ref[2 * t + r, h * hdim:(h + 1) * hdim, h * n:(h + 1) * n] = value[h * hdim:(h + 1) * hdim, r * n:(r + 1) * n]

    def staged(t):
        return jnp.concatenate([stage[pl.ds(2 * t + r, n, stride=rows), :] for r in range(2)], axis=0)

    def unpack(recv):
        stage[...] = recv[...].astype(F32).reshape(group * rows * rows, ch)

    def pack(send, t, value):
        parts = [value[r * n:(r + 1) * n].reshape(group, n // group, ch) for r in range(2)]
        send[:, pl.ds(pl.multiple_of(t * 16, 16), 16), :] = jnp.concatenate(parts, axis=1).astype(BF16)

    def halves(body, init, ex):
        carry = init
        for k in range(2):
            carry = lax.fori_loop(k * pairs // 2, (k + 1) * pairs // 2, body, carry)
            ex.start(pl.ds(k * rows * rows // 2, rows * rows // 2))
        return carry

    def normalize(s, t, x):
        centred = x - jnp.mean(x, axis=0, keepdims=True)
        inv_std = lax.rsqrt(jnp.mean(centred * centred, axis=0, keepdims=True) + EPS)
        x_hat = centred * inv_std
        return (x_hat * column(s, 0) + column(s, 1)).astype(BF16), x_hat, inv_std

    def keep_norm(s, t, x):
        a_t, x_hat, inv_std = normalize(s, t, x)
        xh[s, t] = x_hat
        inv[s, t] = jnp.broadcast_to(inv_std, (8, two))
        b_t = dot(wbt[s], a_t)
        btmp[pl.ds(pl.multiple_of(t * 32, 32), 32), :] = jnp.concatenate([b_t[:, :n], b_t[:, n:]], axis=0)
        return a_t

    def project(s, t, x, a_t):
        xt[s, t] = x
        a = a_t.T
        a_s[s, t] = a
        p = dot(wpt[s], a_t).astype(BF16)
        qt[s, t] = p[:hd]
        kt[s, t] = p[hd:2 * hd]
        vt[s, t] = p[2 * hd:3 * hd]
        store_diag(qbd, t, p[:hd])
        g = jax.nn.sigmoid(p[3 * hd:].astype(F32) + column(s, 2))
        g_s[s, t] = g
        kv[s, t] = dot(a, wp_ref[s, :, hd:3 * hd]).astype(BF16)
        return g

    def send_bias(s):
        for h in range(0, heads, 2):
            some = [btmp[pl.ds(h + r, rows, stride=16), :] for r in range(2)]
            b_send[s, h * rows:(h + 2) * rows, :] = jnp.concatenate(some, axis=0).astype(BF16)
        ex_b[s].start()

    def take_bias(s):
        ex_b[s].wait_recv()
        got = b_recv[s].astype(F32).reshape(group, heads, rows, n)
        for h in range(heads):
            one = got[:, h].reshape(n, n)
            bias[:, h * n:(h + 1) * n] = (one.T if s == 0 else one) * LOG2E

    def probs(s, t, r):
        i = 2 * t + r
        logits = dot(kv[s, t, r * n:(r + 1) * n, :hd], qbd[i])
        fill = maskb[s, i]
        logits = logits * (scale * LOG2E) + bias[...] + jnp.concatenate([fill] * heads, axis=1)
        e = jnp.exp2(logits - jnp.max(logits, axis=0, keepdims=True))
        return e * (1.0 / jnp.sum(e, axis=0, keepdims=True))

    def attend(s, t):
        for r in range(2):
            p = probs(s, t, r)
            pf[s, 2 * t + r] = p
            p_low = p.astype(BF16)
            v = vt[s, t]
            ot[s, t, :, r * n:(r + 1) * n] = jnp.concatenate(
                [dot(v[h * hdim:(h + 1) * hdim, r * n:(r + 1) * n], p_low[:, h * n:(h + 1) * n]) for h in range(heads)], axis=0)
        u = (ot[s, t] * g_s[s, t]).astype(BF16)
        ut[s, t] = u
        return xt[s, t] + dot(wot[s], u) + column(s, 3)

    def attend_bwd(s, t):
        for r in range(2):
            i = 2 * t + r
            p = pf[s, i]
            p_low = p.astype(BF16)
            d_p = dot(kv[s, t, r * n:(r + 1) * n, hd:], dbd[i])
            d_l = p * (d_p - jnp.sum(d_p * p, axis=0, keepdims=True))
            db[...] += d_l
            d_s = (d_l * scale).astype(BF16)
            at = slice(r * n, (r + 1) * n)
            for h in range(heads):
                hs = slice(h * hdim, (h + 1) * hdim)
                d_sh = d_s[:, h * n:(h + 1) * n]
                d_q = dot(kt[s, t, hs, at], d_sh)
                d_k = dot(qt[s, t, hs, at], d_sh, NT)
                d_v = dot(dot_s[t, hs, at], p_low[:, h * n:(h + 1) * n], NT)
                dpt[t, h * hdim:(h + 1) * hdim, at] = d_q.astype(BF16)
                dpt[t, hd + h * hdim:hd + (h + 1) * hdim, at] = d_k.astype(BF16)
                dpt[t, 2 * hd + h * hdim:2 * hd + (h + 1) * hdim, at] = d_v.astype(BF16)

    def store_d_o(t, d_o):
        dot_s[t] = d_o
        store_diag(dbd, t, d_o)

    def after_attention(s, t, gate_sum):
        g = g_s[s, t]
        d_lin = dgt[t] * ot[s, t] * g * (1.0 - g)
        dpt[t, 3 * hd:, :] = d_lin.astype(BF16)
        return dot(wp_ref[s], dpt[t]), gate_sum + d_lin

    def send_weights(s):
        top = wacc[:4 * hd].reshape(2, chips, 4 * hd // group, ch)
        low = wacc[4 * hd:].reshape(2, chips, hd // group, ch)
        w_send[s] = jnp.concatenate([top, low], axis=2).astype(BF16)
        near_w[s].start()

    def chip_sum_weights(s):
        near_w[s].wait_recv()
        w_mid[s] = (w_send[s, core].astype(F32) + w_half[s].astype(F32)).astype(BF16)
        ex_w[s].start()

    def reduce_weights(s):
        ex_w[s].wait_recv()
        w_part[s] = jnp.sum(w_recv[s].astype(F32), axis=0).astype(BF16)
        ex_wf[s].start()

    def forward_weights(s):
        ex_wf[s].wait_recv()
        near_wf[s].start()

    def send_bias_grad(s):
        for h in range(0, heads, 2):
            some = [db[:, (h + r) * n:(h + r + 1) * n] for r in range(2)]
            some = [(one.T if s == 0 else one).reshape(group, rows, n) for one in some]
            db_send[s, :, h * rows:(h + 2) * rows, :] = jnp.concatenate(some, axis=1).astype(BF16)
        ex_db[s].start()

    def take_bias_grad(s):
        ex_db[s].wait_recv()
        return jnp.sum(db_recv[s].astype(F32), axis=0).astype(BF16)

    def norm_bwd(s, t, d_n, d_own, sums):
        at16 = lax.broadcasted_iota(jnp.int32, (16, heads * rows), 0)
        at32 = lax.broadcasted_iota(jnp.int32, (16, heads * rows), 1)
        rows_of = [dot((at32 == at16 * rows + (2 * t + r)).astype(BF16), d_own) for r in range(2)]
        d_b = jnp.concatenate(rows_of, axis=1).astype(BF16)
        d_n = d_n + dot(wbp[s], d_b)
        x_hat = xh[s, t]
        d_hat = d_n * column(s, 0)
        along = jnp.mean(d_hat * x_hat, axis=0, keepdims=True)
        d_in = inv[s, t, 0:1, :] * (d_hat - jnp.mean(d_hat, axis=0, keepdims=True) - x_hat * along)
        gain_sum, shift_sum, wb_sum = sums
        more = dot(d_b, a_s[0, t]) if s == 0 else dot(d_b, at1[t], NT)
        return d_in, (gain_sum + d_n * x_hat, shift_sum + d_n, wb_sum + more)

    def lanes_to_row(value):
        return jnp.sum((value[:, :n] + value[:, n:]).T, axis=0, keepdims=True)

    def send_small(s, sums, gate_sum, b_out_row):
        gain_sum, shift_sum, wb_sum = sums
        sm_send[s, 0:1, :] = lanes_to_row(gain_sum)
        sm_send[s, 1:2, :] = lanes_to_row(shift_sum)
        sm_send[s, 2:3, :] = lanes_to_row(gate_sum)
        sm_send[s, 3:4, :] = b_out_row
        sm_send[s, 4:4 + heads, :] = wb_sum[:heads]
        ex_small[s].start()

    zero_row = jnp.zeros((1, ch), F32)
    zero_tile = jnp.zeros((ch, two), F32)
    zero_sums = (zero_tile, zero_tile, jnp.zeros((16, ch), F32))

    loads[0].wait()

    def project_rows(t, carry):
        x = jnp.concatenate([z_ref[2 * t + r].astype(F32).T for r in range(2)], axis=1)
        project(0, t, x, keep_norm(0, t, x))
        return carry
    lax.fori_loop(0, pairs, project_rows, 0)
    pl.semaphore_wait(barrier, group - 1)
    send_bias(0)
    loads[1].wait()
    loads[2].wait()

    def pack_dz(t, b_out_row):
        d_y = jnp.concatenate([dz_ref[2 * t + r].astype(F32) for r in range(2)], axis=0)
        pack(dz_send, t, d_y)
        dzt[t] = d_y.T
        return b_out_row + jnp.sum(d_y, axis=0, keepdims=True)
    b_out_row1 = lax.fori_loop(0, pairs, pack_dz, zero_row)
    mk_send[...] = mask_ref[...].astype(F32).astype(BF16)
    ex_dz.start()
    ex_mask.start()
    fill_rows = (mask_ref[...].astype(F32) - 1.0) * (MASK_FILL * LOG2E)
    for i in range(rows):
        maskb[0, i] = jnp.broadcast_to(fill_rows[i:i + 1, :], (n, n)).T
    take_bias(0)

    def forward_rows(t, carry):
        y = attend(0, t)
        pack(mid_send, t, y.T)
        at1[t] = keep_norm(1, t, y.astype(BF16).astype(F32))
        return carry
    halves(forward_rows, 0, ex_mid)
    send_bias(1)

    ex_dz.wait_recv()
    unpack(dz_recv)

    def gate_cols(t, carry):
        d_low = staged(t).astype(BF16)
        dlp[t] = d_low
        dgt[t] = dot(wo_ref[1], d_low, NT)
        return carry
    lax.fori_loop(0, pairs, gate_cols, 0)
    ex_mask.wait_recv()
    whole = mk_recv[...].astype(F32).reshape(n, n).astype(BF16)
    for i in range(rows):
        pick = (lax.broadcasted_iota(jnp.int32, (n, n), 0) == me * rows + i).astype(BF16)
        maskb[1, i] = (dot(whole, pick) - 1.0) * (MASK_FILL * LOG2E)

    ex_mid.wait_recv()
    unpack(mid_recv)

    def project_cols(t, carry):
        x = staged(t).T
        g = project(1, t, x, normalize(1, t, x)[0])
        store_d_o(t, (dgt[t] * g).astype(BF16))
        return carry
    lax.fori_loop(0, pairs, project_cols, 0)
    db[...] = jnp.zeros((n, wide), F32)
    take_bias(1)

    def forward_cols(t, carry):
        pack(zo_send, t, attend(1, t).T)
        return carry
    lax.fori_loop(0, pairs, forward_cols, 0)
    ex_zo.start()

    def backward_cols(t, carry):
        attend_bwd(1, t)
        return carry
    lax.fori_loop(0, pairs, backward_cols, 0)
    send_bias_grad(1)

    def finish_cols(t, gate_sum):
        d_n, gate_sum = after_attention(1, t, gate_sum)
        pack(dm_send, t, d_n.T)
        return gate_sum
    gate_sum1 = halves(finish_cols, zero_tile, ex_dm)

    wacc[...] = jnp.zeros(wacc.shape, F32)

    def weights_cols(t, carry):
        wacc[:4 * hd] += dot(dpt[t], a_s[1, t])
        wacc[4 * hd:] += dot(ut[1, t], dlp[t])
        return carry
    lax.fori_loop(0, pairs, weights_cols, 0)
    send_weights(1)
    db[...] = jnp.zeros((n, wide), F32)
    wacc[...] = jnp.zeros(wacc.shape, F32)
    chip_sum_weights(1)

    ex_dm.wait_recv()
    unpack(dm_recv)
    d_own1 = take_bias_grad(1)

    def norm_and_gate(t, carry):
        sums, b_out_sum = carry
        d_in, sums = norm_bwd(1, t, staged(t).T, d_own1, sums)
        d_y = d_in + dzt[t]
        dmt[t] = d_y
        d_low = d_y.astype(BF16)
        dlt[t] = d_low
        d_gated = dot(wo_ref[0], d_low)
        dgt[t] = d_gated
        store_d_o(t, (d_gated * g_s[0, t]).astype(BF16))
        return sums, b_out_sum + d_y
    sums1, b_out_sum = lax.fori_loop(0, pairs, norm_and_gate, (zero_sums, zero_tile))

    def backward_rows(t, carry):
        attend_bwd(0, t)
        return carry
    lax.fori_loop(0, pairs, backward_rows, 0)
    send_bias_grad(0)

    def finish_rows(t, gate_sum):
        d_n, gate_sum = after_attention(0, t, gate_sum)
        dnt[t] = d_n
        wacc[:4 * hd] += dot(dpt[t], a_s[0, t])
        wacc[4 * hd:] += dot(ut[0, t], dlt[t], NT)
        return gate_sum
    gate_sum0 = lax.fori_loop(0, pairs, finish_rows, zero_tile)
    send_weights(0)
    reduce_weights(1)
    send_small(1, sums1, gate_sum1, b_out_row1)
    b_out_row0 = lanes_to_row(b_out_sum)
    chip_sum_weights(0)
    d_own0 = take_bias_grad(0)

    def norm_rows(t, sums):
        d_in, sums = norm_bwd(0, t, dnt[t], d_own0, sums)
        d_x = (d_in + dmt[t]).T.astype(BF16)
        for r in range(2):
            zg_out[2 * t + r] = d_x[r * n:(r + 1) * n]
        return sums
    sums0 = lax.fori_loop(0, pairs, norm_rows, zero_sums)
    send_small(0, sums0, gate_sum0, b_out_row0)
    reduce_weights(0)
    forward_weights(1)
    forward_weights(0)

    for one in [ex_zo] + ex_small + near_wf:
        one.wait_recv()
    for one in ex_b + [ex_mid, ex_dz, ex_mask, ex_zo, ex_dm] + ex_db + ex_small + near_w + ex_w + ex_wf + near_wf:
        one.wait_send()


def finish(dims, zo_ref, zg_ref, w_ref, sm_ref,
           zo_out, zg_out, lns_out, lnb_out, wp_out, wb_out, bg_out, wo_out, bo_out, stage):
    rows, n, ch, heads, hd, group = dims
    zg_out[...] = zg_ref[...]
    stage[...] = zo_ref[...].astype(F32).reshape(group * rows * rows, ch)
    for i in range(rows):
        zo_out[i] = stage[pl.ds(i, n, stride=rows), :].astype(BF16)
    cut = 4 * hd // group
    for s in range(2):
        full = w_ref[s].astype(F32).reshape(group, 5 * hd // group, ch)
        wp_out[s] = full[:, :cut].reshape(4 * hd, ch).T
        wo_out[s] = full[:, cut:].reshape(hd, ch)
        total = jnp.sum(sm_ref[s], axis=0)
        for place, ref in enumerate((lns_out, lnb_out, bg_out, bo_out)):
            ref[s:s + 1, :] = total[place:place + 1, :]
        wb_out[s] = total[4:4 + heads]


def solution(mesh):
    axis = 'dap'
    group = mesh.shape[axis]
    row_spec = P(('dp', axis), None, None)
    mask_spec = P(('dp', axis), None)
    grad_spec = P('dp')

    def per_device(z, pair_mask, dz_out, ln_scale, ln_shift, w_proj, w_bias, b_gate, w_out, b_out):
        rows, n, ch = z.shape
        heads = w_bias.shape[-1]
        hd = b_gate.shape[-1]
        pairs, two, wide = rows // 2, 2 * n, heads * n
        piece = (group, rows * rows, ch)
        w_rows = 5 * hd // group

        def vmem(shape, dtype):
            return pltpu.VMEM(shape, dtype)

        w_heads = jnp.swapaxes(w_bias, 1, 2)
        like = [z, z, ln_scale, ln_shift, w_proj, w_heads, b_gate, w_out, b_out]
        out_shape = [jax.ShapeDtypeStruct(a.shape, BF16 if k < 2 else F32) for k, a in enumerate(like)]
        chips = group // 2
        mid_shape = [jax.ShapeDtypeStruct(piece, BF16), jax.ShapeDtypeStruct(z.shape, BF16),
                     jax.ShapeDtypeStruct((2, 2, chips, w_rows, ch), BF16), jax.ShapeDtypeStruct((2, group, 8, ch), F32)]
        tile = (pairs, ch, two)
        scratch = [
            vmem((2, 4 * hd, ch), BF16), vmem((2, ch, hd), BF16), vmem((2, 16, ch), BF16), vmem((2, ch, 16), BF16), vmem((2, 4, ch, n), F32),
            vmem((2,) + tile, F32), vmem((2,) + tile, F32), vmem((2, pairs, 8, two), F32), vmem((2, pairs, two, ch), BF16), vmem(tile, BF16),
            vmem((2, pairs, hd, two), BF16), vmem((2, pairs, hd, two), BF16), vmem((2, pairs, hd, two), BF16), vmem((2, pairs, two, 2 * hd), BF16),
            vmem((2, pairs, hd, two), F32), vmem((2, pairs, hd, two), F32), vmem((2, pairs, hd, two), BF16), vmem((rows * 16, n), F32),
            vmem((rows, hd, wide), BF16), vmem((rows, hd, wide), BF16), vmem((pairs, hd, two), BF16), vmem((pairs, hd, two), F32),
            vmem((pairs, 4 * hd, two), BF16), vmem(tile, F32), vmem(tile, F32), vmem(tile, F32), vmem((pairs, two, ch), BF16), vmem(tile, BF16),
            vmem((2, rows, n, wide), F32), vmem((n, wide), F32), vmem((n, wide), F32),
            vmem((2, rows, n, n), F32), vmem((group * rows * rows, ch), F32),
            vmem((5 * hd, ch), F32),
            vmem((2, heads * rows, n), BF16), vmem((2, group, heads * rows, n), BF16), vmem(piece, BF16), vmem(piece, BF16), vmem(piece, BF16), vmem(piece, BF16),
            vmem((rows, n), BF16), vmem((group, rows, n), BF16), vmem(piece, BF16), vmem(piece, BF16), vmem(piece, BF16),
            vmem((2, group, heads * rows, n), BF16), vmem((2, group, heads * rows, n), BF16),
            vmem((2, 2, chips, w_rows, ch), BF16), vmem((2, chips, w_rows, ch), BF16), vmem((2, chips, w_rows, ch), BF16), vmem((2, chips, w_rows, ch), BF16),
            vmem((2, w_rows, ch), BF16), vmem((2, 8, ch), F32),
            pltpu.SemaphoreType.DMA((19,)), pltpu.SemaphoreType.DMA((19,)),
        ]
        operands = (z, pair_mask, dz_out, ln_scale, ln_shift, w_proj, w_heads, b_gate, w_out, b_out)
        scratch += [vmem(a.shape, a.dtype) for a in operands] + [pltpu.SemaphoreType.DMA((10,))]
        in_vmem = pl.BlockSpec(memory_space=pltpu.VMEM)
        mid = pl.pallas_call(
            functools.partial(kernel, (rows, n, ch, heads, hd, group, axis)),
            out_shape=mid_shape,
            in_specs=[pl.BlockSpec(memory_space=pltpu.HBM)] * 10,
            out_specs=[in_vmem] * 4,
            scratch_shapes=scratch,
            compiler_params=pltpu.CompilerParams(collective_id=0, has_side_effects=True, vmem_limit_bytes=40 * 1024 * 1024),
        )(*[pltpu.with_memory_space_constraint(a, pltpu.HBM) for a in operands])
        out = pl.pallas_call(
            functools.partial(finish, (rows, n, ch, heads, hd, group)),
            out_shape=out_shape,
            in_specs=[in_vmem] * 4,
            out_specs=[in_vmem] * 9,
            scratch_shapes=[vmem((group * rows * rows, ch), F32)],
            compiler_params=pltpu.CompilerParams(vmem_limit_bytes=16 * 1024 * 1024),
        )(*mid)
        return tuple(out[:5]) + (jnp.swapaxes(out[5], 1, 2),) + tuple(out[6:])

    return jax.shard_map(per_device, mesh=mesh, in_specs=(row_spec, mask_spec, row_spec) + (P(),) * 7,
                         out_specs=(row_spec, row_spec) + (grad_spec,) * 7, check_vma=False)
```

```python
import functools

import jax
import jax.numpy as jnp
from jax import lax
from jax.experimental import pallas as pl
from jax.experimental.pallas import tpu as pltpu
from jax.sharding import PartitionSpec as P

EPS = 1e-5
MASK_FILL = 1e9
LOG2E = 1.4426950408889634
F32 = jnp.float32
BF16 = jnp.bfloat16
NN = (((1,), (0,)), ((), ()))
NT = (((1,), (1,)), ((), ()))


def dot(a, b, dims=NN):
    return lax.dot_general(a, b, dims, preferred_element_type=F32)


class Exchange:
    def __init__(self, group, axis, send, recv, send_sem, recv_sem, same=False):
        self.group, self.axis, self.send, self.recv = group, axis, send, recv
        self.send_sem, self.recv_sem, self.same = send_sem, recv_sem, same

    def start(self, part=None):
        me = lax.axis_index(self.axis)
        half = self.group // 2
        order = [half]
        for hop in range(half - 1, 0, -1):
            order += [hop, self.group - hop]
        for hop in order:
            peer = lax.rem(me + hop, self.group)
            source = self.send if self.same else self.send.at[peer] if part is None else self.send.at[peer, part]
            pltpu.make_async_remote_copy(
                src_ref=source,
                dst_ref=self.recv.at[me] if part is None else self.recv.at[me, part],
                send_sem=self.send_sem,
                recv_sem=self.recv_sem,
                device_id={self.axis: peer},
                device_id_type=pl.DeviceIdType.MESH,
            ).start()
        if part is None:
            self.recv[me] = self.send[...] if self.same else self.send[me]
        else:
            self.recv[me, part] = self.send[me, part]

    def _all(self):
        some = self.recv.at[pl.ds(0, self.group - 1)]
        return pltpu.make_async_remote_copy(
            src_ref=some,
            dst_ref=some,
            send_sem=self.send_sem,
            recv_sem=self.recv_sem,
            device_id={self.axis: lax.axis_index(self.axis)},
            device_id_type=pl.DeviceIdType.MESH,
        )

    def wait_recv(self):
        self._all().wait_recv()

    def wait_send(self):
        self._all().wait_send()


class ChipExchange:
    def __init__(self, chips, axis, send, recv, send_sem, recv_sem, same=False):
        self.chips, self.axis, self.send, self.recv = chips, axis, send, recv
        self.send_sem, self.recv_sem, self.same = send_sem, recv_sem, same

    def start(self):
        me = lax.axis_index(self.axis)
        chip, core = me // 2, me % 2
        order = [self.chips // 2]
        for hop in range(self.chips // 2 - 1, 0, -1):
            order += [hop, self.chips - hop]
        for hop in order:
            to = lax.rem(chip + hop, self.chips)
            pltpu.make_async_remote_copy(
                src_ref=self.send if self.same else self.send.at[to],
                dst_ref=self.recv.at[chip],
                send_sem=self.send_sem,
                recv_sem=self.recv_sem,
                device_id={self.axis: 2 * to + core},
                device_id_type=pl.DeviceIdType.MESH,
            ).start()
        self.recv[chip] = self.send[...] if self.same else self.send[chip]

    def _all(self):
        some = self.recv.at[pl.ds(0, self.chips - 1)]
        return pltpu.make_async_remote_copy(
            src_ref=some,
            dst_ref=some,
            send_sem=self.send_sem,
            recv_sem=self.recv_sem,
            device_id={self.axis: lax.axis_index(self.axis)},
            device_id_type=pl.DeviceIdType.MESH,
        )

    def wait_recv(self):
        self._all().wait_recv()

    def wait_send(self):
        self._all().wait_send()


def kernel(dims, *refs):
    rows, n, ch, heads, hd, group, axis = dims
    hdim = hd // heads
    scale = hdim ** -0.5
    pairs = rows // 2
    two = 2 * n
    wide = heads * n
    chips = group // 2
    operands = refs[:10]
    local = refs[-11:-1]
    (z_ref, mask_ref, dz_ref, lns_ref, lnb_ref, wp_ref, wb_ref, bg_ref, wo_ref, bo_ref) = local
    load_sems, refs = refs[-1], refs[10:-11]
    (zo_recv, zg_out, w_full, sm_recv,
     wpt, wot, wbt, wbp, col,
     xt, xh, inv, a_s, at1, qt, kt, vt, kv, g_s, ot, ut, btmp, qbd, dbd, dot_s, dgt, dpt, dnt, dzt, dmt, dlp, dlt, pf, bias, db, maskb, stage,
     wacc, wsel, dbt,
     b_send, b_recv, mid_send, mid_recv, dz_send, dz_recv, mk_send, mk_recv, zo_send, dm_send, dm_recv,
     db_send, db_recv, w_send, w_half, w_mid, w_recv, w_part, sm_send,
     send_sems, recv_sems) = refs
    me = lax.axis_index(axis)
    core = me % 2
    loads = [pltpu.make_async_copy(src, dst, load_sems.at[k]) for k, (src, dst) in enumerate(zip(operands, local))]
    for one in loads:
        one.start()

    def exchange(slot, send, recv, same=False):
        return Exchange(group, axis, send, recv, send_sems.at[slot], recv_sems.at[slot], same)

    def chip_exchange(slot, send, recv, same=False):
        return ChipExchange(chips, axis, send, recv, send_sems.at[slot], recv_sems.at[slot], same)

    def to_sibling(slot, send, recv):
        return pltpu.make_async_remote_copy(src_ref=send, dst_ref=recv, send_sem=send_sems.at[slot], recv_sem=recv_sems.at[slot],
                                            device_id={axis: me + 1 - 2 * core}, device_id_type=pl.DeviceIdType.MESH)

    ex_b = [exchange(s, b_send.at[s], b_recv.at[s], True) for s in range(2)]
    ex_mid = exchange(2, mid_send, mid_recv)
    ex_dz = exchange(3, dz_send, dz_recv)
    ex_mask = exchange(4, mk_send, mk_recv, True)
    ex_zo = exchange(5, zo_send, zo_recv)
    ex_dm = exchange(6, dm_send, dm_recv)
    ex_db = [exchange(7 + s, db_send.at[s], db_recv.at[s]) for s in range(2)]
    ex_small = [exchange(9 + s, sm_send.at[s], sm_recv.at[s], True) for s in range(2)]
    near_w = [to_sibling(11 + s, w_send.at[s, 1 - core], w_half.at[s]) for s in range(2)]
    ex_w = [chip_exchange(13 + s, w_mid.at[s], w_recv.at[s]) for s in range(2)]
    ex_wf = [chip_exchange(15 + s, w_part.at[s], w_full.at[s, core], True) for s in range(2)]
    near_wf = [to_sibling(17 + s, w_full.at[s, core], w_full.at[s, core]) for s in range(2)]

    barrier = pltpu.get_barrier_semaphore()
    for hop in range(1, group):
        pl.semaphore_signal(barrier, inc=1, device_id={axis: lax.rem(me + hop, group)},
                            device_id_type=pl.DeviceIdType.MESH)

    for k in (3, 4, 5, 6, 7, 8, 9):
        loads[k].wait()
    head_pick = (lax.broadcasted_iota(jnp.int32, (16, heads), 0) == lax.broadcasted_iota(jnp.int32, (16, heads), 1)).astype(BF16)
    eye = (lax.broadcasted_iota(jnp.int32, (ch, ch), 0) == lax.broadcasted_iota(jnp.int32, (ch, ch), 1)).astype(BF16)
    for s in range(2):
        wpt[s] = wp_ref[s].T
        wot[s] = wo_ref[s].T
        w_heads = dot(head_pick, wb_ref[s]).astype(BF16)
        wbt[s] = w_heads
        wbp[s] = dot(eye, w_heads, NT).astype(BF16)
        for place, ref in enumerate((lns_ref, lnb_ref, bg_ref, bo_ref)):
            col[s, place] = jnp.broadcast_to(ref[s:s + 1, :], (n, ch)).T

    def zero_diag(i, carry):
        qbd[i] = jnp.zeros((hd, wide), BF16)
        dbd[i] = jnp.zeros((hd, wide), BF16)
        return carry
    lax.fori_loop(0, rows, zero_diag, 0)

    def column(s, place):
        one = col[s, place]
        return jnp.concatenate([one, one], axis=1)

    def store_diag(ref, t, value):
        for r in range(2):
            for h in range(heads):
                ref[2 * t + r, h * hdim:(h + 1) * hdim, h * n:(h + 1) * n] = value[h * hdim:(h + 1) * hdim, r * n:(r + 1) * n]

    def staged(t):
        return jnp.concatenate([stage[pl.ds(2 * t + r, n, stride=rows), :] for r in range(2)], axis=0)

    def unpack(recv):
        stage[...] = recv[...].astype(F32).reshape(group * rows * rows, ch)

    def pack(send, t, value):
        parts = [value[r * n:(r + 1) * n].reshape(group, n // group, ch) for r in range(2)]
        send[:, pl.ds(pl.multiple_of(t * 16, 16), 16), :] = jnp.concatenate(parts, axis=1).astype(BF16)

    def half(k):
        return pl.ds(k * rows * rows // 2, rows * rows // 2)

    def normalize(s, t, x):
        centred = x - jnp.mean(x, axis=0, keepdims=True)
        inv_std = lax.rsqrt(jnp.mean(centred * centred, axis=0, keepdims=True) + EPS)
        x_hat = centred * inv_std
        return (x_hat * column(s, 0) + column(s, 1)).astype(BF16), x_hat, inv_std

    def keep_norm(s, t, x):
        a_t, x_hat, inv_std = normalize(s, t, x)
        xh[s, t] = x_hat
        inv[s, t] = jnp.broadcast_to(inv_std, (8, two))
        b_t = dot(wbt[s], a_t)
        btmp[pl.ds(pl.multiple_of(t * 32, 32), 32), :] = jnp.concatenate([b_t[:, :n], b_t[:, n:]], axis=0)
        return a_t

    def project(s, t, x, a_t):
        xt[s, t] = x
        a = a_t.T
        a_s[s, t] = a
        p = dot(wpt[s], a_t).astype(BF16)
        qt[s, t] = p[:hd]
        kt[s, t] = p[hd:2 * hd]
        vt[s, t] = p[2 * hd:3 * hd]
        store_diag(qbd, t, p[:hd])
        g = jax.nn.sigmoid(p[3 * hd:].astype(F32) + column(s, 2))
        g_s[s, t] = g
        kv[s, t] = dot(a, wp_ref[s, :, hd:3 * hd]).astype(BF16)
        return g

    def send_bias(s):
        for h in range(0, heads, 2):
            some = [btmp[pl.ds(h + r, rows, stride=16), :] for r in range(2)]
            b_send[s, h * rows:(h + 2) * rows, :] = jnp.concatenate(some, axis=0).astype(BF16)
        ex_b[s].start()

    def take_bias(s):
        ex_b[s].wait_recv()
        got = b_recv[s].astype(F32).reshape(group, heads, rows, n)
        for h in range(heads):
            one = got[:, h].reshape(n, n)
            bias[:, h * n:(h + 1) * n] = (one.T if s == 0 else one) * LOG2E

    def logits(s):
        for i in range(rows):
            t, r = divmod(i, 2)
            fill = maskb[s, i]
            raw = dot(kv[s, t, r * n:(r + 1) * n, :hd], qbd[i])
            for h in range(heads):
                pf[s, i, :, h * n:(h + 1) * n] = raw[:, h * n:(h + 1) * n] * (scale * LOG2E) + fill

    def attend(s, some):
        for i in some:
            t, r = divmod(i, 2)
            for h in range(heads):
                cols = slice(h * n, (h + 1) * n)
                x = pf[s, i, :, cols] + bias[:, cols]
                e = jnp.exp2(x - jnp.max(x, axis=0, keepdims=True))
                p = e * (1.0 / jnp.sum(e, axis=0, keepdims=True))
                pf[s, i, :, cols] = p
                hs = slice(h * hdim, (h + 1) * hdim)
                ot[s, t, hs, r * n:(r + 1) * n] = dot(vt[s, t, hs, r * n:(r + 1) * n], p.astype(BF16))

    def block_out(s, t):
        u = (ot[s, t] * g_s[s, t]).astype(BF16)
        ut[s, t] = u
        return xt[s, t] + dot(wot[s], u) + column(s, 3)

    def attend_bwd(s, some):
        def d_probs(i):
            t, r = divmod(i, 2)
            return dot(kv[s, t, r * n:(r + 1) * n, hd:], dbd[i])
        ahead = d_probs(some[0])
        for k, i in enumerate(some):
            t, r = divmod(i, 2)
            d_p = ahead
            if k + 1 < len(some):
                ahead = d_probs(some[k + 1])
            at = slice(r * n, (r + 1) * n)
            for h in range(heads):
                cols = slice(h * n, (h + 1) * n)
                p = pf[s, i, :, cols]
                d_ph = d_p[:, cols]
                d_l = p * (d_ph - jnp.sum(d_ph * p, axis=0, keepdims=True))
                db[:, cols] += d_l
                d_s = (d_l * scale).astype(BF16)
                hs = slice(h * hdim, (h + 1) * hdim)
                d_q = dot(kt[s, t, hs, at], d_s)
                d_k = dot(qt[s, t, hs, at], d_s, NT)
                d_v = dot(dot_s[t, hs, at], p.astype(BF16), NT)
                dpt[t, h * hdim:(h + 1) * hdim, at] = d_q.astype(BF16)
                dpt[t, hd + h * hdim:hd + (h + 1) * hdim, at] = d_k.astype(BF16)
                dpt[t, 2 * hd + h * hdim:2 * hd + (h + 1) * hdim, at] = d_v.astype(BF16)

    def store_d_o(t, d_o):
        dot_s[t] = d_o
        store_diag(dbd, t, d_o)

    def after_attention(s, t, gate_sum):
        g = g_s[s, t]
        d_lin = dgt[t] * ot[s, t] * g * (1.0 - g)
        dpt[t, 3 * hd:, :] = d_lin.astype(BF16)
        return dot(wp_ref[s], dpt[t]), gate_sum + d_lin

    def send_weights(s):
        top = wacc[:4 * hd].reshape(2, chips, 4 * hd // group, ch)
        low = wacc[4 * hd:].reshape(2, chips, hd // group, ch)
        w_send[s] = jnp.concatenate([top, low], axis=2).astype(BF16)
        near_w[s].start()

    def chip_sum_weights(s):
        near_w[s].wait_recv()
        w_mid[s] = (w_send[s, core].astype(F32) + w_half[s].astype(F32)).astype(BF16)
        ex_w[s].start()

    def reduce_weights(s):
        ex_w[s].wait_recv()
        w_part[s] = jnp.sum(w_recv[s].astype(F32), axis=0).astype(BF16)
        ex_wf[s].start()

    def forward_weights(s):
        ex_wf[s].wait_recv()
        near_wf[s].start()

    def send_bias_grad(s):
        for h in range(0, heads, 2):
            some = [db[:, (h + r) * n:(h + r + 1) * n] for r in range(2)]
            some = [(one.T if s == 0 else one).reshape(group, rows, n) for one in some]
            db_send[s, :, h * rows:(h + 2) * rows, :] = jnp.concatenate(some, axis=1).astype(BF16)
        ex_db[s].start()

    def take_bias_grad(s):
        ex_db[s].wait_recv()
        return jnp.sum(db_recv[s].astype(F32), axis=0).astype(BF16)

    def bias_terms(s, d_own):
        return [jnp.concatenate([dot(wsel[s, 2 * t + r], d_own) for r in range(2)], axis=1) for t in range(pairs)]

    def head_weight_grad(s, d_own):
        at16 = lax.broadcasted_iota(jnp.int32, (16, heads * rows), 0)
        at32 = lax.broadcasted_iota(jnp.int32, (16, heads * rows), 1)
        for t in range(pairs):
            rows_of = [dot((at32 == at16 * rows + (2 * t + r)).astype(BF16), d_own) for r in range(2)]
            dbt[t] = jnp.concatenate(rows_of, axis=1).astype(BF16)
        total = None
        for t in range(pairs):
            one = dot(dbt[t], a_s[0, t]) if s == 0 else dot(dbt[t], at1[t], NT)
            total = one if total is None else total + one
        return total

    def norm_bwd(s, t, d_n, sums):
        x_hat = xh[s, t]
        d_hat = d_n * column(s, 0)
        along = jnp.mean(d_hat * x_hat, axis=0, keepdims=True)
        d_in = inv[s, t, 0:1, :] * (d_hat - jnp.mean(d_hat, axis=0, keepdims=True) - x_hat * along)
        return d_in, (sums[0] + d_n * x_hat, sums[1] + d_n)

    def lanes_to_row(value):
        return jnp.sum((value[:, :n] + value[:, n:]).T, axis=0, keepdims=True)

    def send_small(s, sums, wb_sum, gate_sum, b_out_row):
        gain_sum, shift_sum = sums
        sm_send[s, 0:1, :] = lanes_to_row(gain_sum)
        sm_send[s, 1:2, :] = lanes_to_row(shift_sum)
        sm_send[s, 2:3, :] = lanes_to_row(gate_sum)
        sm_send[s, 3:4, :] = b_out_row
        sm_send[s, 4:4 + heads, :] = wb_sum[:heads]
        ex_small[s].start()

    zero_tile = jnp.zeros((ch, two), F32)
    early, late = range(pairs // 2), range(pairs // 2, pairs)

    loads[0].wait()
    for t in range(pairs):
        x = jnp.concatenate([z_ref[2 * t + r].astype(F32).T for r in range(2)], axis=1)
        project(0, t, x, keep_norm(0, t, x))
    pl.semaphore_wait(barrier, group - 1)
    send_bias(0)
    loads[1].wait()
    fill_rows = (mask_ref[...].astype(F32) - 1.0) * (MASK_FILL * LOG2E)
    for i in range(rows):
        maskb[0, i] = jnp.broadcast_to(fill_rows[i:i + 1, :], (n, n)).T
    logits(0)
    loads[2].wait()
    b_out_row1 = jnp.zeros((1, ch), F32)
    for t in range(pairs):
        d_y = jnp.concatenate([dz_ref[2 * t + r].astype(F32) for r in range(2)], axis=0)
        pack(dz_send, t, d_y)
        dzt[t] = d_y.T
        b_out_row1 = b_out_row1 + jnp.sum(d_y, axis=0, keepdims=True)
    mk_send[...] = mask_ref[...].astype(F32).astype(BF16)
    ex_dz.start()
    ex_mask.start()
    at16 = lax.broadcasted_iota(jnp.int32, (16, heads * rows), 0)
    at32 = lax.broadcasted_iota(jnp.int32, (16, heads * rows), 1)
    for s in range(2):
        for i in range(rows):
            wsel[s, i] = dot(wbp[s], ((at32 == at16 * rows + i) & (at16 < heads)).astype(BF16)).astype(BF16)
    take_bias(0)

    for k, some in enumerate((early, late)):
        attend(0, range(2 * some[0], 2 * some[-1] + 2))
        for t in some:
            y = block_out(0, t)
            pack(mid_send, t, y.T)
            xt[1, t] = y.astype(BF16).astype(F32)
        ex_mid.start(half(k))
    for t in range(pairs):
        at1[t] = keep_norm(1, t, xt[1, t])
    send_bias(1)

    ex_dz.wait_recv()
    unpack(dz_recv)
    for t in range(pairs):
        d_low = staged(t).astype(BF16)
        dlp[t] = d_low
        dgt[t] = dot(wo_ref[1], d_low, NT)
    db[...] = jnp.zeros((n, wide), F32)
    ex_mask.wait_recv()
    whole = mk_recv[...].astype(F32).reshape(n, n).astype(BF16)
    for i in range(rows):
        pick = (lax.broadcasted_iota(jnp.int32, (n, n), 0) == me * rows + i).astype(BF16)
        maskb[1, i] = (dot(whole, pick) - 1.0) * (MASK_FILL * LOG2E)

    ex_mid.wait_recv()
    unpack(mid_recv)
    for t in range(pairs):
        x = staged(t).T
        g = project(1, t, x, normalize(1, t, x)[0])
        store_d_o(t, (dgt[t] * g).astype(BF16))
    logits(1)
    take_bias(1)
    attend(1, range(rows))

    gate_sum1 = zero_tile
    for k, some in enumerate((early, late)):
        attend_bwd(1, range(2 * some[0], 2 * some[-1] + 2))
        for t in some:
            d_n, gate_sum1 = after_attention(1, t, gate_sum1)
            pack(dm_send, t, d_n.T)
        if k == 1:
            send_bias_grad(1)
        ex_dm.start(half(k))
    for t in range(pairs):
        pack(zo_send, t, block_out(1, t).T)
    ex_zo.start()

    def sum_weights(s):
        top, low = None, None
        for t in range(pairs):
            one = dot(dpt[t], a_s[s, t])
            two_ = dot(ut[1, t], dlp[t]) if s == 1 else dot(ut[0, t], dlt[t], NT)
            top, low = (one, two_) if top is None else (top + one, low + two_)
        wacc[:4 * hd] = top
        wacc[4 * hd:] = low
    sum_weights(1)
    send_weights(1)
    db[...] = jnp.zeros((n, wide), F32)
    chip_sum_weights(1)

    d_own1 = take_bias_grad(1)
    terms = bias_terms(1, d_own1)
    for t in range(pairs):
        dnt[t] = terms[t]
    ex_dm.wait_recv()
    unpack(dm_recv)
    sums1, b_out_sum = (zero_tile, zero_tile), zero_tile
    for t in range(pairs):
        d_in, sums1 = norm_bwd(1, t, staged(t).T + dnt[t], sums1)
        d_y = d_in + dzt[t]
        dmt[t] = d_y
        d_low = d_y.astype(BF16)
        dlt[t] = d_low
        d_gated = dot(wo_ref[0], d_low)
        dgt[t] = d_gated
        store_d_o(t, (d_gated * g_s[0, t]).astype(BF16))
        b_out_sum = b_out_sum + d_y

    attend_bwd(0, range(rows))
    send_bias_grad(0)
    gate_sum0 = zero_tile
    for t in range(pairs):
        dnt[t], gate_sum0 = after_attention(0, t, gate_sum0)
    sum_weights(0)
    send_weights(0)
    reduce_weights(1)
    send_small(1, sums1, head_weight_grad(1, d_own1), gate_sum1, b_out_row1)
    b_out_row0 = lanes_to_row(b_out_sum)
    chip_sum_weights(0)

    d_own0 = take_bias_grad(0)
    terms = bias_terms(0, d_own0)
    sums0 = (zero_tile, zero_tile)
    for t in range(pairs):
        d_in, sums0 = norm_bwd(0, t, dnt[t] + terms[t], sums0)
        d_x = (d_in + dmt[t]).T.astype(BF16)
        for r in range(2):
            zg_out[2 * t + r] = d_x[r * n:(r + 1) * n]
    send_small(0, sums0, head_weight_grad(0, d_own0), gate_sum0, b_out_row0)
    reduce_weights(0)
    forward_weights(1)
    forward_weights(0)

    for one in [ex_zo] + ex_small + near_wf:
        one.wait_recv()
    for one in ex_b + [ex_mid, ex_dz, ex_mask, ex_zo, ex_dm] + ex_db + ex_small + near_w + ex_w + ex_wf + near_wf:
        one.wait_send()


def finish(dims, zo_ref, zg_ref, w_ref, sm_ref,
           zo_out, zg_out, lns_out, lnb_out, wp_out, wb_out, bg_out, wo_out, bo_out, stage):
    rows, n, ch, heads, hd, group = dims
    zg_out[...] = zg_ref[...]
    stage[...] = zo_ref[...].astype(F32).reshape(group * rows * rows, ch)
    for i in range(rows):
        zo_out[i] = stage[pl.ds(i, n, stride=rows), :].astype(BF16)
    cut = 4 * hd // group
    for s in range(2):
        full = w_ref[s].astype(F32).reshape(group, 5 * hd // group, ch)
        wp_out[s] = full[:, :cut].reshape(4 * hd, ch).T
        wo_out[s] = full[:, cut:].reshape(hd, ch)
        total = jnp.sum(sm_ref[s], axis=0)
        for place, ref in enumerate((lns_out, lnb_out, bg_out, bo_out)):
            ref[s:s + 1, :] = total[place:place + 1, :]
        wb_out[s] = total[4:4 + heads]


def solution(mesh):
    axis = 'dap'
    group = mesh.shape[axis]
    row_spec = P(('dp', axis), None, None)
    mask_spec = P(('dp', axis), None)
    grad_spec = P('dp')

    def per_device(z, pair_mask, dz_out, ln_scale, ln_shift, w_proj, w_bias, b_gate, w_out, b_out):
        rows, n, ch = z.shape
        heads = w_bias.shape[-1]
        hd = b_gate.shape[-1]
        pairs, two, wide = rows // 2, 2 * n, heads * n
        piece = (group, rows * rows, ch)
        w_rows = 5 * hd // group

        def vmem(shape, dtype):
            return pltpu.VMEM(shape, dtype)

        w_heads = jnp.swapaxes(w_bias, 1, 2)
        like = [z, z, ln_scale, ln_shift, w_proj, w_heads, b_gate, w_out, b_out]
        out_shape = [jax.ShapeDtypeStruct(a.shape, BF16 if k < 2 else F32) for k, a in enumerate(like)]
        chips = group // 2
        mid_shape = [jax.ShapeDtypeStruct(piece, BF16), jax.ShapeDtypeStruct(z.shape, BF16),
                     jax.ShapeDtypeStruct((2, 2, chips, w_rows, ch), BF16), jax.ShapeDtypeStruct((2, group, 8, ch), F32)]
        tile = (pairs, ch, two)
        scratch = [
            vmem((2, 4 * hd, ch), BF16), vmem((2, ch, hd), BF16), vmem((2, 16, ch), BF16), vmem((2, ch, 16), BF16), vmem((2, 4, ch, n), F32),
            vmem((2,) + tile, F32), vmem((2,) + tile, F32), vmem((2, pairs, 8, two), F32), vmem((2, pairs, two, ch), BF16), vmem(tile, BF16),
            vmem((2, pairs, hd, two), BF16), vmem((2, pairs, hd, two), BF16), vmem((2, pairs, hd, two), BF16), vmem((2, pairs, two, 2 * hd), BF16),
            vmem((2, pairs, hd, two), F32), vmem((2, pairs, hd, two), F32), vmem((2, pairs, hd, two), BF16), vmem((rows * 16, n), F32),
            vmem((rows, hd, wide), BF16), vmem((rows, hd, wide), BF16), vmem((pairs, hd, two), BF16), vmem((pairs, hd, two), F32),
            vmem((pairs, 4 * hd, two), BF16), vmem(tile, F32), vmem(tile, F32), vmem(tile, F32), vmem((pairs, two, ch), BF16), vmem(tile, BF16),
            vmem((2, rows, n, wide), F32), vmem((n, wide), F32), vmem((n, wide), F32),
            vmem((2, rows, n, n), F32), vmem((group * rows * rows, ch), F32),
            vmem((5 * hd, ch), F32), vmem((2, rows, ch, heads * rows), BF16), vmem((pairs, 16, two), BF16),
            vmem((2, heads * rows, n), BF16), vmem((2, group, heads * rows, n), BF16), vmem(piece, BF16), vmem(piece, BF16), vmem(piece, BF16), vmem(piece, BF16),
            vmem((rows, n), BF16), vmem((group, rows, n), BF16), vmem(piece, BF16), vmem(piece, BF16), vmem(piece, BF16),
            vmem((2, group, heads * rows, n), BF16), vmem((2, group, heads * rows, n), BF16),
            vmem((2, 2, chips, w_rows, ch), BF16), vmem((2, chips, w_rows, ch), BF16), vmem((2, chips, w_rows, ch), BF16), vmem((2, chips, w_rows, ch), BF16),
            vmem((2, w_rows, ch), BF16), vmem((2, 8, ch), F32),
            pltpu.SemaphoreType.DMA((19,)), pltpu.SemaphoreType.DMA((19,)),
        ]
        operands = (z, pair_mask, dz_out, ln_scale, ln_shift, w_proj, w_heads, b_gate, w_out, b_out)
        scratch += [vmem(a.shape, a.dtype) for a in operands] + [pltpu.SemaphoreType.DMA((10,))]
        in_vmem = pl.BlockSpec(memory_space=pltpu.VMEM)
        mid = pl.pallas_call(
            functools.partial(kernel, (rows, n, ch, heads, hd, group, axis)),
            out_shape=mid_shape,
            in_specs=[pl.BlockSpec(memory_space=pltpu.HBM)] * 10,
            out_specs=[in_vmem] * 4,
            scratch_shapes=scratch,
            compiler_params=pltpu.CompilerParams(collective_id=0, has_side_effects=True, vmem_limit_bytes=40 * 1024 * 1024),
        )(*[pltpu.with_memory_space_constraint(a, pltpu.HBM) for a in operands])
        out = pl.pallas_call(
            functools.partial(finish, (rows, n, ch, heads, hd, group)),
            out_shape=out_shape,
            in_specs=[in_vmem] * 4,
            out_specs=[in_vmem] * 9,
            scratch_shapes=[vmem((group * rows * rows, ch), F32)],
            compiler_params=pltpu.CompilerParams(vmem_limit_bytes=16 * 1024 * 1024),
        )(*mid)
        return tuple(out[:5]) + (jnp.swapaxes(out[5], 1, 2),) + tuple(out[6:])

    return jax.shard_map(per_device, mesh=mesh, in_specs=(row_spec, mask_spec, row_spec) + (P(),) * 7,
                         out_specs=(row_spec, row_spec) + (grad_spec,) * 7, check_vma=False)
```

```python
import functools

import jax
import jax.numpy as jnp
from jax import lax
from jax.experimental import pallas as pl
from jax.experimental.pallas import tpu as pltpu
from jax.sharding import PartitionSpec as P

EPS = 1e-5
MASK_FILL = 1e9
LOG2E = 1.4426950408889634
F32 = jnp.float32
BF16 = jnp.bfloat16
NN = (((1,), (0,)), ((), ()))
NT = (((1,), (1,)), ((), ()))


def dot(a, b, dims=NN):
    return lax.dot_general(a, b, dims, preferred_element_type=F32)


class Exchange:
    def __init__(self, group, axis, send, recv, send_sem, recv_sem, same=False):
        self.group, self.axis, self.send, self.recv = group, axis, send, recv
        self.send_sem, self.recv_sem, self.same = send_sem, recv_sem, same

    def start(self, part=None):
        me = lax.axis_index(self.axis)
        half = self.group // 2
        order = [half]
        for hop in range(half - 1, 0, -1):
            order += [hop, self.group - hop]
        for hop in order:
            peer = lax.rem(me + hop, self.group)
            source = self.send if self.same else self.send.at[peer] if part is None else self.send.at[peer, part]
            pltpu.make_async_remote_copy(
                src_ref=source,
                dst_ref=self.recv.at[me] if part is None else self.recv.at[me, part],
                send_sem=self.send_sem,
                recv_sem=self.recv_sem,
                device_id={self.axis: peer},
                device_id_type=pl.DeviceIdType.MESH,
            ).start()
        if part is None:
            self.recv[me] = self.send[...] if self.same else self.send[me]
        else:
            self.recv[me, part] = self.send[me, part]

    def _all(self):
        some = self.recv.at[pl.ds(0, self.group - 1)]
        return pltpu.make_async_remote_copy(
            src_ref=some,
            dst_ref=some,
            send_sem=self.send_sem,
            recv_sem=self.recv_sem,
            device_id={self.axis: lax.axis_index(self.axis)},
            device_id_type=pl.DeviceIdType.MESH,
        )

    def wait_recv(self):
        self._all().wait_recv()

    def wait_send(self):
        self._all().wait_send()


class ChipExchange:
    def __init__(self, chips, axis, send, recv, send_sem, recv_sem, same=False):
        self.chips, self.axis, self.send, self.recv = chips, axis, send, recv
        self.send_sem, self.recv_sem, self.same = send_sem, recv_sem, same

    def start(self):
        me = lax.axis_index(self.axis)
        chip, core = me // 2, me % 2
        order = [self.chips // 2]
        for hop in range(self.chips // 2 - 1, 0, -1):
            order += [hop, self.chips - hop]
        for hop in order:
            to = lax.rem(chip + hop, self.chips)
            pltpu.make_async_remote_copy(
                src_ref=self.send if self.same else self.send.at[to],
                dst_ref=self.recv.at[chip],
                send_sem=self.send_sem,
                recv_sem=self.recv_sem,
                device_id={self.axis: 2 * to + core},
                device_id_type=pl.DeviceIdType.MESH,
            ).start()
        self.recv[chip] = self.send[...] if self.same else self.send[chip]

    def _all(self):
        some = self.recv.at[pl.ds(0, self.chips - 1)]
        return pltpu.make_async_remote_copy(
            src_ref=some,
            dst_ref=some,
            send_sem=self.send_sem,
            recv_sem=self.recv_sem,
            device_id={self.axis: lax.axis_index(self.axis)},
            device_id_type=pl.DeviceIdType.MESH,
        )

    def wait_recv(self):
        self._all().wait_recv()

    def wait_send(self):
        self._all().wait_send()


def kernel(dims, *refs):
    rows, n, ch, heads, hd, group, axis = dims
    hdim = hd // heads
    scale = hdim ** -0.5
    pairs = rows // 2
    two = 2 * n
    wide = heads * n
    chips = group // 2
    operands = refs[:10]
    local = refs[-11:-1]
    (z_ref, mask_ref, dz_ref, lns_ref, lnb_ref, wp_ref, wb_ref, bg_ref, wo_ref, bo_ref) = local
    load_sems, refs = refs[-1], refs[10:-11]
    (zo_recv, zg_out, w_full, sm_recv,
     wpt, wot, wbt, col,
     xt, xh, inv, a_s, at1, qt, kt, vt, kv, g_s, ot, ut, btmp, qbd, dbd, dot_s, dgt, dpt, dnt, dzt, dmt, dlp, dlt, pf, bias, db, maskb, stage,
     wacc, wsel, dbt,
     b_send, b_recv, b1_recv, mid_send, mid_recv, dz_send, dz_recv, mk_send, mk_recv, zo_send, dm_send, dm_recv,
     db_send, db_recv, d1_send, d1_half, d1_mid, d1_recv, w_send, w_half, w_mid, w_recv, w_part, sm_send, sm_half, sm_mid,
     send_sems, recv_sems) = refs
    me = lax.axis_index(axis)
    core = me % 2
    loads = [pltpu.make_async_copy(src, dst, load_sems.at[k]) for k, (src, dst) in enumerate(zip(operands, local))]
    for one in loads:
        one.start()

    def exchange(slot, send, recv, same=False):
        return Exchange(group, axis, send, recv, send_sems.at[slot], recv_sems.at[slot], same)

    def chip_exchange(slot, send, recv, same=False):
        return ChipExchange(chips, axis, send, recv, send_sems.at[slot], recv_sems.at[slot], same)

    def to_sibling(slot, send, recv):
        return pltpu.make_async_remote_copy(src_ref=send, dst_ref=recv, send_sem=send_sems.at[slot], recv_sem=recv_sems.at[slot],
                                            device_id={axis: me + 1 - 2 * core}, device_id_type=pl.DeviceIdType.MESH)

    ex_b0 = exchange(0, b_send.at[0], b_recv, True)
    ex_b1 = chip_exchange(1, b_send.at[1], b1_recv.at[core], True)
    near_b1 = to_sibling(19, b1_recv.at[core], b1_recv.at[core])
    ex_mid = exchange(2, mid_send, mid_recv)
    ex_dz = exchange(3, dz_send, dz_recv)
    ex_mask = exchange(4, mk_send, mk_recv, True)
    ex_zo = exchange(5, zo_send, zo_recv)
    ex_dm = exchange(6, dm_send, dm_recv)
    ex_db0 = exchange(7, db_send, db_recv)
    near_db1 = to_sibling(8, d1_send.at[1 - core], d1_half)
    ex_db1 = chip_exchange(20, d1_mid, d1_recv)
    near_small = [to_sibling(9 + s, sm_send.at[s], sm_half.at[s]) for s in range(2)]
    ex_small = [chip_exchange(21 + s, sm_mid.at[s], sm_recv.at[s], True) for s in range(2)]
    near_w = [to_sibling(11 + s, w_send.at[s, 1 - core], w_half.at[s]) for s in range(2)]
    ex_w = [chip_exchange(13 + s, w_mid.at[s], w_recv.at[s]) for s in range(2)]
    ex_wf = [chip_exchange(15 + s, w_part.at[s], w_full.at[s, core], True) for s in range(2)]
    near_wf = [to_sibling(17 + s, w_full.at[s, core], w_full.at[s, core]) for s in range(2)]

    barrier = pltpu.get_barrier_semaphore()
    for hop in range(1, group):
        pl.semaphore_signal(barrier, inc=1, device_id={axis: lax.rem(me + hop, group)},
                            device_id_type=pl.DeviceIdType.MESH)

    def zero_diag(i, carry):
        qbd[i] = jnp.zeros((hd, wide), BF16)
        dbd[i] = jnp.zeros((hd, wide), BF16)
        return carry
    lax.fori_loop(0, rows, zero_diag, 0)
    for k in (3, 4, 5, 6, 7, 8, 9):
        loads[k].wait()
    head_pick = (lax.broadcasted_iota(jnp.int32, (16, heads), 0) == lax.broadcasted_iota(jnp.int32, (16, heads), 1)).astype(BF16)
    eye = (lax.broadcasted_iota(jnp.int32, (ch, ch), 0) == lax.broadcasted_iota(jnp.int32, (ch, ch), 1)).astype(BF16)

    def prepare(s):
        wpt[s] = wp_ref[s].T
        wbt[s] = dot(head_pick, wb_ref[s]).astype(BF16)
        for place, ref in enumerate((lns_ref, lnb_ref, bg_ref, bo_ref)):
            col[s, place] = jnp.broadcast_to(ref[s:s + 1, :], (n, ch)).T
    prepare(0)

    def prepare_late():
        prepare(1)
        at16 = lax.broadcasted_iota(jnp.int32, (16, heads * rows), 0)
        at32 = lax.broadcasted_iota(jnp.int32, (16, heads * rows), 1)
        for s in range(2):
            wot[s] = wo_ref[s].T
            w_heads = dot(eye, wbt[s], NT).astype(BF16)
            for i in range(rows):
                wsel[s, i] = dot(w_heads, ((at32 == at16 * rows + i) & (at16 < heads)).astype(BF16)).astype(BF16)

    def column(s, place):
        one = col[s, place]
        return jnp.concatenate([one, one], axis=1)

    def store_diag(ref, t, value):
        for r in range(2):
            for h in range(heads):
                ref[2 * t + r, h * hdim:(h + 1) * hdim, h * n:(h + 1) * n] = value[h * hdim:(h + 1) * hdim, r * n:(r + 1) * n]

    def staged(t):
        return jnp.concatenate([stage[pl.ds(2 * t + r, n, stride=rows), :] for r in range(2)], axis=0)

    def unpack(recv):
        stage[...] = recv[...].astype(F32).reshape(group * rows * rows, ch)

    def pack(send, t, value):
        parts = [value[r * n:(r + 1) * n].reshape(group, n // group, ch) for r in range(2)]
        send[:, pl.ds(pl.multiple_of(t * 16, 16), 16), :] = jnp.concatenate(parts, axis=1).astype(BF16)

    def half(k):
        return pl.ds(k * rows * rows // 2, rows * rows // 2)

    def normalize(s, t, x):
        centred = x - jnp.mean(x, axis=0, keepdims=True)
        inv_std = lax.rsqrt(jnp.mean(centred * centred, axis=0, keepdims=True) + EPS)
        x_hat = centred * inv_std
        return (x_hat * column(s, 0) + column(s, 1)).astype(BF16), x_hat, inv_std

    def keep_norm(s, t, x):
        a_t, x_hat, inv_std = normalize(s, t, x)
        xh[s, t] = x_hat
        inv[s, t] = jnp.broadcast_to(inv_std, (8, two))
        b_t = dot(wbt[s], a_t)
        btmp[pl.ds(pl.multiple_of(t * 32, 32), 32), :] = jnp.concatenate([b_t[:, :n], b_t[:, n:]], axis=0)
        return a_t

    def project(s, t, x, a_t):
        xt[s, t] = x
        a = a_t.T
        a_s[s, t] = a
        p = dot(wpt[s], a_t).astype(BF16)
        qt[s, t] = p[:hd]
        kt[s, t] = p[hd:2 * hd]
        vt[s, t] = p[2 * hd:3 * hd]
        store_diag(qbd, t, p[:hd])
        g = jax.nn.sigmoid(p[3 * hd:].astype(F32) + column(s, 2))
        g_s[s, t] = g
        kv[s, t] = dot(a, wp_ref[s, :, hd:3 * hd]).astype(BF16)
        return g

    def send_bias(s):
        for h in range(0, heads, 2):
            some = [btmp[pl.ds(h + r, rows, stride=16), :] for r in range(2)]
            b_send[s, h * rows:(h + 2) * rows, :] = jnp.concatenate(some, axis=0).astype(BF16)
        (ex_b0, ex_b1)[s].start()

    def take_bias0():
        ex_b0.wait_recv()
        got = b_recv[...].astype(F32).reshape(group, heads, rows, n)
        for h in range(heads):
            bias[:, h * n:(h + 1) * n] = got[:, h].reshape(n, n).T * LOG2E

    def take_bias1():
        near_b1.wait_recv()
        for c in range(2):
            got = b1_recv[c].astype(F32) * LOG2E
            for chip in range(chips):
                for h in range(heads):
                    at = (2 * chip + c) * rows
                    bias[at:at + rows, h * n:(h + 1) * n] = got[chip, h * rows:(h + 1) * rows]

    def logits(s):
        for i in range(rows):
            t, r = divmod(i, 2)
            fill = maskb[s, i]
            raw = dot(kv[s, t, r * n:(r + 1) * n, :hd], qbd[i])
            for h in range(heads):
                pf[s, i, :, h * n:(h + 1) * n] = raw[:, h * n:(h + 1) * n] * (scale * LOG2E) + fill

    def attend(s, some):
        for i in some:
            t, r = divmod(i, 2)
            for h in range(heads):
                cols = slice(h * n, (h + 1) * n)
                x = pf[s, i, :, cols] + bias[:, cols]
                e = jnp.exp2(x - jnp.max(x, axis=0, keepdims=True))
                p = e * (1.0 / jnp.sum(e, axis=0, keepdims=True))
                pf[s, i, :, cols] = p
                hs = slice(h * hdim, (h + 1) * hdim)
                ot[s, t, hs, r * n:(r + 1) * n] = dot(vt[s, t, hs, r * n:(r + 1) * n], p.astype(BF16))

    def block_out(s, t):
        u = (ot[s, t] * g_s[s, t]).astype(BF16)
        ut[s, t] = u
        return xt[s, t] + dot(wot[s], u) + column(s, 3)

    def attend_bwd(s, some):
        def d_probs(i):
            t, r = divmod(i, 2)
            return dot(kv[s, t, r * n:(r + 1) * n, hd:], dbd[i])
        ahead = d_probs(some[0])
        for k, i in enumerate(some):
            t, r = divmod(i, 2)
            d_p = ahead
            if k + 1 < len(some):
                ahead = d_probs(some[k + 1])
            at = slice(r * n, (r + 1) * n)
            for h in range(heads):
                cols = slice(h * n, (h + 1) * n)
                p = pf[s, i, :, cols]
                d_ph = d_p[:, cols]
                d_l = p * (d_ph - jnp.sum(d_ph * p, axis=0, keepdims=True))
                db[:, cols] += d_l
                d_s = (d_l * scale).astype(BF16)
                hs = slice(h * hdim, (h + 1) * hdim)
                d_q = dot(kt[s, t, hs, at], d_s)
                d_k = dot(qt[s, t, hs, at], d_s, NT)
                d_v = dot(dot_s[t, hs, at], p.astype(BF16), NT)
                dpt[t, h * hdim:(h + 1) * hdim, at] = d_q.astype(BF16)
                dpt[t, hd + h * hdim:hd + (h + 1) * hdim, at] = d_k.astype(BF16)
                dpt[t, 2 * hd + h * hdim:2 * hd + (h + 1) * hdim, at] = d_v.astype(BF16)

    def store_d_o(t, d_o):
        dot_s[t] = d_o
        store_diag(dbd, t, d_o)

    def after_attention(s, t, gate_sum):
        g = g_s[s, t]
        d_lin = dgt[t] * ot[s, t] * g * (1.0 - g)
        dpt[t, 3 * hd:, :] = d_lin.astype(BF16)
        return dot(wp_ref[s], dpt[t]), gate_sum + d_lin

    def send_weights(s):
        top = wacc[:4 * hd].reshape(2, chips, 4 * hd // group, ch)
        low = wacc[4 * hd:].reshape(2, chips, hd // group, ch)
        w_send[s] = jnp.concatenate([top, low], axis=2).astype(BF16)
        near_w[s].start()

    def chip_sum_weights(s):
        near_w[s].wait_recv()
        w_mid[s] = (w_send[s, core].astype(F32) + w_half[s].astype(F32)).astype(BF16)
        ex_w[s].start()

    def reduce_weights(s):
        ex_w[s].wait_recv()
        w_part[s] = jnp.sum(w_recv[s].astype(F32), axis=0).astype(BF16)
        ex_wf[s].start()

    def forward_weights(s):
        ex_wf[s].wait_recv()
        near_wf[s].start()

    def send_bias_grad0():
        for h in range(0, heads, 2):
            some = [db[:, (h + r) * n:(h + r + 1) * n].T.reshape(group, rows, n) for r in range(2)]
            db_send[:, h * rows:(h + 2) * rows, :] = jnp.concatenate(some, axis=1).astype(BF16)
        ex_db0.start()

    def send_bias_grad1():
        for h in range(0, heads, 2):
            some = [db[:, (h + r) * n:(h + r + 1) * n].reshape(chips, 2, rows, n) for r in range(2)]
            for c in range(2):
                d1_send[c, :, h * rows:(h + 2) * rows, :] = jnp.concatenate([one[:, c] for one in some], axis=1).astype(BF16)
        near_db1.start()

    def chip_sum_bias_grad1():
        near_db1.wait_recv()
        d1_mid[...] = (d1_send[core].astype(F32) + d1_half[...].astype(F32)).astype(BF16)
        ex_db1.start()

    def take_bias_grad(s):
        (ex_db0, ex_db1)[s].wait_recv()
        got = (db_recv, d1_recv)[s]
        return jnp.sum(got[...].astype(F32), axis=0).astype(BF16)

    def bias_terms(s, d_own):
        return [jnp.concatenate([dot(wsel[s, 2 * t + r], d_own) for r in range(2)], axis=1) for t in range(pairs)]

    def head_weight_grad(s, d_own):
        at16 = lax.broadcasted_iota(jnp.int32, (16, heads * rows), 0)
        at32 = lax.broadcasted_iota(jnp.int32, (16, heads * rows), 1)
        for t in range(pairs):
            rows_of = [dot((at32 == at16 * rows + (2 * t + r)).astype(BF16), d_own) for r in range(2)]
            dbt[t] = jnp.concatenate(rows_of, axis=1).astype(BF16)
        total = None
        for t in range(pairs):
            one = dot(dbt[t], a_s[0, t]) if s == 0 else dot(dbt[t], at1[t], NT)
            total = one if total is None else total + one
        return total

    def norm_bwd(s, t, d_n, sums):
        x_hat = xh[s, t]
        d_hat = d_n * column(s, 0)
        along = jnp.mean(d_hat * x_hat, axis=0, keepdims=True)
        d_in = inv[s, t, 0:1, :] * (d_hat - jnp.mean(d_hat, axis=0, keepdims=True) - x_hat * along)
        return d_in, (sums[0] + d_n * x_hat, sums[1] + d_n)

    def lanes_to_row(value):
        return jnp.sum((value[:, :n] + value[:, n:]).T, axis=0, keepdims=True)

    def send_small(s, sums, wb_sum, gate_sum, b_out_row):
        gain_sum, shift_sum = sums
        sm_send[s, 0:1, :] = lanes_to_row(gain_sum)
        sm_send[s, 1:2, :] = lanes_to_row(shift_sum)
        sm_send[s, 2:3, :] = lanes_to_row(gate_sum)
        sm_send[s, 3:4, :] = b_out_row
        sm_send[s, 4:4 + heads, :] = wb_sum[:heads]
        near_small[s].start()

    def chip_sum_small(s):
        near_small[s].wait_recv()
        sm_mid[s] = sm_send[s] + sm_half[s]
        ex_small[s].start()

    zero_tile = jnp.zeros((ch, two), F32)
    early, late = range(pairs // 2), range(pairs // 2, pairs)

    loads[0].wait()
    for t in range(pairs):
        x = jnp.concatenate([z_ref[2 * t + r].astype(F32).T for r in range(2)], axis=1)
        project(0, t, x, keep_norm(0, t, x))
    pl.semaphore_wait(barrier, group - 1)
    send_bias(0)
    loads[1].wait()
    fill_rows = (mask_ref[...].astype(F32) - 1.0) * (MASK_FILL * LOG2E)
    for i in range(rows):
        maskb[0, i] = jnp.broadcast_to(fill_rows[i:i + 1, :], (n, n)).T
    logits(0)
    loads[2].wait()
    b_out_row1 = jnp.zeros((1, ch), F32)
    for t in range(pairs):
        d_y = jnp.concatenate([dz_ref[2 * t + r].astype(F32) for r in range(2)], axis=0)
        pack(dz_send, t, d_y)
        dzt[t] = d_y.T
        b_out_row1 = b_out_row1 + jnp.sum(d_y, axis=0, keepdims=True)
    mk_send[...] = mask_ref[...].astype(F32).astype(BF16)
    ex_dz.start(half(0))
    ex_mask.start()
    prepare_late()
    take_bias0()

    for k, some in enumerate((early, late)):
        attend(0, range(2 * some[0], 2 * some[-1] + 2))
        for t in some:
            y = block_out(0, t)
            pack(mid_send, t, y.T)
            xt[1, t] = y.astype(BF16).astype(F32)
        ex_mid.start(half(k))
    for t in range(pairs):
        at1[t] = keep_norm(1, t, xt[1, t])
    send_bias(1)
    ex_dz.start(half(1))

    db[...] = jnp.zeros((n, wide), F32)
    ex_mask.wait_recv()
    whole = mk_recv[...].astype(F32).reshape(n, n).astype(BF16)
    for i in range(rows):
        pick = (lax.broadcasted_iota(jnp.int32, (n, n), 0) == me * rows + i).astype(BF16)
        maskb[1, i] = (dot(whole, pick) - 1.0) * (MASK_FILL * LOG2E)

    ex_mid.wait_recv()
    unpack(mid_recv)
    for t in range(pairs):
        x = staged(t).T
        project(1, t, x, normalize(1, t, x)[0])
    ex_b1.wait_recv()
    near_b1.start()
    logits(1)
    take_bias1()
    attend(1, range(rows // 2))
    for t in early:
        pack(zo_send, t, block_out(1, t).T)
    ex_zo.start(half(0))
    attend(1, range(rows // 2, rows))
    ex_dz.wait_recv()
    unpack(dz_recv)
    for t in range(pairs):
        d_low = staged(t).astype(BF16)
        dlp[t] = d_low
        dgt[t] = dot(wo_ref[1], d_low, NT)
    for t in range(pairs):
        store_d_o(t, (dgt[t] * g_s[1, t]).astype(BF16))

    gate_sum1 = zero_tile
    for k, some in enumerate((early, late)):
        attend_bwd(1, range(2 * some[0], 2 * some[-1] + 2))
        if k == 1:
            send_bias_grad1()
        for t in some:
            d_n, gate_sum1 = after_attention(1, t, gate_sum1)
            pack(dm_send, t, d_n.T)
        ex_dm.start(half(k))
    for t in late:
        pack(zo_send, t, block_out(1, t).T)
    chip_sum_bias_grad1()

    def sum_weights(s):
        top, low = None, None
        for t in range(pairs):
            one = dot(dpt[t], a_s[s, t])
            two_ = dot(ut[1, t], dlp[t]) if s == 1 else dot(ut[0, t], dlt[t], NT)
            top, low = (one, two_) if top is None else (top + one, low + two_)
        wacc[:4 * hd] = top
        wacc[4 * hd:] = low
    sum_weights(1)
    send_weights(1)
    db[...] = jnp.zeros((n, wide), F32)

    d_own1 = take_bias_grad(1)
    terms = bias_terms(1, d_own1)
    for t in range(pairs):
        dnt[t] = terms[t]
    ex_dm.wait_recv()
    chip_sum_weights(1)
    unpack(dm_recv)
    sums1, b_out_sum = (zero_tile, zero_tile), zero_tile
    for t in range(pairs):
        d_in, sums1 = norm_bwd(1, t, staged(t).T + dnt[t], sums1)
        d_y = d_in + dzt[t]
        dmt[t] = d_y
        d_low = d_y.astype(BF16)
        dlt[t] = d_low
        d_gated = dot(wo_ref[0], d_low)
        dgt[t] = d_gated
        store_d_o(t, (d_gated * g_s[0, t]).astype(BF16))
        b_out_sum = b_out_sum + d_y

    attend_bwd(0, range(rows))
    send_bias_grad0()
    gate_sum0 = zero_tile
    for t in range(pairs):
        dnt[t], gate_sum0 = after_attention(0, t, gate_sum0)
    sum_weights(0)
    send_weights(0)
    send_small(1, sums1, head_weight_grad(1, d_own1), gate_sum1, b_out_row1)
    b_out_row0 = lanes_to_row(b_out_sum)
    chip_sum_weights(0)
    ex_zo.start(half(1))
    chip_sum_small(1)
    reduce_weights(1)

    d_own0 = take_bias_grad(0)
    terms = bias_terms(0, d_own0)
    sums0 = (zero_tile, zero_tile)
    for t in range(pairs):
        d_in, sums0 = norm_bwd(0, t, dnt[t] + terms[t], sums0)
        d_x = (d_in + dmt[t]).T.astype(BF16)
        for r in range(2):
            zg_out[2 * t + r] = d_x[r * n:(r + 1) * n]
    send_small(0, sums0, head_weight_grad(0, d_own0), gate_sum0, b_out_row0)
    chip_sum_small(0)
    reduce_weights(0)
    forward_weights(1)
    forward_weights(0)

    for one in [ex_zo] + ex_small + near_wf:
        one.wait_recv()
    for one in [ex_b0, ex_b1, near_b1, ex_mid, ex_dz, ex_mask, ex_zo, ex_dm, ex_db0, near_db1, ex_db1] + near_small + ex_small + near_w + ex_w + ex_wf + near_wf:
        one.wait_send()


def finish(dims, zo_ref, zg_ref, w_ref, sm_ref,
           zo_out, zg_out, lns_out, lnb_out, wp_out, wb_out, bg_out, wo_out, bo_out, stage):
    rows, n, ch, heads, hd, group = dims
    zg_out[...] = zg_ref[...]
    stage[...] = zo_ref[...].astype(F32).reshape(group * rows * rows, ch)
    for i in range(rows):
        zo_out[i] = stage[pl.ds(i, n, stride=rows), :].astype(BF16)
    cut = 4 * hd // group
    for s in range(2):
        full = w_ref[s].astype(F32).reshape(group, 5 * hd // group, ch)
        wp_out[s] = full[:, :cut].reshape(4 * hd, ch).T
        wo_out[s] = full[:, cut:].reshape(hd, ch)
        total = jnp.sum(sm_ref[s], axis=0)
        for place, ref in enumerate((lns_out, lnb_out, bg_out, bo_out)):
            ref[s:s + 1, :] = total[place:place + 1, :]
        wb_out[s] = total[4:4 + heads]


def solution(mesh):
    axis = 'dap'
    group = mesh.shape[axis]
    row_spec = P(('dp', axis), None, None)
    mask_spec = P(('dp', axis), None)
    grad_spec = P('dp')

    def per_device(z, pair_mask, dz_out, ln_scale, ln_shift, w_proj, w_bias, b_gate, w_out, b_out):
        rows, n, ch = z.shape
        heads = w_bias.shape[-1]
        hd = b_gate.shape[-1]
        pairs, two, wide = rows // 2, 2 * n, heads * n
        piece = (group, rows * rows, ch)
        w_rows = 5 * hd // group

        def vmem(shape, dtype):
            return pltpu.VMEM(shape, dtype)

        w_heads = jnp.swapaxes(w_bias, 1, 2)
        like = [z, z, ln_scale, ln_shift, w_proj, w_heads, b_gate, w_out, b_out]
        out_shape = [jax.ShapeDtypeStruct(a.shape, BF16 if k < 2 else F32) for k, a in enumerate(like)]
        chips = group // 2
        mid_shape = [jax.ShapeDtypeStruct(piece, BF16), jax.ShapeDtypeStruct(z.shape, BF16),
                     jax.ShapeDtypeStruct((2, 2, chips, w_rows, ch), BF16), jax.ShapeDtypeStruct((2, chips, 8, ch), F32)]
        tile = (pairs, ch, two)
        scratch = [
            vmem((2, 4 * hd, ch), BF16), vmem((2, ch, hd), BF16), vmem((2, 16, ch), BF16), vmem((2, 4, ch, n), F32),
            vmem((2,) + tile, F32), vmem((2,) + tile, F32), vmem((2, pairs, 8, two), F32), vmem((2, pairs, two, ch), BF16), vmem(tile, BF16),
            vmem((2, pairs, hd, two), BF16), vmem((2, pairs, hd, two), BF16), vmem((2, pairs, hd, two), BF16), vmem((2, pairs, two, 2 * hd), BF16),
            vmem((2, pairs, hd, two), F32), vmem((2, pairs, hd, two), F32), vmem((2, pairs, hd, two), BF16), vmem((rows * 16, n), F32),
            vmem((rows, hd, wide), BF16), vmem((rows, hd, wide), BF16), vmem((pairs, hd, two), BF16), vmem((pairs, hd, two), F32),
            vmem((pairs, 4 * hd, two), BF16), vmem(tile, F32), vmem(tile, F32), vmem(tile, F32), vmem((pairs, two, ch), BF16), vmem(tile, BF16),
            vmem((2, rows, n, wide), F32), vmem((n, wide), F32), vmem((n, wide), F32),
            vmem((2, rows, n, n), F32), vmem((group * rows * rows, ch), F32),
            vmem((5 * hd, ch), F32), vmem((2, rows, ch, heads * rows), BF16), vmem((pairs, 16, two), BF16),
            vmem((2, heads * rows, n), BF16), vmem((group, heads * rows, n), BF16), vmem((2, chips, heads * rows, n), BF16), vmem(piece, BF16), vmem(piece, BF16), vmem(piece, BF16), vmem(piece, BF16),
            vmem((rows, n), BF16), vmem((group, rows, n), BF16), vmem(piece, BF16), vmem(piece, BF16), vmem(piece, BF16),
            vmem((group, heads * rows, n), BF16), vmem((group, heads * rows, n), BF16),
            vmem((2, chips, heads * rows, n), BF16), vmem((chips, heads * rows, n), BF16), vmem((chips, heads * rows, n), BF16), vmem((chips, heads * rows, n), BF16),
            vmem((2, 2, chips, w_rows, ch), BF16), vmem((2, chips, w_rows, ch), BF16), vmem((2, chips, w_rows, ch), BF16), vmem((2, chips, w_rows, ch), BF16),
            vmem((2, w_rows, ch), BF16), vmem((2, 8, ch), F32), vmem((2, 8, ch), F32), vmem((2, 8, ch), F32),
            pltpu.SemaphoreType.DMA((23,)), pltpu.SemaphoreType.DMA((23,)),
        ]
        operands = (z, pair_mask, dz_out, ln_scale, ln_shift, w_proj, w_heads, b_gate, w_out, b_out)
        scratch += [vmem(a.shape, a.dtype) for a in operands] + [pltpu.SemaphoreType.DMA((10,))]
        in_vmem = pl.BlockSpec(memory_space=pltpu.VMEM)
        mid = pl.pallas_call(
            functools.partial(kernel, (rows, n, ch, heads, hd, group, axis)),
            out_shape=mid_shape,
            in_specs=[pl.BlockSpec(memory_space=pltpu.HBM)] * 10,
            out_specs=[in_vmem] * 4,
            scratch_shapes=scratch,
            compiler_params=pltpu.CompilerParams(collective_id=0, has_side_effects=True, vmem_limit_bytes=40 * 1024 * 1024),
        )(*[pltpu.with_memory_space_constraint(a, pltpu.HBM) for a in operands])
        out = pl.pallas_call(
            functools.partial(finish, (rows, n, ch, heads, hd, group)),
            out_shape=out_shape,
            in_specs=[in_vmem] * 4,
            out_specs=[in_vmem] * 9,
            scratch_shapes=[vmem((group * rows * rows, ch), F32)],
            compiler_params=pltpu.CompilerParams(vmem_limit_bytes=16 * 1024 * 1024),
        )(*mid)
        return tuple(out[:5]) + (jnp.swapaxes(out[5], 1, 2),) + tuple(out[6:])

    return jax.shard_map(per_device, mesh=mesh, in_specs=(row_spec, mask_spec, row_spec) + (P(),) * 7,
                         out_specs=(row_spec, row_spec) + (grad_spec,) * 7, check_vma=False)
```

```python
import functools

import jax
import jax.numpy as jnp
from jax import lax
from jax.experimental import pallas as pl
from jax.experimental.pallas import tpu as pltpu
from jax.sharding import PartitionSpec as P

EPS = 1e-5
MASK_FILL = 1e9
LOG2E = 1.4426950408889634
F32 = jnp.float32
BF16 = jnp.bfloat16
NN = (((1,), (0,)), ((), ()))
NT = (((1,), (1,)), ((), ()))


def dot(a, b, dims=NN):
    return lax.dot_general(a, b, dims, preferred_element_type=F32)


class Exchange:
    def __init__(self, group, axis, send, recv, send_sem, recv_sem, same=False):
        self.group, self.axis, self.send, self.recv = group, axis, send, recv
        self.send_sem, self.recv_sem, self.same = send_sem, recv_sem, same

    def start(self, part=None):
        me = lax.axis_index(self.axis)
        half = self.group // 2
        order = [half]
        for hop in range(half - 1, 0, -1):
            order += [hop, self.group - hop]
        for hop in order:
            peer = lax.rem(me + hop, self.group)
            source = self.send if self.same else self.send.at[peer] if part is None else self.send.at[peer, part]
            pltpu.make_async_remote_copy(
                src_ref=source,
                dst_ref=self.recv.at[me] if part is None else self.recv.at[me, part],
                send_sem=self.send_sem,
                recv_sem=self.recv_sem,
                device_id={self.axis: peer},
                device_id_type=pl.DeviceIdType.MESH,
            ).start()
        if part is None:
            self.recv[me] = self.send[...] if self.same else self.send[me]
        else:
            self.recv[me, part] = self.send[me, part]

    def _all(self):
        some = self.recv.at[pl.ds(0, self.group - 1)]
        return pltpu.make_async_remote_copy(
            src_ref=some,
            dst_ref=some,
            send_sem=self.send_sem,
            recv_sem=self.recv_sem,
            device_id={self.axis: lax.axis_index(self.axis)},
            device_id_type=pl.DeviceIdType.MESH,
        )

    def wait_recv(self):
        self._all().wait_recv()

    def wait_send(self):
        self._all().wait_send()


class ChipExchange:
    def __init__(self, chips, axis, send, recv, send_sem, recv_sem, same=False):
        self.chips, self.axis, self.send, self.recv = chips, axis, send, recv
        self.send_sem, self.recv_sem, self.same = send_sem, recv_sem, same

    def start(self):
        me = lax.axis_index(self.axis)
        chip, core = me // 2, me % 2
        order = [self.chips // 2]
        for hop in range(self.chips // 2 - 1, 0, -1):
            order += [hop, self.chips - hop]
        for hop in order:
            to = lax.rem(chip + hop, self.chips)
            pltpu.make_async_remote_copy(
                src_ref=self.send if self.same else self.send.at[to],
                dst_ref=self.recv.at[chip],
                send_sem=self.send_sem,
                recv_sem=self.recv_sem,
                device_id={self.axis: 2 * to + core},
                device_id_type=pl.DeviceIdType.MESH,
            ).start()
        self.recv[chip] = self.send[...] if self.same else self.send[chip]

    def _all(self):
        some = self.recv.at[pl.ds(0, self.chips - 1)]
        return pltpu.make_async_remote_copy(
            src_ref=some,
            dst_ref=some,
            send_sem=self.send_sem,
            recv_sem=self.recv_sem,
            device_id={self.axis: lax.axis_index(self.axis)},
            device_id_type=pl.DeviceIdType.MESH,
        )

    def wait_recv(self):
        self._all().wait_recv()

    def wait_send(self):
        self._all().wait_send()


def kernel(dims, *refs):
    rows, n, ch, heads, hd, group, axis = dims
    hdim = hd // heads
    scale = hdim ** -0.5
    pairs = rows // 2
    two = 2 * n
    wide = heads * n
    chips = group // 2
    operands = refs[:10]
    local = refs[-11:-1]
    (z_ref, mask_ref, dz_ref, lns_ref, lnb_ref, wp_ref, wb_ref, bg_ref, wo_ref, bo_ref) = local
    load_sems, refs = refs[-1], refs[10:-11]
    (zo_recv, zg_out, w_full, sm_recv,
     wpt, wot, wbt, col,
     xt, xh, inv, a_s, at1, qt, kt, vt, kv, g_s, ot, ut, btmp, qbd, dbd, dot_s, dgt, dpt, dnt, dzt, dmt, dlp, dlt, pf, bias, db, maskb, stage,
     wacc, wsel, dbt,
     b_send, b_recv, b1_recv, mid_send, mid_recv, dz_send, dz_recv, mk_send, mk_recv, zo_send, dm_send, dm_recv,
     db_send, db_recv, d1_send, d1_half, d1_mid, d1_recv, w_send, w_half, w_mid, w_recv, w_part, sm_send, sm_half, sm_mid,
     send_sems, recv_sems) = refs
    me = lax.axis_index(axis)
    core = me % 2
    loads = [pltpu.make_async_copy(src, dst, load_sems.at[k]) for k, (src, dst) in enumerate(zip(operands, local))]
    for one in loads:
        one.start()

    def exchange(slot, send, recv, same=False):
        return Exchange(group, axis, send, recv, send_sems.at[slot], recv_sems.at[slot], same)

    def chip_exchange(slot, send, recv, same=False):
        return ChipExchange(chips, axis, send, recv, send_sems.at[slot], recv_sems.at[slot], same)

    def to_sibling(slot, send, recv):
        return pltpu.make_async_remote_copy(src_ref=send, dst_ref=recv, send_sem=send_sems.at[slot], recv_sem=recv_sems.at[slot],
                                            device_id={axis: me + 1 - 2 * core}, device_id_type=pl.DeviceIdType.MESH)

    ex_b0 = exchange(0, b_send.at[0], b_recv, True)
    ex_b1 = chip_exchange(1, b_send.at[1], b1_recv.at[core], True)
    near_b1 = to_sibling(19, b1_recv.at[core], b1_recv.at[core])
    ex_mid = exchange(2, mid_send, mid_recv)
    ex_dz = exchange(3, dz_send, dz_recv)
    ex_mask = exchange(4, mk_send, mk_recv, True)
    ex_zo = exchange(5, zo_send, zo_recv)
    ex_dm = exchange(6, dm_send, dm_recv)
    ex_db0 = exchange(7, db_send, db_recv)
    near_db1 = to_sibling(8, d1_send.at[1 - core], d1_half)
    ex_db1 = chip_exchange(20, d1_mid, d1_recv)
    near_small = [to_sibling(9 + s, sm_send.at[s], sm_half.at[s]) for s in range(2)]
    ex_small = [chip_exchange(21 + s, sm_mid.at[s], sm_recv.at[s], True) for s in range(2)]
    near_w = [to_sibling(11 + s, w_send.at[s, 1 - core], w_half.at[s]) for s in range(2)]
    ex_w = [chip_exchange(13 + s, w_mid.at[s], w_recv.at[s]) for s in range(2)]
    ex_wf = [chip_exchange(15 + s, w_part.at[s], w_full.at[s, core], True) for s in range(2)]
    near_wf = [to_sibling(17 + s, w_full.at[s, core], w_full.at[s, core]) for s in range(2)]

    barrier = pltpu.get_barrier_semaphore()
    for hop in range(1, group):
        pl.semaphore_signal(barrier, inc=1, device_id={axis: lax.rem(me + hop, group)},
                            device_id_type=pl.DeviceIdType.MESH)

    def zero_diag(i, carry):
        qbd[i] = jnp.zeros((hd, wide), BF16)
        dbd[i] = jnp.zeros((hd, wide), BF16)
        return carry
    lax.fori_loop(0, rows, zero_diag, 0)
    for k in (3, 4, 5, 6, 7, 8, 9):
        loads[k].wait()
    head_pick = (lax.broadcasted_iota(jnp.int32, (16, heads), 0) == lax.broadcasted_iota(jnp.int32, (16, heads), 1)).astype(BF16)
    eye = (lax.broadcasted_iota(jnp.int32, (ch, ch), 0) == lax.broadcasted_iota(jnp.int32, (ch, ch), 1)).astype(BF16)

    def prepare(s):
        wpt[s] = wp_ref[s].T
        wbt[s] = dot(head_pick, wb_ref[s]).astype(BF16)
        for place, ref in enumerate((lns_ref, lnb_ref, bg_ref, bo_ref)):
            col[s, place] = jnp.broadcast_to(ref[s:s + 1, :], (n, ch)).T
    prepare(0)

    def prepare_late():
        prepare(1)
        at16 = lax.broadcasted_iota(jnp.int32, (16, heads * rows), 0)
        at32 = lax.broadcasted_iota(jnp.int32, (16, heads * rows), 1)
        for s in range(2):
            wot[s] = wo_ref[s].T
            w_heads = dot(eye, wbt[s], NT).astype(BF16)
            for i in range(rows):
                wsel[s, i] = dot(w_heads, ((at32 == at16 * rows + i) & (at16 < heads)).astype(BF16)).astype(BF16)

    def column(s, place):
        one = col[s, place]
        return jnp.concatenate([one, one], axis=1)

    def store_diag(ref, t, value):
        for r in range(2):
            for h in range(heads):
                ref[2 * t + r, h * hdim:(h + 1) * hdim, h * n:(h + 1) * n] = value[h * hdim:(h + 1) * hdim, r * n:(r + 1) * n]

    def staged(t):
        return jnp.concatenate([stage[pl.ds(2 * t + r, n, stride=rows), :] for r in range(2)], axis=0)

    def unpack(recv):
        stage[...] = recv[...].astype(F32).reshape(group * rows * rows, ch)

    def pack(send, t, value):
        parts = [value[r * n:(r + 1) * n].reshape(group, n // group, ch) for r in range(2)]
        send[:, pl.ds(pl.multiple_of(t * 16, 16), 16), :] = jnp.concatenate(parts, axis=1).astype(BF16)

    def half(k):
        return pl.ds(k * rows * rows // 2, rows * rows // 2)

    def normalize(s, t, x):
        centred = x - jnp.mean(x, axis=0, keepdims=True)
        inv_std = lax.rsqrt(jnp.mean(centred * centred, axis=0, keepdims=True) + EPS)
        x_hat = centred * inv_std
        return (x_hat * column(s, 0) + column(s, 1)).astype(BF16), x_hat, inv_std

    def keep_norm(s, t, x):
        a_t, x_hat, inv_std = normalize(s, t, x)
        xh[s, t] = x_hat
        inv[s, t] = jnp.broadcast_to(inv_std, (8, two))
        b_t = dot(wbt[s], a_t)
        btmp[pl.ds(pl.multiple_of(t * 32, 32), 32), :] = jnp.concatenate([b_t[:, :n], b_t[:, n:]], axis=0)
        return a_t

    def project(s, t, x, a_t):
        xt[s, t] = x
        a = a_t.T
        a_s[s, t] = a
        p = dot(wpt[s], a_t).astype(BF16)
        qt[s, t] = p[:hd]
        kt[s, t] = p[hd:2 * hd]
        vt[s, t] = p[2 * hd:3 * hd]
        store_diag(qbd, t, p[:hd])
        g = jax.nn.sigmoid(p[3 * hd:].astype(F32) + column(s, 2))
        g_s[s, t] = g
        kv[s, t] = dot(a, wp_ref[s, :, hd:3 * hd]).astype(BF16)
        return g

    def send_bias(s):
        for h in range(0, heads, 2):
            some = [btmp[pl.ds(h + r, rows, stride=16), :] for r in range(2)]
            b_send[s, h * rows:(h + 2) * rows, :] = jnp.concatenate(some, axis=0).astype(BF16)
        (ex_b0, ex_b1)[s].start()

    def take_bias0():
        ex_b0.wait_recv()
        got = b_recv[...].astype(F32).reshape(group, heads, rows, n)
        for h in range(heads):
            bias[:, h * n:(h + 1) * n] = got[:, h].reshape(n, n).T * LOG2E

    def take_bias1():
        near_b1.wait_recv()
        for c in range(2):
            got = b1_recv[c].astype(F32) * LOG2E
            for chip in range(chips):
                for h in range(heads):
                    at = (2 * chip + c) * rows
                    bias[at:at + rows, h * n:(h + 1) * n] = got[chip, h * rows:(h + 1) * rows]

    def logits(s):
        for i in range(rows):
            t, r = divmod(i, 2)
            fill = maskb[s, i]
            raw = dot(kv[s, t, r * n:(r + 1) * n, :hd], qbd[i])
            for h in range(heads):
                pf[s, i, :, h * n:(h + 1) * n] = raw[:, h * n:(h + 1) * n] * (scale * LOG2E) + fill

    def attend(s, some):
        for i in some:
            t, r = divmod(i, 2)
            for h in range(heads):
                cols = slice(h * n, (h + 1) * n)
                x = pf[s, i, :, cols] + bias[:, cols]
                e = jnp.exp2(x - jnp.max(x, axis=0, keepdims=True))
                p = e * (1.0 / jnp.sum(e, axis=0, keepdims=True))
                pf[s, i, :, cols] = p
                hs = slice(h * hdim, (h + 1) * hdim)
                ot[s, t, hs, r * n:(r + 1) * n] = dot(vt[s, t, hs, r * n:(r + 1) * n], p.astype(BF16))

    def block_out(s, t):
        u = (ot[s, t] * g_s[s, t]).astype(BF16)
        ut[s, t] = u
        return xt[s, t] + dot(wot[s], u) + column(s, 3)

    def attend_bwd(s, some):
        def d_probs(i):
            t, r = divmod(i, 2)
            return dot(kv[s, t, r * n:(r + 1) * n, hd:], dbd[i])
        ahead = d_probs(some[0])
        for k, i in enumerate(some):
            t, r = divmod(i, 2)
            d_p = ahead
            if k + 1 < len(some):
                ahead = d_probs(some[k + 1])
            at = slice(r * n, (r + 1) * n)
            for h in range(heads):
                cols = slice(h * n, (h + 1) * n)
                p = pf[s, i, :, cols]
                d_ph = d_p[:, cols]
                d_l = p * (d_ph - jnp.sum(d_ph * p, axis=0, keepdims=True))
                db[:, cols] += d_l
                d_s = (d_l * scale).astype(BF16)
                hs = slice(h * hdim, (h + 1) * hdim)
                d_q = dot(kt[s, t, hs, at], d_s)
                d_k = dot(qt[s, t, hs, at], d_s, NT)
                d_v = dot(dot_s[t, hs, at], p.astype(BF16), NT)
                dpt[t, h * hdim:(h + 1) * hdim, at] = d_q.astype(BF16)
                dpt[t, hd + h * hdim:hd + (h + 1) * hdim, at] = d_k.astype(BF16)
                dpt[t, 2 * hd + h * hdim:2 * hd + (h + 1) * hdim, at] = d_v.astype(BF16)

    def store_d_o(t, d_o):
        dot_s[t] = d_o
        store_diag(dbd, t, d_o)

    def gate_grad(s, t, gate_sum):
        g = g_s[s, t]
        d_lin = dgt[t] * ot[s, t] * g * (1.0 - g)
        dpt[t, 3 * hd:, :] = d_lin.astype(BF16)
        return gate_sum + d_lin

    def send_weights(s):
        top = wacc[:4 * hd].reshape(2, chips, 4 * hd // group, ch)
        low = wacc[4 * hd:].reshape(2, chips, hd // group, ch)
        w_send[s] = jnp.concatenate([top, low], axis=2).astype(BF16)
        near_w[s].start()

    def chip_sum_weights(s):
        near_w[s].wait_recv()
        w_mid[s] = (w_send[s, core].astype(F32) + w_half[s].astype(F32)).astype(BF16)
        ex_w[s].start()

    def reduce_weights(s):
        ex_w[s].wait_recv()
        w_part[s] = jnp.sum(w_recv[s].astype(F32), axis=0).astype(BF16)
        ex_wf[s].start()

    def forward_weights(s):
        ex_wf[s].wait_recv()
        near_wf[s].start()

    def send_bias_grad0():
        for h in range(0, heads, 2):
            some = [db[:, (h + r) * n:(h + r + 1) * n].T.reshape(group, rows, n) for r in range(2)]
            db_send[:, h * rows:(h + 2) * rows, :] = jnp.concatenate(some, axis=1).astype(BF16)
        ex_db0.start()

    def send_bias_grad1():
        for h in range(0, heads, 2):
            some = [db[:, (h + r) * n:(h + r + 1) * n].reshape(chips, 2, rows, n) for r in range(2)]
            for c in range(2):
                d1_send[c, :, h * rows:(h + 2) * rows, :] = jnp.concatenate([one[:, c] for one in some], axis=1).astype(BF16)
        near_db1.start()

    def chip_sum_bias_grad1():
        near_db1.wait_recv()
        d1_mid[...] = (d1_send[core].astype(F32) + d1_half[...].astype(F32)).astype(BF16)
        ex_db1.start()

    def take_bias_grad(s):
        (ex_db0, ex_db1)[s].wait_recv()
        got = (db_recv, d1_recv)[s]
        return jnp.sum(got[...].astype(F32), axis=0).astype(BF16)

    def bias_terms(s, d_own):
        return [jnp.concatenate([dot(wsel[s, 2 * t + r], d_own) for r in range(2)], axis=1) for t in range(pairs)]

    def head_weight_grad(s, d_own):
        at16 = lax.broadcasted_iota(jnp.int32, (16, heads * rows), 0)
        at32 = lax.broadcasted_iota(jnp.int32, (16, heads * rows), 1)
        for t in range(pairs):
            rows_of = [dot((at32 == at16 * rows + (2 * t + r)).astype(BF16), d_own) for r in range(2)]
            dbt[t] = jnp.concatenate(rows_of, axis=1).astype(BF16)
        total = None
        for t in range(pairs):
            one = dot(dbt[t], a_s[0, t]) if s == 0 else dot(dbt[t], at1[t], NT)
            total = one if total is None else total + one
        return total

    def norm_bwd(s, t, d_n, sums):
        x_hat = xh[s, t]
        d_hat = d_n * column(s, 0)
        along = jnp.mean(d_hat * x_hat, axis=0, keepdims=True)
        d_in = inv[s, t, 0:1, :] * (d_hat - jnp.mean(d_hat, axis=0, keepdims=True) - x_hat * along)
        return d_in, (sums[0] + d_n * x_hat, sums[1] + d_n)

    def lanes_to_row(value):
        return jnp.sum((value[:, :n] + value[:, n:]).T, axis=0, keepdims=True)

    def send_small(s, sums, wb_sum, gate_sum, b_out_row):
        gain_sum, shift_sum = sums
        sm_send[s, 0:1, :] = lanes_to_row(gain_sum)
        sm_send[s, 1:2, :] = lanes_to_row(shift_sum)
        sm_send[s, 2:3, :] = lanes_to_row(gate_sum)
        sm_send[s, 3:4, :] = b_out_row
        sm_send[s, 4:4 + heads, :] = wb_sum[:heads]
        near_small[s].start()

    def chip_sum_small(s):
        near_small[s].wait_recv()
        sm_mid[s] = sm_send[s] + sm_half[s]
        ex_small[s].start()

    zero_tile = jnp.zeros((ch, two), F32)
    early, late = range(pairs // 2), range(pairs // 2, pairs)

    loads[0].wait()
    for t in range(pairs):
        x = jnp.concatenate([z_ref[2 * t + r].astype(F32).T for r in range(2)], axis=1)
        project(0, t, x, keep_norm(0, t, x))
    pl.semaphore_wait(barrier, group - 1)
    send_bias(0)
    loads[1].wait()
    fill_rows = (mask_ref[...].astype(F32) - 1.0) * (MASK_FILL * LOG2E)
    for i in range(rows):
        maskb[0, i] = jnp.broadcast_to(fill_rows[i:i + 1, :], (n, n)).T
    logits(0)
    loads[2].wait()
    b_out_row1 = jnp.zeros((1, ch), F32)
    for t in range(pairs):
        d_y = jnp.concatenate([dz_ref[2 * t + r].astype(F32) for r in range(2)], axis=0)
        pack(dz_send, t, d_y)
        dzt[t] = d_y.T
        b_out_row1 = b_out_row1 + jnp.sum(d_y, axis=0, keepdims=True)
    mk_send[...] = mask_ref[...].astype(F32).astype(BF16)
    prepare_late()
    ex_dz.start(half(0))
    ex_mask.start()
    take_bias0()

    for k, some in enumerate((early, late)):
        attend(0, range(2 * some[0], 2 * some[-1] + 2))
        for t in some:
            y = block_out(0, t)
            pack(mid_send, t, y.T)
            xt[1, t] = y.astype(BF16).astype(F32)
        ex_mid.start(half(k))
    for t in range(pairs):
        at1[t] = keep_norm(1, t, xt[1, t])
    send_bias(1)
    ex_dz.start(half(1))

    db[...] = jnp.zeros((n, wide), F32)
    ex_mask.wait_recv()
    whole = mk_recv[...].astype(F32).reshape(n, n).astype(BF16)
    for i in range(rows):
        pick = (lax.broadcasted_iota(jnp.int32, (n, n), 0) == me * rows + i).astype(BF16)
        maskb[1, i] = (dot(whole, pick) - 1.0) * (MASK_FILL * LOG2E)

    ex_mid.wait_recv()
    unpack(mid_recv)
    for t in range(pairs):
        x = staged(t).T
        project(1, t, x, normalize(1, t, x)[0])
    ex_b1.wait_recv()
    near_b1.start()
    logits(1)
    take_bias1()
    attend(1, range(rows // 2))
    for t in early:
        pack(zo_send, t, block_out(1, t).T)
    ex_zo.start(half(0))
    attend(1, range(rows // 2, rows))
    ex_dz.wait_recv()
    unpack(dz_recv)
    for t in range(pairs):
        d_low = staged(t).astype(BF16)
        dlp[t] = d_low
        dgt[t] = dot(wo_ref[1], d_low, NT)
    for t in range(pairs):
        store_d_o(t, (dgt[t] * g_s[1, t]).astype(BF16))

    gate_sum1 = zero_tile
    for k, some in enumerate((early, late)):
        attend_bwd(1, range(2 * some[0], 2 * some[-1] + 2))
        if k == 1:
            send_bias_grad1()
        for t in some:
            gate_sum1 = gate_grad(1, t, gate_sum1)
            pack(dm_send, t, dot(wp_ref[1], dpt[t]).T)
        ex_dm.start(half(k))
    for t in late:
        pack(zo_send, t, block_out(1, t).T)
    chip_sum_bias_grad1()

    def sum_weights(s):
        top, low = None, None
        for t in range(pairs):
            one = dot(dpt[t], a_s[s, t])
            two_ = dot(ut[1, t], dlp[t]) if s == 1 else dot(ut[0, t], dlt[t], NT)
            top, low = (one, two_) if top is None else (top + one, low + two_)
        wacc[:4 * hd] = top
        wacc[4 * hd:] = low
    sum_weights(1)
    send_weights(1)
    db[...] = jnp.zeros((n, wide), F32)
    chip_sum_weights(1)

    d_own1 = take_bias_grad(1)
    terms = bias_terms(1, d_own1)
    for t in range(pairs):
        dnt[t] = terms[t]
    ex_dm.wait_recv()
    ex_zo.start(half(1))
    unpack(dm_recv)
    sums1, b_out_sum = (zero_tile, zero_tile), zero_tile
    for t in range(pairs):
        d_in, sums1 = norm_bwd(1, t, staged(t).T + dnt[t], sums1)
        d_y = d_in + dzt[t]
        dmt[t] = d_y
        d_low = d_y.astype(BF16)
        dlt[t] = d_low
        d_gated = dot(wo_ref[0], d_low)
        dgt[t] = d_gated
        store_d_o(t, (d_gated * g_s[0, t]).astype(BF16))
        b_out_sum = b_out_sum + d_y
    gate_sum0 = zero_tile
    for t in range(pairs):
        gate_sum0 = gate_grad(0, t, gate_sum0)

    attend_bwd(0, range(rows))
    send_bias_grad0()
    sum_weights(0)
    send_weights(0)
    for t in range(pairs):
        dnt[t] = dot(wp_ref[0], dpt[t])
    send_small(1, sums1, head_weight_grad(1, d_own1), gate_sum1, b_out_row1)
    b_out_row0 = lanes_to_row(b_out_sum)
    chip_sum_weights(0)
    reduce_weights(1)
    chip_sum_small(1)

    d_own0 = take_bias_grad(0)
    terms = bias_terms(0, d_own0)
    sums0 = (zero_tile, zero_tile)
    for t in range(pairs):
        d_in, sums0 = norm_bwd(0, t, dnt[t] + terms[t], sums0)
        d_x = (d_in + dmt[t]).T.astype(BF16)
        for r in range(2):
            zg_out[2 * t + r] = d_x[r * n:(r + 1) * n]
    send_small(0, sums0, head_weight_grad(0, d_own0), gate_sum0, b_out_row0)
    chip_sum_small(0)
    reduce_weights(0)
    forward_weights(1)
    forward_weights(0)

    for one in [ex_zo] + ex_small + near_wf:
        one.wait_recv()
    for one in [ex_b0, ex_b1, near_b1, ex_mid, ex_dz, ex_mask, ex_zo, ex_dm, ex_db0, near_db1, ex_db1] + near_small + ex_small + near_w + ex_w + ex_wf + near_wf:
        one.wait_send()


def finish(dims, zo_ref, zg_ref, w_ref, sm_ref,
           zo_out, zg_out, lns_out, lnb_out, wp_out, wb_out, bg_out, wo_out, bo_out, stage):
    rows, n, ch, heads, hd, group = dims
    zg_out[...] = zg_ref[...]
    stage[...] = zo_ref[...].astype(F32).reshape(group * rows * rows, ch)
    for i in range(rows):
        zo_out[i] = stage[pl.ds(i, n, stride=rows), :].astype(BF16)
    cut = 4 * hd // group
    for s in range(2):
        full = w_ref[s].astype(F32).reshape(group, 5 * hd // group, ch)
        wp_out[s] = full[:, :cut].reshape(4 * hd, ch).T
        wo_out[s] = full[:, cut:].reshape(hd, ch)
        total = jnp.sum(sm_ref[s], axis=0)
        for place, ref in enumerate((lns_out, lnb_out, bg_out, bo_out)):
            ref[s:s + 1, :] = total[place:place + 1, :]
        wb_out[s] = total[4:4 + heads]


def solution(mesh):
    axis = 'dap'
    group = mesh.shape[axis]
    row_spec = P(('dp', axis), None, None)
    mask_spec = P(('dp', axis), None)
    grad_spec = P('dp')

    def per_device(z, pair_mask, dz_out, ln_scale, ln_shift, w_proj, w_bias, b_gate, w_out, b_out):
        rows, n, ch = z.shape
        heads = w_bias.shape[-1]
        hd = b_gate.shape[-1]
        pairs, two, wide = rows // 2, 2 * n, heads * n
        piece = (group, rows * rows, ch)
        w_rows = 5 * hd // group

        def vmem(shape, dtype):
            return pltpu.VMEM(shape, dtype)

        w_heads = jnp.swapaxes(w_bias, 1, 2)
        like = [z, z, ln_scale, ln_shift, w_proj, w_heads, b_gate, w_out, b_out]
        out_shape = [jax.ShapeDtypeStruct(a.shape, BF16 if k < 2 else F32) for k, a in enumerate(like)]
        chips = group // 2
        mid_shape = [jax.ShapeDtypeStruct(piece, BF16), jax.ShapeDtypeStruct(z.shape, BF16),
                     jax.ShapeDtypeStruct((2, 2, chips, w_rows, ch), BF16), jax.ShapeDtypeStruct((2, chips, 8, ch), F32)]
        tile = (pairs, ch, two)
        scratch = [
            vmem((2, 4 * hd, ch), BF16), vmem((2, ch, hd), BF16), vmem((2, 16, ch), BF16), vmem((2, 4, ch, n), F32),
            vmem((2,) + tile, F32), vmem((2,) + tile, F32), vmem((2, pairs, 8, two), F32), vmem((2, pairs, two, ch), BF16), vmem(tile, BF16),
            vmem((2, pairs, hd, two), BF16), vmem((2, pairs, hd, two), BF16), vmem((2, pairs, hd, two), BF16), vmem((2, pairs, two, 2 * hd), BF16),
            vmem((2, pairs, hd, two), F32), vmem((2, pairs, hd, two), F32), vmem((2, pairs, hd, two), BF16), vmem((rows * 16, n), F32),
            vmem((rows, hd, wide), BF16), vmem((rows, hd, wide), BF16), vmem((pairs, hd, two), BF16), vmem((pairs, hd, two), F32),
            vmem((pairs, 4 * hd, two), BF16), vmem(tile, F32), vmem(tile, F32), vmem(tile, F32), vmem((pairs, two, ch), BF16), vmem(tile, BF16),
            vmem((2, rows, n, wide), F32), vmem((n, wide), F32), vmem((n, wide), F32),
            vmem((2, rows, n, n), F32), vmem((group * rows * rows, ch), F32),
            vmem((5 * hd, ch), F32), vmem((2, rows, ch, heads * rows), BF16), vmem((pairs, 16, two), BF16),
            vmem((2, heads * rows, n), BF16), vmem((group, heads * rows, n), BF16), vmem((2, chips, heads * rows, n), BF16), vmem(piece, BF16), vmem(piece, BF16), vmem(piece, BF16), vmem(piece, BF16),
            vmem((rows, n), BF16), vmem((group, rows, n), BF16), vmem(piece, BF16), vmem(piece, BF16), vmem(piece, BF16),
            vmem((group, heads * rows, n), BF16), vmem((group, heads * rows, n), BF16),
            vmem((2, chips, heads * rows, n), BF16), vmem((chips, heads * rows, n), BF16), vmem((chips, heads * rows, n), BF16), vmem((chips, heads * rows, n), BF16),
            vmem((2, 2, chips, w_rows, ch), BF16), vmem((2, chips, w_rows, ch), BF16), vmem((2, chips, w_rows, ch), BF16), vmem((2, chips, w_rows, ch), BF16),
            vmem((2, w_rows, ch), BF16), vmem((2, 8, ch), F32), vmem((2, 8, ch), F32), vmem((2, 8, ch), F32),
            pltpu.SemaphoreType.DMA((23,)), pltpu.SemaphoreType.DMA((23,)),
        ]
        operands = (z, pair_mask, dz_out, ln_scale, ln_shift, w_proj, w_heads, b_gate, w_out, b_out)
        scratch += [vmem(a.shape, a.dtype) for a in operands] + [pltpu.SemaphoreType.DMA((10,))]
        in_vmem = pl.BlockSpec(memory_space=pltpu.VMEM)
        mid = pl.pallas_call(
            functools.partial(kernel, (rows, n, ch, heads, hd, group, axis)),
            out_shape=mid_shape,
            in_specs=[pl.BlockSpec(memory_space=pltpu.HBM)] * 10,
            out_specs=[in_vmem] * 4,
            scratch_shapes=scratch,
            compiler_params=pltpu.CompilerParams(collective_id=0, has_side_effects=True, vmem_limit_bytes=40 * 1024 * 1024),
        )(*[pltpu.with_memory_space_constraint(a, pltpu.HBM) for a in operands])
        out = pl.pallas_call(
            functools.partial(finish, (rows, n, ch, heads, hd, group)),
            out_shape=out_shape,
            in_specs=[in_vmem] * 4,
            out_specs=[in_vmem] * 9,
            scratch_shapes=[vmem((group * rows * rows, ch), F32)],
            compiler_params=pltpu.CompilerParams(vmem_limit_bytes=16 * 1024 * 1024),
        )(*mid)
        return tuple(out[:5]) + (jnp.swapaxes(out[5], 1, 2),) + tuple(out[6:])

    return jax.shard_map(per_device, mesh=mesh, in_specs=(row_spec, mask_spec, row_spec) + (P(),) * 7,
                         out_specs=(row_spec, row_spec) + (grad_spec,) * 7, check_vma=False)
```

```python
import functools

import jax
import jax.numpy as jnp
from jax import lax
from jax.experimental import pallas as pl
from jax.experimental.pallas import tpu as pltpu
from jax.sharding import PartitionSpec as P

EPS = 1e-5
MASK_FILL = 1e9
LOG2E = 1.4426950408889634
F32 = jnp.float32
BF16 = jnp.bfloat16
NN = (((1,), (0,)), ((), ()))
NT = (((1,), (1,)), ((), ()))


def dot(a, b, dims=NN):
    return lax.dot_general(a, b, dims, preferred_element_type=F32)


class Exchange:
    def __init__(self, group, axis, send, recv, send_sem, recv_sem, same=False):
        self.group, self.axis, self.send, self.recv = group, axis, send, recv
        self.send_sem, self.recv_sem, self.same = send_sem, recv_sem, same

    def start(self, part=None):
        me = lax.axis_index(self.axis)
        half = self.group // 2
        order = [half]
        for hop in range(half - 1, 0, -1):
            order += [hop, self.group - hop]
        for hop in order:
            peer = lax.rem(me + hop, self.group)
            source = self.send if self.same else self.send.at[peer] if part is None else self.send.at[peer, part]
            pltpu.make_async_remote_copy(
                src_ref=source,
                dst_ref=self.recv.at[me] if part is None else self.recv.at[me, part],
                send_sem=self.send_sem,
                recv_sem=self.recv_sem,
                device_id={self.axis: peer},
                device_id_type=pl.DeviceIdType.MESH,
            ).start()
        if part is None:
            self.recv[me] = self.send[...] if self.same else self.send[me]
        else:
            self.recv[me, part] = self.send[me, part]

    def _all(self):
        some = self.recv.at[pl.ds(0, self.group - 1)]
        return pltpu.make_async_remote_copy(
            src_ref=some,
            dst_ref=some,
            send_sem=self.send_sem,
            recv_sem=self.recv_sem,
            device_id={self.axis: lax.axis_index(self.axis)},
            device_id_type=pl.DeviceIdType.MESH,
        )

    def wait_recv(self):
        self._all().wait_recv()

    def wait_send(self):
        self._all().wait_send()


class ChipExchange:
    def __init__(self, chips, axis, send, recv, send_sem, recv_sem, same=False):
        self.chips, self.axis, self.send, self.recv = chips, axis, send, recv
        self.send_sem, self.recv_sem, self.same = send_sem, recv_sem, same

    def start(self):
        me = lax.axis_index(self.axis)
        chip, core = me // 2, me % 2
        order = [self.chips // 2]
        for hop in range(self.chips // 2 - 1, 0, -1):
            order += [hop, self.chips - hop]
        for hop in order:
            to = lax.rem(chip + hop, self.chips)
            pltpu.make_async_remote_copy(
                src_ref=self.send if self.same else self.send.at[to],
                dst_ref=self.recv.at[chip],
                send_sem=self.send_sem,
                recv_sem=self.recv_sem,
                device_id={self.axis: 2 * to + core},
                device_id_type=pl.DeviceIdType.MESH,
            ).start()
        self.recv[chip] = self.send[...] if self.same else self.send[chip]

    def _all(self):
        some = self.recv.at[pl.ds(0, self.chips - 1)]
        return pltpu.make_async_remote_copy(
            src_ref=some,
            dst_ref=some,
            send_sem=self.send_sem,
            recv_sem=self.recv_sem,
            device_id={self.axis: lax.axis_index(self.axis)},
            device_id_type=pl.DeviceIdType.MESH,
        )

    def wait_recv(self):
        self._all().wait_recv()

    def wait_send(self):
        self._all().wait_send()


def kernel(dims, *refs):
    rows, n, ch, heads, hd, group, axis = dims
    hdim = hd // heads
    scale = hdim ** -0.5
    pairs = rows // 2
    two = 2 * n
    wide = heads * n
    chips = group // 2
    operands = refs[:10]
    local = refs[-11:-1]
    (z_ref, mask_ref, dz_ref, lns_ref, lnb_ref, wp_ref, wb_ref, bg_ref, wo_ref, bo_ref) = local
    load_sems, refs = refs[-1], refs[10:-11]
    (zo_recv, zg_out, w_full, sm_recv,
     wpt, wot, wbt, col,
     xt, xh, inv, a_s, at0, at1, qt, kt, vt, kv, g_s, ot, ut, btmp, qbd, dbd, dot_s, dgt, dpt, dnt, dzt, dmt, dlp, dlt, pf, bias, db, maskb, stage,
     wacc, wsel, dbt,
     b_send, b_recv, b1_recv, mid_send, mid_recv, dz_send, dz_recv, mk_send, mk_recv, zo_send, dm_send, dm_recv,
     db_send, db_recv, d1_send, d1_half, d1_mid, d1_recv, w_send, w_half, w_mid, w_recv, w_part, sm_send, sm_half, sm_mid,
     send_sems, recv_sems) = refs
    me = lax.axis_index(axis)
    core = me % 2
    loads = [pltpu.make_async_copy(src, dst, load_sems.at[k]) for k, (src, dst) in enumerate(zip(operands, local))]
    for k in (3, 4, 6, 0, 5, 7, 1, 2, 8, 9):
        loads[k].start()

    def exchange(slot, send, recv, same=False):
        return Exchange(group, axis, send, recv, send_sems.at[slot], recv_sems.at[slot], same)

    def chip_exchange(slot, send, recv, same=False):
        return ChipExchange(chips, axis, send, recv, send_sems.at[slot], recv_sems.at[slot], same)

    def to_sibling(slot, send, recv):
        return pltpu.make_async_remote_copy(src_ref=send, dst_ref=recv, send_sem=send_sems.at[slot], recv_sem=recv_sems.at[slot],
                                            device_id={axis: me + 1 - 2 * core}, device_id_type=pl.DeviceIdType.MESH)

    ex_b0 = exchange(0, b_send.at[0], b_recv, True)
    ex_b1 = chip_exchange(1, b_send.at[1], b1_recv.at[core], True)
    near_b1 = to_sibling(19, b1_recv.at[core], b1_recv.at[core])
    ex_mid = exchange(2, mid_send, mid_recv)
    ex_dz = exchange(3, dz_send, dz_recv)
    ex_mask = exchange(4, mk_send, mk_recv, True)
    ex_zo = exchange(5, zo_send, zo_recv)
    ex_dm = exchange(6, dm_send, dm_recv)
    ex_db0 = exchange(7, db_send, db_recv)
    near_db1 = to_sibling(8, d1_send.at[1 - core], d1_half)
    ex_db1 = chip_exchange(20, d1_mid, d1_recv)
    near_small = [to_sibling(9 + s, sm_send.at[s], sm_half.at[s]) for s in range(2)]
    ex_small = [chip_exchange(21 + s, sm_mid.at[s], sm_recv.at[s], True) for s in range(2)]
    near_w = [to_sibling(11 + s, w_send.at[s, 1 - core], w_half.at[s]) for s in range(2)]
    ex_w = [chip_exchange(13 + s, w_mid.at[s], w_recv.at[s]) for s in range(2)]
    ex_wf = [chip_exchange(15 + s, w_part.at[s], w_full.at[s, core], True) for s in range(2)]
    near_wf = [to_sibling(17 + s, w_full.at[s, core], w_full.at[s, core]) for s in range(2)]

    barrier = pltpu.get_barrier_semaphore()
    for hop in range(1, group):
        pl.semaphore_signal(barrier, inc=1, device_id={axis: lax.rem(me + hop, group)},
                            device_id_type=pl.DeviceIdType.MESH)

    def zero_diag(i, carry):
        qbd[i] = jnp.zeros((hd, wide), BF16)
        dbd[i] = jnp.zeros((hd, wide), BF16)
        return carry
    lax.fori_loop(0, rows, zero_diag, 0)
    for k in (3, 4, 6):
        loads[k].wait()
    head_pick = (lax.broadcasted_iota(jnp.int32, (16, heads), 0) == lax.broadcasted_iota(jnp.int32, (16, heads), 1)).astype(BF16)
    eye = (lax.broadcasted_iota(jnp.int32, (ch, ch), 0) == lax.broadcasted_iota(jnp.int32, (ch, ch), 1)).astype(BF16)

    def to_column(s, place):
        ref = (lns_ref, lnb_ref, bg_ref, bo_ref)[place]
        col[s, place] = jnp.broadcast_to(ref[s:s + 1, :], (n, ch)).T

    def prepare_norm(s):
        wbt[s] = dot(head_pick, wb_ref[s]).astype(BF16)
        to_column(s, 0)
        to_column(s, 1)
    prepare_norm(0)

    def prepare_project(s):
        wpt[s] = wp_ref[s].T
        to_column(s, 2)

    def prepare_late():
        prepare_norm(1)
        prepare_project(1)
        to_column(0, 3)
        to_column(1, 3)
        at16 = lax.broadcasted_iota(jnp.int32, (16, heads * rows), 0)
        at32 = lax.broadcasted_iota(jnp.int32, (16, heads * rows), 1)
        for s in range(2):
            wot[s] = wo_ref[s].T
            w_heads = dot(eye, wbt[s], NT).astype(BF16)
            for i in range(rows):
                wsel[s, i] = dot(w_heads, ((at32 == at16 * rows + i) & (at16 < heads)).astype(BF16)).astype(BF16)

    def column(s, place):
        one = col[s, place]
        return jnp.concatenate([one, one], axis=1)

    def store_diag(ref, t, value):
        for r in range(2):
            for h in range(heads):
                ref[2 * t + r, h * hdim:(h + 1) * hdim, h * n:(h + 1) * n] = value[h * hdim:(h + 1) * hdim, r * n:(r + 1) * n]

    def staged(t):
        return jnp.concatenate([stage[pl.ds(2 * t + r, n, stride=rows), :] for r in range(2)], axis=0)

    def unpack(recv):
        stage[...] = recv[...].astype(F32).reshape(group * rows * rows, ch)

    def pack(send, t, value):
        parts = [value[r * n:(r + 1) * n].reshape(group, n // group, ch) for r in range(2)]
        send[:, pl.ds(pl.multiple_of(t * 16, 16), 16), :] = jnp.concatenate(parts, axis=1).astype(BF16)

    def half(k):
        return pl.ds(k * rows * rows // 2, rows * rows // 2)

    def normalize(s, t, x):
        centred = x - jnp.mean(x, axis=0, keepdims=True)
        inv_std = lax.rsqrt(jnp.mean(centred * centred, axis=0, keepdims=True) + EPS)
        x_hat = centred * inv_std
        return (x_hat * column(s, 0) + column(s, 1)).astype(BF16), x_hat, inv_std

    def keep_norm(s, t, x):
        a_t, x_hat, inv_std = normalize(s, t, x)
        xh[s, t] = x_hat
        inv[s, t] = jnp.broadcast_to(inv_std, (8, two))
        b_t = dot(wbt[s], a_t)
        btmp[pl.ds(pl.multiple_of(t * 32, 32), 32), :] = jnp.concatenate([b_t[:, :n], b_t[:, n:]], axis=0)
        return a_t

    def project(s, t, a_t):
        a = a_t.T
        a_s[s, t] = a
        p = dot(wpt[s], a_t).astype(BF16)
        qt[s, t] = p[:hd]
        kt[s, t] = p[hd:2 * hd]
        vt[s, t] = p[2 * hd:3 * hd]
        store_diag(qbd, t, p[:hd])
        g = jax.nn.sigmoid(p[3 * hd:].astype(F32) + column(s, 2))
        g_s[s, t] = g
        kv[s, t] = dot(a, wp_ref[s, :, hd:3 * hd]).astype(BF16)
        return g

    def send_bias(s):
        for h in range(0, heads, 2):
            some = [btmp[pl.ds(h + r, rows, stride=16), :] for r in range(2)]
            b_send[s, h * rows:(h + 2) * rows, :] = jnp.concatenate(some, axis=0).astype(BF16)
        (ex_b0, ex_b1)[s].start()

    def take_bias0():
        ex_b0.wait_recv()
        got = b_recv[...].astype(F32).reshape(group, heads, rows, n)
        for h in range(heads):
            bias[:, h * n:(h + 1) * n] = got[:, h].reshape(n, n).T * LOG2E

    def take_bias1():
        near_b1.wait_recv()
        for c in range(2):
            got = b1_recv[c].astype(F32) * LOG2E
            for chip in range(chips):
                for h in range(heads):
                    at = (2 * chip + c) * rows
                    bias[at:at + rows, h * n:(h + 1) * n] = got[chip, h * rows:(h + 1) * rows]

    def logits(s):
        for i in range(rows):
            t, r = divmod(i, 2)
            fill = maskb[s, i]
            raw = dot(kv[s, t, r * n:(r + 1) * n, :hd], qbd[i])
            for h in range(heads):
                pf[s, i, :, h * n:(h + 1) * n] = raw[:, h * n:(h + 1) * n] * (scale * LOG2E) + fill

    def attend(s, some):
        for i in some:
            t, r = divmod(i, 2)
            for h in range(heads):
                cols = slice(h * n, (h + 1) * n)
                x = pf[s, i, :, cols] + bias[:, cols]
                e = jnp.exp2(x - jnp.max(x, axis=0, keepdims=True))
                p = e * (1.0 / jnp.sum(e, axis=0, keepdims=True))
                pf[s, i, :, cols] = p
                hs = slice(h * hdim, (h + 1) * hdim)
                ot[s, t, hs, r * n:(r + 1) * n] = dot(vt[s, t, hs, r * n:(r + 1) * n], p.astype(BF16))

    def block_out(s, t):
        u = (ot[s, t] * g_s[s, t]).astype(BF16)
        ut[s, t] = u
        return xt[s, t] + dot(wot[s], u) + column(s, 3)

    def attend_bwd(s, some):
        def d_probs(i):
            t, r = divmod(i, 2)
            return dot(kv[s, t, r * n:(r + 1) * n, hd:], dbd[i])
        ahead = d_probs(some[0])
        for k, i in enumerate(some):
            t, r = divmod(i, 2)
            d_p = ahead
            if k + 1 < len(some):
                ahead = d_probs(some[k + 1])
            at = slice(r * n, (r + 1) * n)
            for h in range(heads):
                cols = slice(h * n, (h + 1) * n)
                p = pf[s, i, :, cols]
                d_ph = d_p[:, cols]
                d_l = p * (d_ph - jnp.sum(d_ph * p, axis=0, keepdims=True))
                db[:, cols] += d_l
                d_s = (d_l * scale).astype(BF16)
                hs = slice(h * hdim, (h + 1) * hdim)
                d_q = dot(kt[s, t, hs, at], d_s)
                d_k = dot(qt[s, t, hs, at], d_s, NT)
                d_v = dot(dot_s[t, hs, at], p.astype(BF16), NT)
                dpt[t, h * hdim:(h + 1) * hdim, at] = d_q.astype(BF16)
                dpt[t, hd + h * hdim:hd + (h + 1) * hdim, at] = d_k.astype(BF16)
                dpt[t, 2 * hd + h * hdim:2 * hd + (h + 1) * hdim, at] = d_v.astype(BF16)

    def store_d_o(t, d_o):
        dot_s[t] = d_o
        store_diag(dbd, t, d_o)

    def gate_grad(s, t, gate_sum):
        g = g_s[s, t]
        d_lin = dgt[t] * ot[s, t] * g * (1.0 - g)
        dpt[t, 3 * hd:, :] = d_lin.astype(BF16)
        return gate_sum + d_lin

    def send_weights(s):
        top = wacc[:4 * hd].reshape(2, chips, 4 * hd // group, ch)
        low = wacc[4 * hd:].reshape(2, chips, hd // group, ch)
        w_send[s] = jnp.concatenate([top, low], axis=2).astype(BF16)
        near_w[s].start()

    def chip_sum_weights(s):
        near_w[s].wait_recv()
        w_mid[s] = (w_send[s, core].astype(F32) + w_half[s].astype(F32)).astype(BF16)
        ex_w[s].start()

    def reduce_weights(s):
        ex_w[s].wait_recv()
        w_part[s] = jnp.sum(w_recv[s].astype(F32), axis=0).astype(BF16)
        ex_wf[s].start()

    def forward_weights(s):
        ex_wf[s].wait_recv()
        near_wf[s].start()

    def send_bias_grad0():
        for h in range(0, heads, 2):
            some = [db[:, (h + r) * n:(h + r + 1) * n].T.reshape(group, rows, n) for r in range(2)]
            db_send[:, h * rows:(h + 2) * rows, :] = jnp.concatenate(some, axis=1).astype(BF16)
        ex_db0.start()

    def send_bias_grad1():
        for h in range(0, heads, 2):
            some = [db[:, (h + r) * n:(h + r + 1) * n].reshape(chips, 2, rows, n) for r in range(2)]
            for c in range(2):
                d1_send[c, :, h * rows:(h + 2) * rows, :] = jnp.concatenate([one[:, c] for one in some], axis=1).astype(BF16)
        near_db1.start()

    def chip_sum_bias_grad1():
        near_db1.wait_recv()
        d1_mid[...] = (d1_send[core].astype(F32) + d1_half[...].astype(F32)).astype(BF16)
        ex_db1.start()

    def take_bias_grad(s):
        (ex_db0, ex_db1)[s].wait_recv()
        got = (db_recv, d1_recv)[s]
        return jnp.sum(got[...].astype(F32), axis=0).astype(BF16)

    def bias_terms(s, d_own):
        return [jnp.concatenate([dot(wsel[s, 2 * t + r], d_own) for r in range(2)], axis=1) for t in range(pairs)]

    def head_weight_grad(s, d_own):
        at16 = lax.broadcasted_iota(jnp.int32, (16, heads * rows), 0)
        at32 = lax.broadcasted_iota(jnp.int32, (16, heads * rows), 1)
        for t in range(pairs):
            rows_of = [dot((at32 == at16 * rows + (2 * t + r)).astype(BF16), d_own) for r in range(2)]
            dbt[t] = jnp.concatenate(rows_of, axis=1).astype(BF16)
        total = None
        for t in range(pairs):
            one = dot(dbt[t], a_s[0, t]) if s == 0 else dot(dbt[t], at1[t], NT)
            total = one if total is None else total + one
        return total

    def norm_bwd(s, t, d_n, sums):
        x_hat = xh[s, t]
        d_hat = d_n * column(s, 0)
        along = jnp.mean(d_hat * x_hat, axis=0, keepdims=True)
        d_in = inv[s, t, 0:1, :] * (d_hat - jnp.mean(d_hat, axis=0, keepdims=True) - x_hat * along)
        return d_in, (sums[0] + d_n * x_hat, sums[1] + d_n)

    def lanes_to_row(value):
        return jnp.sum((value[:, :n] + value[:, n:]).T, axis=0, keepdims=True)

    def send_small(s, sums, wb_sum, gate_sum, b_out_row):
        gain_sum, shift_sum = sums
        sm_send[s, 0:1, :] = lanes_to_row(gain_sum)
        sm_send[s, 1:2, :] = lanes_to_row(shift_sum)
        sm_send[s, 2:3, :] = lanes_to_row(gate_sum)
        sm_send[s, 3:4, :] = b_out_row
        sm_send[s, 4:4 + heads, :] = wb_sum[:heads]
        near_small[s].start()

    def chip_sum_small(s):
        near_small[s].wait_recv()
        sm_mid[s] = sm_send[s] + sm_half[s]
        ex_small[s].start()

    zero_tile = jnp.zeros((ch, two), F32)
    early, late = range(pairs // 2), range(pairs // 2, pairs)

    loads[0].wait()
    for t in range(pairs):
        x = jnp.concatenate([z_ref[2 * t + r].astype(F32).T for r in range(2)], axis=1)
        xt[0, t] = x
        at0[t] = keep_norm(0, t, x)
    pl.semaphore_wait(barrier, group - 1)
    send_bias(0)
    loads[5].wait()
    loads[7].wait()
    prepare_project(0)
    for t in range(pairs):
        project(0, t, at0[t])
    loads[1].wait()
    fill_rows = (mask_ref[...].astype(F32) - 1.0) * (MASK_FILL * LOG2E)
    for i in range(rows):
        maskb[0, i] = jnp.broadcast_to(fill_rows[i:i + 1, :], (n, n)).T
    logits(0)
    for k in (2, 8, 9):
        loads[k].wait()
    b_out_row1 = jnp.zeros((1, ch), F32)
    for t in range(pairs):
        d_y = jnp.concatenate([dz_ref[2 * t + r].astype(F32) for r in range(2)], axis=0)
        pack(dz_send, t, d_y)
        dzt[t] = d_y.T
        b_out_row1 = b_out_row1 + jnp.sum(d_y, axis=0, keepdims=True)
    mk_send[...] = mask_ref[...].astype(F32).astype(BF16)
    prepare_late()
    ex_dz.start(half(0))
    ex_mask.start()
    take_bias0()

    for k, some in enumerate((early, late)):
        attend(0, range(2 * some[0], 2 * some[-1] + 2))
        for t in some:
            y = block_out(0, t)
            pack(mid_send, t, y.T)
            xt[1, t] = y.astype(BF16).astype(F32)
        ex_mid.start(half(k))
    for t in range(pairs):
        at1[t] = keep_norm(1, t, xt[1, t])
    send_bias(1)
    ex_dz.start(half(1))

    db[...] = jnp.zeros((n, wide), F32)
    ex_mask.wait_recv()
    whole = mk_recv[...].astype(F32).reshape(n, n).astype(BF16)
    for i in range(rows):
        pick = (lax.broadcasted_iota(jnp.int32, (n, n), 0) == me * rows + i).astype(BF16)
        maskb[1, i] = (dot(whole, pick) - 1.0) * (MASK_FILL * LOG2E)

    ex_mid.wait_recv()
    unpack(mid_recv)
    for t in range(pairs):
        x = staged(t).T
        xt[1, t] = x
        project(1, t, normalize(1, t, x)[0])
    ex_b1.wait_recv()
    near_b1.start()
    logits(1)
    take_bias1()
    attend(1, range(rows // 2))
    for t in early:
        pack(zo_send, t, block_out(1, t).T)
    ex_zo.start(half(0))
    attend(1, range(rows // 2, rows))
    ex_dz.wait_recv()
    unpack(dz_recv)
    for t in range(pairs):
        d_low = staged(t).astype(BF16)
        dlp[t] = d_low
        dgt[t] = dot(wo_ref[1], d_low, NT)
    for t in range(pairs):
        store_d_o(t, (dgt[t] * g_s[1, t]).astype(BF16))

    gate_sum1 = zero_tile
    for k, some in enumerate((early, late)):
        attend_bwd(1, range(2 * some[0], 2 * some[-1] + 2))
        if k == 1:
            send_bias_grad1()
        for t in some:
            gate_sum1 = gate_grad(1, t, gate_sum1)
            pack(dm_send, t, dot(wp_ref[1], dpt[t]).T)
        ex_dm.start(half(k))
    for t in late:
        pack(zo_send, t, block_out(1, t).T)
    chip_sum_bias_grad1()

    def sum_weights(s):
        top, low = None, None
        for t in range(pairs):
            one = dot(dpt[t], a_s[s, t])
            two_ = dot(ut[1, t], dlp[t]) if s == 1 else dot(ut[0, t], dlt[t], NT)
            top, low = (one, two_) if top is None else (top + one, low + two_)
        wacc[:4 * hd] = top
        wacc[4 * hd:] = low
    sum_weights(1)
    send_weights(1)
    db[...] = jnp.zeros((n, wide), F32)
    chip_sum_weights(1)

    d_own1 = take_bias_grad(1)
    terms = bias_terms(1, d_own1)
    for t in range(pairs):
        dnt[t] = terms[t]
    ex_dm.wait_recv()
    ex_zo.start(half(1))
    unpack(dm_recv)
    sums1, b_out_sum = (zero_tile, zero_tile), zero_tile
    for t in range(pairs):
        d_in, sums1 = norm_bwd(1, t, staged(t).T + dnt[t], sums1)
        d_y = d_in + dzt[t]
        dmt[t] = d_y
        d_low = d_y.astype(BF16)
        dlt[t] = d_low
        d_gated = dot(wo_ref[0], d_low)
        dgt[t] = d_gated
        store_d_o(t, (d_gated * g_s[0, t]).astype(BF16))
        b_out_sum = b_out_sum + d_y
    gate_sum0 = zero_tile
    for t in range(pairs):
        gate_sum0 = gate_grad(0, t, gate_sum0)

    attend_bwd(0, range(rows))
    send_bias_grad0()
    sum_weights(0)
    send_weights(0)
    for t in range(pairs):
        dnt[t] = dot(wp_ref[0], dpt[t])
    send_small(1, sums1, head_weight_grad(1, d_own1), gate_sum1, b_out_row1)
    b_out_row0 = lanes_to_row(b_out_sum)
    chip_sum_weights(0)
    reduce_weights(1)
    chip_sum_small(1)

    d_own0 = take_bias_grad(0)
    terms = bias_terms(0, d_own0)
    sums0 = (zero_tile, zero_tile)
    for t in range(pairs):
        d_in, sums0 = norm_bwd(0, t, dnt[t] + terms[t], sums0)
        d_x = (d_in + dmt[t]).T.astype(BF16)
        for r in range(2):
            zg_out[2 * t + r] = d_x[r * n:(r + 1) * n]
    send_small(0, sums0, head_weight_grad(0, d_own0), gate_sum0, b_out_row0)
    chip_sum_small(0)
    reduce_weights(0)
    forward_weights(1)
    forward_weights(0)

    for one in [ex_zo] + ex_small + near_wf:
        one.wait_recv()
    for one in [ex_b0, ex_b1, near_b1, ex_mid, ex_dz, ex_mask, ex_zo, ex_dm, ex_db0, near_db1, ex_db1] + near_small + ex_small + near_w + ex_w + ex_wf + near_wf:
        one.wait_send()


def finish(dims, zo_ref, zg_ref, w_ref, sm_ref,
           zo_out, zg_out, lns_out, lnb_out, wp_out, wb_out, bg_out, wo_out, bo_out, stage):
    rows, n, ch, heads, hd, group = dims
    zg_out[...] = zg_ref[...]
    stage[...] = zo_ref[...].astype(F32).reshape(group * rows * rows, ch)
    for i in range(rows):
        zo_out[i] = stage[pl.ds(i, n, stride=rows), :].astype(BF16)
    cut = 4 * hd // group
    for s in range(2):
        full = w_ref[s].astype(F32).reshape(group, 5 * hd // group, ch)
        wp_out[s] = full[:, :cut].reshape(4 * hd, ch).T
        wo_out[s] = full[:, cut:].reshape(hd, ch)
        total = jnp.sum(sm_ref[s], axis=0)
        for place, ref in enumerate((lns_out, lnb_out, bg_out, bo_out)):
            ref[s:s + 1, :] = total[place:place + 1, :]
        wb_out[s] = total[4:4 + heads]


def solution(mesh):
    axis = 'dap'
    group = mesh.shape[axis]
    row_spec = P(('dp', axis), None, None)
    mask_spec = P(('dp', axis), None)
    grad_spec = P('dp')

    def per_device(z, pair_mask, dz_out, ln_scale, ln_shift, w_proj, w_bias, b_gate, w_out, b_out):
        rows, n, ch = z.shape
        heads = w_bias.shape[-1]
        hd = b_gate.shape[-1]
        pairs, two, wide = rows // 2, 2 * n, heads * n
        piece = (group, rows * rows, ch)
        w_rows = 5 * hd // group

        def vmem(shape, dtype):
            return pltpu.VMEM(shape, dtype)

        w_heads = jnp.swapaxes(w_bias, 1, 2)
        like = [z, z, ln_scale, ln_shift, w_proj, w_heads, b_gate, w_out, b_out]
        out_shape = [jax.ShapeDtypeStruct(a.shape, BF16 if k < 2 else F32) for k, a in enumerate(like)]
        chips = group // 2
        mid_shape = [jax.ShapeDtypeStruct(piece, BF16), jax.ShapeDtypeStruct(z.shape, BF16),
                     jax.ShapeDtypeStruct((2, 2, chips, w_rows, ch), BF16), jax.ShapeDtypeStruct((2, chips, 8, ch), F32)]
        tile = (pairs, ch, two)
        scratch = [
            vmem((2, 4 * hd, ch), BF16), vmem((2, ch, hd), BF16), vmem((2, 16, ch), BF16), vmem((2, 4, ch, n), F32),
            vmem((2,) + tile, F32), vmem((2,) + tile, F32), vmem((2, pairs, 8, two), F32), vmem((2, pairs, two, ch), BF16), vmem(tile, BF16), vmem(tile, BF16),
            vmem((2, pairs, hd, two), BF16), vmem((2, pairs, hd, two), BF16), vmem((2, pairs, hd, two), BF16), vmem((2, pairs, two, 2 * hd), BF16),
            vmem((2, pairs, hd, two), F32), vmem((2, pairs, hd, two), F32), vmem((2, pairs, hd, two), BF16), vmem((rows * 16, n), F32),
            vmem((rows, hd, wide), BF16), vmem((rows, hd, wide), BF16), vmem((pairs, hd, two), BF16), vmem((pairs, hd, two), F32),
            vmem((pairs, 4 * hd, two), BF16), vmem(tile, F32), vmem(tile, F32), vmem(tile, F32), vmem((pairs, two, ch), BF16), vmem(tile, BF16),
            vmem((2, rows, n, wide), F32), vmem((n, wide), F32), vmem((n, wide), F32),
            vmem((2, rows, n, n), F32), vmem((group * rows * rows, ch), F32),
            vmem((5 * hd, ch), F32), vmem((2, rows, ch, heads * rows), BF16), vmem((pairs, 16, two), BF16),
            vmem((2, heads * rows, n), BF16), vmem((group, heads * rows, n), BF16), vmem((2, chips, heads * rows, n), BF16), vmem(piece, BF16), vmem(piece, BF16), vmem(piece, BF16), vmem(piece, BF16),
            vmem((rows, n), BF16), vmem((group, rows, n), BF16), vmem(piece, BF16), vmem(piece, BF16), vmem(piece, BF16),
            vmem((group, heads * rows, n), BF16), vmem((group, heads * rows, n), BF16),
            vmem((2, chips, heads * rows, n), BF16), vmem((chips, heads * rows, n), BF16), vmem((chips, heads * rows, n), BF16), vmem((chips, heads * rows, n), BF16),
            vmem((2, 2, chips, w_rows, ch), BF16), vmem((2, chips, w_rows, ch), BF16), vmem((2, chips, w_rows, ch), BF16), vmem((2, chips, w_rows, ch), BF16),
            vmem((2, w_rows, ch), BF16), vmem((2, 8, ch), F32), vmem((2, 8, ch), F32), vmem((2, 8, ch), F32),
            pltpu.SemaphoreType.DMA((23,)), pltpu.SemaphoreType.DMA((23,)),
        ]
        operands = (z, pair_mask, dz_out, ln_scale, ln_shift, w_proj, w_heads, b_gate, w_out, b_out)
        scratch += [vmem(a.shape, a.dtype) for a in operands] + [pltpu.SemaphoreType.DMA((10,))]
        in_vmem = pl.BlockSpec(memory_space=pltpu.VMEM)
        mid = pl.pallas_call(
            functools.partial(kernel, (rows, n, ch, heads, hd, group, axis)),
            out_shape=mid_shape,
            in_specs=[pl.BlockSpec(memory_space=pltpu.HBM)] * 10,
            out_specs=[in_vmem] * 4,
            scratch_shapes=scratch,
            compiler_params=pltpu.CompilerParams(collective_id=0, has_side_effects=True, vmem_limit_bytes=40 * 1024 * 1024),
        )(*[pltpu.with_memory_space_constraint(a, pltpu.HBM) for a in operands])
        out = pl.pallas_call(
            functools.partial(finish, (rows, n, ch, heads, hd, group)),
            out_shape=out_shape,
            in_specs=[in_vmem] * 4,
            out_specs=[in_vmem] * 9,
            scratch_shapes=[vmem((group * rows * rows, ch), F32)],
            compiler_params=pltpu.CompilerParams(vmem_limit_bytes=16 * 1024 * 1024),
        )(*mid)
        return tuple(out[:5]) + (jnp.swapaxes(out[5], 1, 2),) + tuple(out[6:])

    return jax.shard_map(per_device, mesh=mesh, in_specs=(row_spec, mask_spec, row_spec) + (P(),) * 7,
                         out_specs=(row_spec, row_spec) + (grad_spec,) * 7, check_vma=False)
```

```python
import functools

import jax
import jax.numpy as jnp
from jax import lax
from jax.experimental import pallas as pl
from jax.experimental.pallas import tpu as pltpu
from jax.sharding import PartitionSpec as P

EPS = 1e-5
MASK_FILL = 1e9
LOG2E = 1.4426950408889634
F32 = jnp.float32
BF16 = jnp.bfloat16
NN = (((1,), (0,)), ((), ()))
NT = (((1,), (1,)), ((), ()))


def dot(a, b, dims=NN):
    return lax.dot_general(a, b, dims, preferred_element_type=F32)


def far_first(size):
    order = [size // 2]
    for hop in range(size // 2 - 1, 0, -1):
        order += [hop, size - hop]
    return order


class Exchange:
    def __init__(self, group, axis, send, recv, send_sem, recv_sem, same=False):
        self.group, self.axis, self.send, self.recv = group, axis, send, recv
        self.send_sem, self.recv_sem, self.same = send_sem, recv_sem, same

    def start(self, part=None):
        me = lax.axis_index(self.axis)
        for hop in far_first(self.group):
            peer = lax.rem(me + hop, self.group)
            source = self.send if self.same else self.send.at[peer] if part is None else self.send.at[peer, part]
            pltpu.make_async_remote_copy(
                src_ref=source,
                dst_ref=self.recv.at[me] if part is None else self.recv.at[me, part],
                send_sem=self.send_sem,
                recv_sem=self.recv_sem,
                device_id={self.axis: peer},
                device_id_type=pl.DeviceIdType.MESH,
            ).start()
        if part is None:
            self.recv[me] = self.send[...] if self.same else self.send[me]
        else:
            self.recv[me, part] = self.send[me, part]

    def _all(self):
        some = self.recv.at[pl.ds(0, self.group - 1)]
        return pltpu.make_async_remote_copy(
            src_ref=some,
            dst_ref=some,
            send_sem=self.send_sem,
            recv_sem=self.recv_sem,
            device_id={self.axis: lax.axis_index(self.axis)},
            device_id_type=pl.DeviceIdType.MESH,
        )

    def wait_recv(self):
        self._all().wait_recv()

    def wait_send(self):
        self._all().wait_send()


class ChipExchange:
    def __init__(self, chips, axis, send, recv, send_sem, recv_sem, same=False):
        self.chips, self.axis, self.send, self.recv = chips, axis, send, recv
        self.send_sem, self.recv_sem, self.same = send_sem, recv_sem, same

    def start(self):
        me = lax.axis_index(self.axis)
        chip, core = me // 2, me % 2
        for hop in far_first(self.chips):
            to = lax.rem(chip + hop, self.chips)
            pltpu.make_async_remote_copy(
                src_ref=self.send if self.same else self.send.at[to],
                dst_ref=self.recv.at[chip],
                send_sem=self.send_sem,
                recv_sem=self.recv_sem,
                device_id={self.axis: 2 * to + core},
                device_id_type=pl.DeviceIdType.MESH,
            ).start()
        self.recv[chip] = self.send[...] if self.same else self.send[chip]

    def _all(self):
        some = self.recv.at[pl.ds(0, self.chips - 1)]
        return pltpu.make_async_remote_copy(
            src_ref=some,
            dst_ref=some,
            send_sem=self.send_sem,
            recv_sem=self.recv_sem,
            device_id={self.axis: lax.axis_index(self.axis)},
            device_id_type=pl.DeviceIdType.MESH,
        )

    def wait_recv(self):
        self._all().wait_recv()

    def wait_send(self):
        self._all().wait_send()


def kernel(dims, *refs):
    rows, n, ch, heads, hd, group, axis = dims
    hdim = hd // heads
    scale = hdim ** -0.5
    pairs = rows // 2
    two = 2 * n
    wide = heads * n
    chips = group // 2
    operands = refs[:10]
    local = refs[-11:-1]
    (z_ref, mask_ref, dz_ref, lns_ref, lnb_ref, wp_ref, wb_ref, bg_ref, wo_ref, bo_ref) = local
    load_sems, refs = refs[-1], refs[10:-11]
    (zo_recv, zg_out, w_full, sm_recv,
     wpt, wot, wbt, col,
     xt, xh, inv, a_s, at0, at1, qt, kt, vt, kv, g_s, ot, ut, btmp, qbd, dbd, dot_s, dgt, dpt, dnt, dzt, dmt, dlp, dlt, pf, bias, db, maskb, stage,
     wacc, wsel, dbt,
     b_send, b_recv, b1_recv, mid_send, mid_recv, dz_send, dz_recv, mk_send, mk_recv, zo_send, dm_send, dm_recv,
     db_send, db_half, db_mid, db_recv, w_send, w_half, w_mid, w_recv, w_part, sm_send, sm_half, sm_mid,
     send_sems, recv_sems) = refs
    me = lax.axis_index(axis)
    core = me % 2
    barrier = pltpu.get_barrier_semaphore()
    for hop in far_first(group):
        pl.semaphore_signal(barrier, inc=1, device_id={axis: lax.rem(me + hop, group)},
                            device_id_type=pl.DeviceIdType.MESH)
    loads = [pltpu.make_async_copy(src, dst, load_sems.at[k]) for k, (src, dst) in enumerate(zip(operands, local))]
    for k in (3, 4, 6, 0, 5, 7, 1, 2, 8, 9):
        loads[k].start()

    def exchange(slot, send, recv, same=False):
        return Exchange(group, axis, send, recv, send_sems.at[slot], recv_sems.at[slot], same)

    def chip_exchange(slot, send, recv, same=False):
        return ChipExchange(chips, axis, send, recv, send_sems.at[slot], recv_sems.at[slot], same)

    def to_sibling(slot, send, recv):
        return pltpu.make_async_remote_copy(src_ref=send, dst_ref=recv, send_sem=send_sems.at[slot], recv_sem=recv_sems.at[slot],
                                            device_id={axis: me + 1 - 2 * core}, device_id_type=pl.DeviceIdType.MESH)

    ex_b0 = exchange(0, b_send.at[0], b_recv, True)
    ex_b1 = chip_exchange(1, b_send.at[1], b1_recv.at[core], True)
    near_b1 = to_sibling(19, b1_recv.at[core], b1_recv.at[core])
    ex_mid = exchange(2, mid_send, mid_recv)
    ex_dz = exchange(3, dz_send, dz_recv)
    ex_mask = exchange(4, mk_send, mk_recv, True)
    ex_zo = exchange(5, zo_send, zo_recv)
    ex_dm = exchange(6, dm_send, dm_recv)
    near_db = [to_sibling(7 + s, db_send.at[s, 1 - core], db_half.at[s]) for s in range(2)]
    ex_db = [chip_exchange((20, 23)[s], db_mid.at[s], db_recv.at[s]) for s in range(2)]
    near_small = [to_sibling(9 + s, sm_send.at[s], sm_half.at[s]) for s in range(2)]
    ex_small = [chip_exchange(21 + s, sm_mid.at[s], sm_recv.at[s], True) for s in range(2)]
    near_w = [to_sibling(11 + s, w_send.at[s, 1 - core], w_half.at[s]) for s in range(2)]
    ex_w = [chip_exchange(13 + s, w_mid.at[s], w_recv.at[s]) for s in range(2)]
    ex_wf = [chip_exchange(15 + s, w_part.at[s], w_full.at[s, core], True) for s in range(2)]
    near_wf = [to_sibling(17 + s, w_full.at[s, core], w_full.at[s, core]) for s in range(2)]

    def zero_diag(i, carry):
        qbd[i] = jnp.zeros((hd, wide), BF16)
        dbd[i] = jnp.zeros((hd, wide), BF16)
        return carry
    lax.fori_loop(0, rows, zero_diag, 0)
    for k in (3, 4, 6):
        loads[k].wait()
    head_pick = (lax.broadcasted_iota(jnp.int32, (16, heads), 0) == lax.broadcasted_iota(jnp.int32, (16, heads), 1)).astype(BF16)
    eye = (lax.broadcasted_iota(jnp.int32, (ch, ch), 0) == lax.broadcasted_iota(jnp.int32, (ch, ch), 1)).astype(BF16)

    def to_column(s, place):
        ref = (lns_ref, lnb_ref, bg_ref, bo_ref)[place]
        col[s, place] = jnp.broadcast_to(ref[s:s + 1, :], (n, ch)).T

    def prepare_norm(s):
        wbt[s] = dot(head_pick, wb_ref[s]).astype(BF16)
        to_column(s, 0)
        to_column(s, 1)
    prepare_norm(0)

    def prepare_project(s):
        wpt[s] = wp_ref[s].T
        to_column(s, 2)

    def prepare_late():
        prepare_norm(1)
        prepare_project(1)
        to_column(0, 3)
        to_column(1, 3)
        at16 = lax.broadcasted_iota(jnp.int32, (16, heads * rows), 0)
        at32 = lax.broadcasted_iota(jnp.int32, (16, heads * rows), 1)
        for s in range(2):
            wot[s] = wo_ref[s].T
            w_heads = dot(eye, wbt[s], NT).astype(BF16)
            for i in range(rows):
                wsel[s, i] = dot(w_heads, ((at32 == at16 * rows + i) & (at16 < heads)).astype(BF16)).astype(BF16)

    def column(s, place):
        one = col[s, place]
        return jnp.concatenate([one, one], axis=1)

    def store_diag(ref, t, value):
        for r in range(2):
            for h in range(heads):
                ref[2 * t + r, h * hdim:(h + 1) * hdim, h * n:(h + 1) * n] = value[h * hdim:(h + 1) * hdim, r * n:(r + 1) * n]

    def staged(t):
        return jnp.concatenate([stage[pl.ds(2 * t + r, n, stride=rows), :] for r in range(2)], axis=0)

    def unpack(recv):
        stage[...] = recv[...].astype(F32).reshape(group * rows * rows, ch)

    def pack(send, t, value):
        parts = [value[r * n:(r + 1) * n].reshape(group, n // group, ch) for r in range(2)]
        send[:, pl.ds(pl.multiple_of(t * 16, 16), 16), :] = jnp.concatenate(parts, axis=1).astype(BF16)

    def part_of(some):
        return pl.ds(2 * some[0] * rows, 2 * len(some) * rows)

    def normalize(s, t, x):
        centred = x - jnp.mean(x, axis=0, keepdims=True)
        inv_std = lax.rsqrt(jnp.mean(centred * centred, axis=0, keepdims=True) + EPS)
        x_hat = centred * inv_std
        return (x_hat * column(s, 0) + column(s, 1)).astype(BF16), x_hat, inv_std

    def keep_norm(s, t, x):
        a_t, x_hat, inv_std = normalize(s, t, x)
        xh[s, t] = x_hat
        inv[s, t] = jnp.broadcast_to(inv_std, (8, two))
        b_t = dot(wbt[s], a_t)
        btmp[pl.ds(pl.multiple_of(t * 32, 32), 32), :] = jnp.concatenate([b_t[:, :n], b_t[:, n:]], axis=0)
        return a_t

    def project(s, t, a_t):
        a = a_t.T
        a_s[s, t] = a
        p = dot(wpt[s], a_t).astype(BF16)
        qt[s, t] = p[:hd]
        kt[s, t] = p[hd:2 * hd]
        vt[s, t] = p[2 * hd:3 * hd]
        store_diag(qbd, t, p[:hd])
        g = jax.nn.sigmoid(p[3 * hd:].astype(F32) + column(s, 2))
        g_s[s, t] = g
        kv[s, t] = dot(a, wp_ref[s, :, hd:3 * hd]).astype(BF16)
        return g

    def send_bias(s):
        for h in range(0, heads, 2):
            some = [btmp[pl.ds(h + r, rows, stride=16), :] for r in range(2)]
            b_send[s, h * rows:(h + 2) * rows, :] = jnp.concatenate(some, axis=0).astype(BF16)
        (ex_b0, ex_b1)[s].start()

    def take_bias0():
        ex_b0.wait_recv()
        got = b_recv[...].astype(F32).reshape(group, heads, rows, n)
        for h in range(heads):
            bias[:, h * n:(h + 1) * n] = got[:, h].reshape(n, n).T * LOG2E

    def take_bias1():
        near_b1.wait_recv()
        for c in range(2):
            got = b1_recv[c].astype(F32) * LOG2E
            for chip in range(chips):
                for h in range(heads):
                    at = (2 * chip + c) * rows
                    bias[at:at + rows, h * n:(h + 1) * n] = got[chip, h * rows:(h + 1) * rows]

    def logits(s):
        for i in range(rows):
            t, r = divmod(i, 2)
            fill = maskb[s, i]
            raw = dot(kv[s, t, r * n:(r + 1) * n, :hd], qbd[i])
            for h in range(heads):
                pf[s, i, :, h * n:(h + 1) * n] = raw[:, h * n:(h + 1) * n] * (scale * LOG2E) + fill

    def attend(s, some):
        for i in some:
            t, r = divmod(i, 2)
            for h in range(heads):
                cols = slice(h * n, (h + 1) * n)
                x = pf[s, i, :, cols] + bias[:, cols]
                e = jnp.exp2(x - jnp.max(x, axis=0, keepdims=True))
                p = e * (1.0 / jnp.sum(e, axis=0, keepdims=True))
                pf[s, i, :, cols] = p
                hs = slice(h * hdim, (h + 1) * hdim)
                ot[s, t, hs, r * n:(r + 1) * n] = dot(vt[s, t, hs, r * n:(r + 1) * n], p.astype(BF16))

    def block_out(s, t):
        u = (ot[s, t] * g_s[s, t]).astype(BF16)
        ut[s, t] = u
        return xt[s, t] + dot(wot[s], u) + column(s, 3)

    def attend_bwd(s, some):
        def d_probs(i):
            t, r = divmod(i, 2)
            return dot(kv[s, t, r * n:(r + 1) * n, hd:], dbd[i])
        ahead = d_probs(some[0])
        for k, i in enumerate(some):
            t, r = divmod(i, 2)
            d_p = ahead
            if k + 1 < len(some):
                ahead = d_probs(some[k + 1])
            at = slice(r * n, (r + 1) * n)
            for h in range(heads):
                cols = slice(h * n, (h + 1) * n)
                p = pf[s, i, :, cols]
                d_ph = d_p[:, cols]
                d_l = p * (d_ph - jnp.sum(d_ph * p, axis=0, keepdims=True))
                db[:, cols] += d_l
                d_s = (d_l * scale).astype(BF16)
                hs = slice(h * hdim, (h + 1) * hdim)
                d_q = dot(kt[s, t, hs, at], d_s)
                d_k = dot(qt[s, t, hs, at], d_s, NT)
                d_v = dot(dot_s[t, hs, at], p.astype(BF16), NT)
                dpt[t, h * hdim:(h + 1) * hdim, at] = d_q.astype(BF16)
                dpt[t, hd + h * hdim:hd + (h + 1) * hdim, at] = d_k.astype(BF16)
                dpt[t, 2 * hd + h * hdim:2 * hd + (h + 1) * hdim, at] = d_v.astype(BF16)

    def store_d_o(t, d_o):
        dot_s[t] = d_o
        store_diag(dbd, t, d_o)

    def gate_grad(s, t, gate_sum):
        g = g_s[s, t]
        d_lin = dgt[t] * ot[s, t] * g * (1.0 - g)
        dpt[t, 3 * hd:, :] = d_lin.astype(BF16)
        return gate_sum + d_lin

    def send_weights(s):
        top = wacc[:4 * hd].reshape(2, chips, 4 * hd // group, ch)
        low = wacc[4 * hd:].reshape(2, chips, hd // group, ch)
        w_send[s] = jnp.concatenate([top, low], axis=2).astype(BF16)
        near_w[s].start()

    def chip_sum_weights(s):
        near_w[s].wait_recv()
        w_mid[s] = (w_send[s, core].astype(F32) + w_half[s].astype(F32)).astype(BF16)
        ex_w[s].start()

    def reduce_weights(s):
        ex_w[s].wait_recv()
        w_part[s] = jnp.sum(w_recv[s].astype(F32), axis=0).astype(BF16)
        ex_wf[s].start()

    def forward_weights(s):
        ex_wf[s].wait_recv()
        near_wf[s].start()

    def send_bias_grad(s):
        for h in range(0, heads, 2):
            some = [db[:, (h + r) * n:(h + r + 1) * n] for r in range(2)]
            some = [(one.T if s == 0 else one).reshape(chips, 2, rows, n) for one in some]
            for c in range(2):
                db_send[s, c, :, h * rows:(h + 2) * rows, :] = jnp.concatenate([one[:, c] for one in some], axis=1).astype(BF16)
        near_db[s].start()

    def chip_sum_bias_grad(s):
        near_db[s].wait_recv()
        db_mid[s] = (db_send[s, core].astype(F32) + db_half[s].astype(F32)).astype(BF16)
        ex_db[s].start()

    def take_bias_grad(s):
        ex_db[s].wait_recv()
        return jnp.sum(db_recv[s].astype(F32), axis=0).astype(BF16)

    def bias_terms(s, d_own):
        return [jnp.concatenate([dot(wsel[s, 2 * t + r], d_own) for r in range(2)], axis=1) for t in range(pairs)]

    def head_weight_grad(s, d_own):
        at16 = lax.broadcasted_iota(jnp.int32, (16, heads * rows), 0)
        at32 = lax.broadcasted_iota(jnp.int32, (16, heads * rows), 1)
        for t in range(pairs):
            rows_of = [dot((at32 == at16 * rows + (2 * t + r)).astype(BF16), d_own) for r in range(2)]
            dbt[t] = jnp.concatenate(rows_of, axis=1).astype(BF16)
        total = None
        for t in range(pairs):
            one = dot(dbt[t], a_s[0, t]) if s == 0 else dot(dbt[t], at1[t], NT)
            total = one if total is None else total + one
        return total

    def norm_bwd(s, t, d_n, sums):
        x_hat = xh[s, t]
        d_hat = d_n * column(s, 0)
        along = jnp.mean(d_hat * x_hat, axis=0, keepdims=True)
        d_in = inv[s, t, 0:1, :] * (d_hat - jnp.mean(d_hat, axis=0, keepdims=True) - x_hat * along)
        return d_in, (sums[0] + d_n * x_hat, sums[1] + d_n)

    def lanes_to_row(value):
        return jnp.sum((value[:, :n] + value[:, n:]).T, axis=0, keepdims=True)

    def send_small(s, sums, wb_sum, gate_sum, b_out_row):
        gain_sum, shift_sum = sums
        sm_send[s, 0:1, :] = lanes_to_row(gain_sum)
        sm_send[s, 1:2, :] = lanes_to_row(shift_sum)
        sm_send[s, 2:3, :] = lanes_to_row(gate_sum)
        sm_send[s, 3:4, :] = b_out_row
        sm_send[s, 4:4 + heads, :] = wb_sum[:heads]
        near_small[s].start()

    def chip_sum_small(s):
        near_small[s].wait_recv()
        sm_mid[s] = sm_send[s] + sm_half[s]
        ex_small[s].start()

    zero_tile = jnp.zeros((ch, two), F32)
    early, late = range(pairs // 2), range(pairs // 2, pairs)

    loads[0].wait()
    for t in range(pairs):
        x = jnp.concatenate([z_ref[2 * t + r].astype(F32).T for r in range(2)], axis=1)
        xt[0, t] = x
        at0[t] = keep_norm(0, t, x)
    pl.semaphore_wait(barrier, group - 1)
    send_bias(0)
    loads[5].wait()
    loads[7].wait()
    prepare_project(0)
    for t in range(pairs):
        project(0, t, at0[t])
    for k in (1, 2):
        loads[k].wait()
    b_out_row1 = jnp.zeros((1, ch), F32)
    for t in range(pairs):
        d_y = jnp.concatenate([dz_ref[2 * t + r].astype(F32) for r in range(2)], axis=0)
        pack(dz_send, t, d_y)
        dzt[t] = d_y.T
        b_out_row1 = b_out_row1 + jnp.sum(d_y, axis=0, keepdims=True)
    mk_send[...] = mask_ref[...].astype(F32).astype(BF16)
    ex_dz.start(part_of(early))
    ex_mask.start()
    fill_rows = (mask_ref[...].astype(F32) - 1.0) * (MASK_FILL * LOG2E)
    for i in range(rows):
        maskb[0, i] = jnp.broadcast_to(fill_rows[i:i + 1, :], (n, n)).T
    logits(0)
    loads[8].wait()
    loads[9].wait()
    prepare_late()
    take_bias0()

    for some in (range(1), range(1, pairs)):
        attend(0, range(2 * some[0], 2 * some[-1] + 2))
        for t in some:
            y = block_out(0, t)
            pack(mid_send, t, y.T)
            xt[1, t] = y.astype(BF16).astype(F32)
        ex_mid.start(part_of(some))
    for t in range(pairs):
        at1[t] = keep_norm(1, t, xt[1, t])
    send_bias(1)
    ex_dz.start(part_of(late))

    db[...] = jnp.zeros((n, wide), F32)
    ex_mask.wait_recv()
    whole = mk_recv[...].astype(F32).reshape(n, n).astype(BF16)
    for i in range(rows):
        pick = (lax.broadcasted_iota(jnp.int32, (n, n), 0) == me * rows + i).astype(BF16)
        maskb[1, i] = (dot(whole, pick) - 1.0) * (MASK_FILL * LOG2E)

    ex_mid.wait_recv()
    unpack(mid_recv)
    for t in range(pairs):
        x = staged(t).T
        xt[1, t] = x
        project(1, t, normalize(1, t, x)[0])
    ex_b1.wait_recv()
    near_b1.start()
    logits(1)
    take_bias1()
    attend(1, range(rows // 2))
    for t in early:
        pack(zo_send, t, block_out(1, t).T)
    ex_zo.start(part_of(early))
    attend(1, range(rows // 2, rows))
    ex_dz.wait_recv()
    unpack(dz_recv)
    for t in range(pairs):
        d_low = staged(t).astype(BF16)
        dlp[t] = d_low
        dgt[t] = dot(wo_ref[1], d_low, NT)
    for t in range(pairs):
        store_d_o(t, (dgt[t] * g_s[1, t]).astype(BF16))

    gate_sum1 = zero_tile
    for k, some in enumerate((early, late)):
        attend_bwd(1, range(2 * some[0], 2 * some[-1] + 2))
        if k == 1:
            send_bias_grad(1)
        for t in some:
            gate_sum1 = gate_grad(1, t, gate_sum1)
            pack(dm_send, t, dot(wp_ref[1], dpt[t]).T)
        ex_dm.start(part_of(some))
    for t in late:
        pack(zo_send, t, block_out(1, t).T)
    chip_sum_bias_grad(1)

    def sum_weights(s):
        top, low = None, None
        for t in range(pairs):
            one = dot(dpt[t], a_s[s, t])
            two_ = dot(ut[1, t], dlp[t]) if s == 1 else dot(ut[0, t], dlt[t], NT)
            top, low = (one, two_) if top is None else (top + one, low + two_)
        wacc[:4 * hd] = top
        wacc[4 * hd:] = low
    sum_weights(1)
    send_weights(1)
    db[...] = jnp.zeros((n, wide), F32)
    chip_sum_weights(1)
    ex_zo.start(part_of(late))

    d_own1 = take_bias_grad(1)
    terms = bias_terms(1, d_own1)
    for t in range(pairs):
        dnt[t] = terms[t]
    ex_dm.wait_recv()
    unpack(dm_recv)
    sums1, b_out_sum = (zero_tile, zero_tile), zero_tile
    for t in range(pairs):
        d_in, sums1 = norm_bwd(1, t, staged(t).T + dnt[t], sums1)
        d_y = d_in + dzt[t]
        dmt[t] = d_y
        d_low = d_y.astype(BF16)
        dlt[t] = d_low
        d_gated = dot(wo_ref[0], d_low)
        dgt[t] = d_gated
        store_d_o(t, (d_gated * g_s[0, t]).astype(BF16))
        b_out_sum = b_out_sum + d_y
    gate_sum0 = zero_tile
    for t in range(pairs):
        gate_sum0 = gate_grad(0, t, gate_sum0)

    attend_bwd(0, range(rows))
    send_bias_grad(0)
    sum_weights(0)
    send_weights(0)
    chip_sum_bias_grad(0)
    for t in range(pairs):
        dnt[t] = dot(wp_ref[0], dpt[t])
    send_small(1, sums1, head_weight_grad(1, d_own1), gate_sum1, b_out_row1)
    b_out_row0 = lanes_to_row(b_out_sum)
    chip_sum_weights(0)
    reduce_weights(1)
    chip_sum_small(1)

    d_own0 = take_bias_grad(0)
    terms = bias_terms(0, d_own0)
    sums0 = (zero_tile, zero_tile)
    for t in range(pairs):
        d_in, sums0 = norm_bwd(0, t, dnt[t] + terms[t], sums0)
        d_x = (d_in + dmt[t]).T.astype(BF16)
        for r in range(2):
            zg_out[2 * t + r] = d_x[r * n:(r + 1) * n]
    send_small(0, sums0, head_weight_grad(0, d_own0), gate_sum0, b_out_row0)
    chip_sum_small(0)
    reduce_weights(0)
    forward_weights(1)
    forward_weights(0)

    for one in [ex_zo] + ex_small + near_wf:
        one.wait_recv()
    for one in [ex_b0, ex_b1, near_b1, ex_mid, ex_dz, ex_mask, ex_zo, ex_dm] + near_db + ex_db + near_small + ex_small + near_w + ex_w + ex_wf + near_wf:
        one.wait_send()


def finish(dims, zo_ref, zg_ref, w_ref, sm_ref,
           zo_out, zg_out, lns_out, lnb_out, wp_out, wb_out, bg_out, wo_out, bo_out, stage):
    rows, n, ch, heads, hd, group = dims
    zg_out[...] = zg_ref[...]
    stage[...] = zo_ref[...].astype(F32).reshape(group * rows * rows, ch)
    for i in range(rows):
        zo_out[i] = stage[pl.ds(i, n, stride=rows), :].astype(BF16)
    cut = 4 * hd // group
    for s in range(2):
        full = w_ref[s].astype(F32).reshape(group, 5 * hd // group, ch)
        wp_out[s] = full[:, :cut].reshape(4 * hd, ch).T
        wo_out[s] = full[:, cut:].reshape(hd, ch)
        total = jnp.sum(sm_ref[s], axis=0)
        for place, ref in enumerate((lns_out, lnb_out, bg_out, bo_out)):
            ref[s:s + 1, :] = total[place:place + 1, :]
        wb_out[s] = total[4:4 + heads]


def solution(mesh):
    axis = 'dap'
    group = mesh.shape[axis]
    row_spec = P(('dp', axis), None, None)
    mask_spec = P(('dp', axis), None)
    grad_spec = P('dp')

    def per_device(z, pair_mask, dz_out, ln_scale, ln_shift, w_proj, w_bias, b_gate, w_out, b_out):
        rows, n, ch = z.shape
        heads = w_bias.shape[-1]
        hd = b_gate.shape[-1]
        pairs, two, wide = rows // 2, 2 * n, heads * n
        piece = (group, rows * rows, ch)
        w_rows = 5 * hd // group

        def vmem(shape, dtype):
            return pltpu.VMEM(shape, dtype)

        w_heads = jnp.swapaxes(w_bias, 1, 2)
        like = [z, z, ln_scale, ln_shift, w_proj, w_heads, b_gate, w_out, b_out]
        out_shape = [jax.ShapeDtypeStruct(a.shape, BF16 if k < 2 else F32) for k, a in enumerate(like)]
        chips = group // 2
        mid_shape = [jax.ShapeDtypeStruct(piece, BF16), jax.ShapeDtypeStruct(z.shape, BF16),
                     jax.ShapeDtypeStruct((2, 2, chips, w_rows, ch), BF16), jax.ShapeDtypeStruct((2, chips, 8, ch), F32)]
        tile = (pairs, ch, two)
        scratch = [
            vmem((2, 4 * hd, ch), BF16), vmem((2, ch, hd), BF16), vmem((2, 16, ch), BF16), vmem((2, 4, ch, n), F32),
            vmem((2,) + tile, F32), vmem((2,) + tile, F32), vmem((2, pairs, 8, two), F32), vmem((2, pairs, two, ch), BF16), vmem(tile, BF16), vmem(tile, BF16),
            vmem((2, pairs, hd, two), BF16), vmem((2, pairs, hd, two), BF16), vmem((2, pairs, hd, two), BF16), vmem((2, pairs, two, 2 * hd), BF16),
            vmem((2, pairs, hd, two), F32), vmem((2, pairs, hd, two), F32), vmem((2, pairs, hd, two), BF16), vmem((rows * 16, n), F32),
            vmem((rows, hd, wide), BF16), vmem((rows, hd, wide), BF16), vmem((pairs, hd, two), BF16), vmem((pairs, hd, two), F32),
            vmem((pairs, 4 * hd, two), BF16), vmem(tile, F32), vmem(tile, F32), vmem(tile, F32), vmem((pairs, two, ch), BF16), vmem(tile, BF16),
            vmem((2, rows, n, wide), F32), vmem((n, wide), F32), vmem((n, wide), F32),
            vmem((2, rows, n, n), F32), vmem((group * rows * rows, ch), F32),
            vmem((5 * hd, ch), F32), vmem((2, rows, ch, heads * rows), BF16), vmem((pairs, 16, two), BF16),
            vmem((2, heads * rows, n), BF16), vmem((group, heads * rows, n), BF16), vmem((2, chips, heads * rows, n), BF16), vmem(piece, BF16), vmem(piece, BF16), vmem(piece, BF16), vmem(piece, BF16),
            vmem((rows, n), BF16), vmem((group, rows, n), BF16), vmem(piece, BF16), vmem(piece, BF16), vmem(piece, BF16),
            vmem((2, 2, chips, heads * rows, n), BF16), vmem((2, chips, heads * rows, n), BF16), vmem((2, chips, heads * rows, n), BF16), vmem((2, chips, heads * rows, n), BF16),
            vmem((2, 2, chips, w_rows, ch), BF16), vmem((2, chips, w_rows, ch), BF16), vmem((2, chips, w_rows, ch), BF16), vmem((2, chips, w_rows, ch), BF16),
            vmem((2, w_rows, ch), BF16), vmem((2, 8, ch), F32), vmem((2, 8, ch), F32), vmem((2, 8, ch), F32),
            pltpu.SemaphoreType.DMA((24,)), pltpu.SemaphoreType.DMA((24,)),
        ]
        operands = (z, pair_mask, dz_out, ln_scale, ln_shift, w_proj, w_heads, b_gate, w_out, b_out)
        scratch += [vmem(a.shape, a.dtype) for a in operands] + [pltpu.SemaphoreType.DMA((10,))]
        in_vmem = pl.BlockSpec(memory_space=pltpu.VMEM)
        mid = pl.pallas_call(
            functools.partial(kernel, (rows, n, ch, heads, hd, group, axis)),
            out_shape=mid_shape,
            in_specs=[pl.BlockSpec(memory_space=pltpu.HBM)] * 10,
            out_specs=[in_vmem] * 4,
            scratch_shapes=scratch,
            compiler_params=pltpu.CompilerParams(collective_id=0, has_side_effects=True, vmem_limit_bytes=40 * 1024 * 1024),
        )(*[pltpu.with_memory_space_constraint(a, pltpu.HBM) for a in operands])
        out = pl.pallas_call(
            functools.partial(finish, (rows, n, ch, heads, hd, group)),
            out_shape=out_shape,
            in_specs=[in_vmem] * 4,
            out_specs=[in_vmem] * 9,
            scratch_shapes=[vmem((group * rows * rows, ch), F32)],
            compiler_params=pltpu.CompilerParams(vmem_limit_bytes=16 * 1024 * 1024),
        )(*mid)
        return tuple(out[:5]) + (jnp.swapaxes(out[5], 1, 2),) + tuple(out[6:])

    return jax.shard_map(per_device, mesh=mesh, in_specs=(row_spec, mask_spec, row_spec) + (P(),) * 7,
                         out_specs=(row_spec, row_spec) + (grad_spec,) * 7, check_vma=False)
```

```python
import functools

import jax
import jax.numpy as jnp
from jax import lax
from jax.experimental import pallas as pl
from jax.experimental.pallas import tpu as pltpu
from jax.sharding import PartitionSpec as P

EPS = 1e-5
MASK_FILL = 1e9
LOG2E = 1.4426950408889634
F32 = jnp.float32
BF16 = jnp.bfloat16
NN = (((1,), (0,)), ((), ()))
NT = (((1,), (1,)), ((), ()))


def dot(a, b, dims=NN):
    return lax.dot_general(a, b, dims, preferred_element_type=F32)


def far_first(size):
    order = [size // 2]
    for hop in range(size // 2 - 1, 0, -1):
        order += [hop, size - hop]
    return order


class Exchange:
    def __init__(self, group, axis, send, recv, send_sem, recv_sem, same=False):
        self.group, self.axis, self.send, self.recv = group, axis, send, recv
        self.send_sem, self.recv_sem, self.same = send_sem, recv_sem, same

    def start(self, part=None):
        me = lax.axis_index(self.axis)
        for hop in far_first(self.group):
            peer = lax.rem(me + hop, self.group)
            source = self.send if self.same else self.send.at[peer] if part is None else self.send.at[peer, part]
            pltpu.make_async_remote_copy(
                src_ref=source,
                dst_ref=self.recv.at[me] if part is None else self.recv.at[me, part],
                send_sem=self.send_sem,
                recv_sem=self.recv_sem,
                device_id={self.axis: peer},
                device_id_type=pl.DeviceIdType.MESH,
            ).start()
        if part is None:
            self.recv[me] = self.send[...] if self.same else self.send[me]
        else:
            self.recv[me, part] = self.send[me, part]

    def _all(self):
        some = self.recv.at[pl.ds(0, self.group - 1)]
        return pltpu.make_async_remote_copy(
            src_ref=some,
            dst_ref=some,
            send_sem=self.send_sem,
            recv_sem=self.recv_sem,
            device_id={self.axis: lax.axis_index(self.axis)},
            device_id_type=pl.DeviceIdType.MESH,
        )

    def wait_recv(self):
        self._all().wait_recv()

    def wait_send(self):
        self._all().wait_send()


class ChipExchange:
    def __init__(self, chips, axis, send, recv, send_sem, recv_sem, same=False):
        self.chips, self.axis, self.send, self.recv = chips, axis, send, recv
        self.send_sem, self.recv_sem, self.same = send_sem, recv_sem, same

    def start(self):
        me = lax.axis_index(self.axis)
        chip, core = me // 2, me % 2
        for hop in far_first(self.chips):
            to = lax.rem(chip + hop, self.chips)
            pltpu.make_async_remote_copy(
                src_ref=self.send if self.same else self.send.at[to],
                dst_ref=self.recv.at[chip],
                send_sem=self.send_sem,
                recv_sem=self.recv_sem,
                device_id={self.axis: 2 * to + core},
                device_id_type=pl.DeviceIdType.MESH,
            ).start()
        self.recv[chip] = self.send[...] if self.same else self.send[chip]

    def _all(self):
        some = self.recv.at[pl.ds(0, self.chips - 1)]
        return pltpu.make_async_remote_copy(
            src_ref=some,
            dst_ref=some,
            send_sem=self.send_sem,
            recv_sem=self.recv_sem,
            device_id={self.axis: lax.axis_index(self.axis)},
            device_id_type=pl.DeviceIdType.MESH,
        )

    def wait_recv(self):
        self._all().wait_recv()

    def wait_send(self):
        self._all().wait_send()


def kernel(dims, *refs):
    rows, n, ch, heads, hd, group, axis = dims
    hdim = hd // heads
    scale = hdim ** -0.5
    pairs = rows // 2
    two = 2 * n
    wide = heads * n
    chips = group // 2
    operands = refs[:10]
    local = refs[-11:-1]
    (z_ref, mask_ref, dz_ref, lns_ref, lnb_ref, wp_ref, wb_ref, bg_ref, wo_ref, bo_ref) = local
    load_sems, refs = refs[-1], refs[10:-11]
    (zo_recv, zg_out, w_full, sm_recv,
     wpt, wot, wbt, col,
     xt, xh, inv, a_s, at0, at1, qt, kt, vt, kv, g_s, ot, ut, btmp, qbd, dbd, dot_s, dgt, dpt, dnt, dzt, dmt, dlp, dlt, pf, bias, db, maskb, stage,
     wacc, wsel, dbt,
     b_send, b_recv, b1_recv, mid_send, mid_recv, dz_send, dz_recv, mk_send, mk_recv, zo_send, dm_send, dm_recv,
     db_send, db_half, db_mid, db_recv, w_send, w_half, w_mid, w_recv, w_part, sm_send, sm_half, sm_mid,
     send_sems, recv_sems) = refs
    me = lax.axis_index(axis)
    core = me % 2
    barrier = pltpu.get_barrier_semaphore()
    for hop in far_first(group):
        pl.semaphore_signal(barrier, inc=1, device_id={axis: lax.rem(me + hop, group)},
                            device_id_type=pl.DeviceIdType.MESH)
    loads = [pltpu.make_async_copy(src, dst, load_sems.at[k]) for k, (src, dst) in enumerate(zip(operands, local))]
    for k in (3, 4, 6, 0, 5, 7, 1, 2, 8, 9):
        loads[k].start()

    def exchange(slot, send, recv, same=False):
        return Exchange(group, axis, send, recv, send_sems.at[slot], recv_sems.at[slot], same)

    def chip_exchange(slot, send, recv, same=False):
        return ChipExchange(chips, axis, send, recv, send_sems.at[slot], recv_sems.at[slot], same)

    def to_sibling(slot, send, recv):
        return pltpu.make_async_remote_copy(src_ref=send, dst_ref=recv, send_sem=send_sems.at[slot], recv_sem=recv_sems.at[slot],
                                            device_id={axis: me + 1 - 2 * core}, device_id_type=pl.DeviceIdType.MESH)

    ex_b0 = exchange(0, b_send.at[0], b_recv, True)
    ex_b1 = chip_exchange(1, b_send.at[1], b1_recv.at[core], True)
    near_b1 = to_sibling(19, b1_recv.at[core], b1_recv.at[core])
    ex_mid = exchange(2, mid_send, mid_recv)
    ex_dz = exchange(3, dz_send, dz_recv)
    ex_mask = exchange(4, mk_send, mk_recv, True)
    ex_zo = exchange(5, zo_send, zo_recv)
    ex_dm = exchange(6, dm_send, dm_recv)
    near_db = [to_sibling(7 + s, db_send.at[s, 1 - core], db_half.at[s]) for s in range(2)]
    ex_db = [chip_exchange((20, 23)[s], db_mid.at[s], db_recv.at[s]) for s in range(2)]
    near_small = [to_sibling(9 + s, sm_send.at[s], sm_half.at[s]) for s in range(2)]
    ex_small = [chip_exchange(21 + s, sm_mid.at[s], sm_recv.at[s], True) for s in range(2)]
    near_w = [to_sibling(11 + s, w_send.at[s, 1 - core], w_half.at[s]) for s in range(2)]
    ex_w = [chip_exchange(13 + s, w_mid.at[s], w_recv.at[s]) for s in range(2)]
    ex_wf = [chip_exchange(15 + s, w_part.at[s], w_full.at[s, core], True) for s in range(2)]
    near_wf = [to_sibling(17 + s, w_full.at[s, core], w_full.at[s, core]) for s in range(2)]

    def zero_diag(i, carry):
        qbd[i] = jnp.zeros((hd, wide), BF16)
        dbd[i] = jnp.zeros((hd, wide), BF16)
        return carry
    lax.fori_loop(0, rows, zero_diag, 0)
    for k in (3, 4, 6):
        loads[k].wait()
    head_pick = (lax.broadcasted_iota(jnp.int32, (16, heads), 0) == lax.broadcasted_iota(jnp.int32, (16, heads), 1)).astype(BF16)
    eye = (lax.broadcasted_iota(jnp.int32, (ch, ch), 0) == lax.broadcasted_iota(jnp.int32, (ch, ch), 1)).astype(BF16)

    def to_column(s, place):
        ref = (lns_ref, lnb_ref, bg_ref, bo_ref)[place]
        col[s, place] = jnp.broadcast_to(ref[s:s + 1, :], (n, ch)).T

    def prepare_norm(s):
        wbt[s] = dot(head_pick, wb_ref[s]).astype(BF16)
        to_column(s, 0)
        to_column(s, 1)
    prepare_norm(0)

    def prepare_project(s):
        wpt[s] = wp_ref[s].T
        to_column(s, 2)

    def prepare_late():
        prepare_norm(1)
        prepare_project(1)
        to_column(0, 3)
        to_column(1, 3)
        at16 = lax.broadcasted_iota(jnp.int32, (16, heads * rows), 0)
        at32 = lax.broadcasted_iota(jnp.int32, (16, heads * rows), 1)
        for s in range(2):
            wot[s] = wo_ref[s].T
            w_heads = dot(eye, wbt[s], NT).astype(BF16)
            for i in range(rows):
                wsel[s, i] = dot(w_heads, ((at32 == at16 * rows + i) & (at16 < heads)).astype(BF16)).astype(BF16)

    def column(s, place):
        one = col[s, place]
        return jnp.concatenate([one, one], axis=1)

    def store_diag(ref, t, value):
        for r in range(2):
            for h in range(heads):
                ref[2 * t + r, h * hdim:(h + 1) * hdim, h * n:(h + 1) * n] = value[h * hdim:(h + 1) * hdim, r * n:(r + 1) * n]

    def staged(t):
        return jnp.concatenate([stage[pl.ds(2 * t + r, n, stride=rows), :] for r in range(2)], axis=0)

    def unpack(recv):
        stage[...] = recv[...].astype(F32).reshape(group * rows * rows, ch)

    def pack(send, t, value):
        parts = [value[r * n:(r + 1) * n].reshape(group, n // group, ch) for r in range(2)]
        send[:, pl.ds(pl.multiple_of(t * 16, 16), 16), :] = jnp.concatenate(parts, axis=1).astype(BF16)

    def pair(t):
        return slice(t * two, (t + 1) * two)

    def part_of(some):
        return pl.ds(2 * some[0] * rows, 2 * len(some) * rows)

    def normalize(s, t, x):
        centred = x - jnp.mean(x, axis=0, keepdims=True)
        inv_std = lax.rsqrt(jnp.mean(centred * centred, axis=0, keepdims=True) + EPS)
        x_hat = centred * inv_std
        return (x_hat * column(s, 0) + column(s, 1)).astype(BF16), x_hat, inv_std

    def keep_norm(s, t, x):
        a_t, x_hat, inv_std = normalize(s, t, x)
        xh[s, t] = x_hat
        inv[s, t] = jnp.broadcast_to(inv_std, (8, two))
        b_t = dot(wbt[s], a_t)
        btmp[pl.ds(pl.multiple_of(t * 32, 32), 32), :] = jnp.concatenate([b_t[:, :n], b_t[:, n:]], axis=0)
        return a_t

    def project(s, t, a_t):
        a = a_t.T
        a_s[s, pair(t), :] = a
        p = dot(wpt[s], a_t).astype(BF16)
        qt[s, t] = p[:hd]
        kt[s, t] = p[hd:2 * hd]
        vt[s, t] = p[2 * hd:3 * hd]
        store_diag(qbd, t, p[:hd])
        g = jax.nn.sigmoid(p[3 * hd:].astype(F32) + column(s, 2))
        g_s[s, t] = g
        kv[s, t] = dot(a, wp_ref[s, :, hd:3 * hd]).astype(BF16)
        return g

    def send_bias(s):
        for h in range(0, heads, 2):
            some = [btmp[pl.ds(h + r, rows, stride=16), :] for r in range(2)]
            b_send[s, h * rows:(h + 2) * rows, :] = jnp.concatenate(some, axis=0).astype(BF16)
        (ex_b0, ex_b1)[s].start()

    def take_bias0():
        ex_b0.wait_recv()
        got = b_recv[...].astype(F32).reshape(group, heads, rows, n)
        for h in range(heads):
            bias[:, h * n:(h + 1) * n] = got[:, h].reshape(n, n).T * LOG2E

    def take_bias1():
        near_b1.wait_recv()
        for c in range(2):
            got = b1_recv[c].astype(F32) * LOG2E
            for chip in range(chips):
                for h in range(heads):
                    at = (2 * chip + c) * rows
                    bias[at:at + rows, h * n:(h + 1) * n] = got[chip, h * rows:(h + 1) * rows]

    def logits(s):
        for i in range(rows):
            t, r = divmod(i, 2)
            fill = maskb[s, i]
            raw = dot(kv[s, t, r * n:(r + 1) * n, :hd], qbd[i])
            for h in range(heads):
                pf[s, i, :, h * n:(h + 1) * n] = raw[:, h * n:(h + 1) * n] * (scale * LOG2E) + fill

    def attend(s, some):
        for i in some:
            t, r = divmod(i, 2)
            for h in range(heads):
                cols = slice(h * n, (h + 1) * n)
                x = pf[s, i, :, cols] + bias[:, cols]
                e = jnp.exp2(x - jnp.max(x, axis=0, keepdims=True))
                p = e * (1.0 / jnp.sum(e, axis=0, keepdims=True))
                pf[s, i, :, cols] = p
                hs = slice(h * hdim, (h + 1) * hdim)
                ot[s, t, hs, r * n:(r + 1) * n] = dot(vt[s, t, hs, r * n:(r + 1) * n], p.astype(BF16))

    def block_out(s, t):
        u = (ot[s, t] * g_s[s, t]).astype(BF16)
        ut[s, :, pair(t)] = u
        return xt[s, t] + dot(wot[s], u) + column(s, 3)

    def attend_bwd(s, some):
        def d_probs(i):
            t, r = divmod(i, 2)
            return dot(kv[s, t, r * n:(r + 1) * n, hd:], dbd[i])
        ahead = d_probs(some[0])
        for k, i in enumerate(some):
            t, r = divmod(i, 2)
            d_p = ahead
            if k + 1 < len(some):
                ahead = d_probs(some[k + 1])
            at = slice(r * n, (r + 1) * n)
            here = slice(i * n, (i + 1) * n)
            for h in range(heads):
                cols = slice(h * n, (h + 1) * n)
                p = pf[s, i, :, cols]
                d_ph = d_p[:, cols]
                d_l = p * (d_ph - jnp.sum(d_ph * p, axis=0, keepdims=True))
                db[:, cols] += d_l
                d_s = (d_l * scale).astype(BF16)
                hs = slice(h * hdim, (h + 1) * hdim)
                d_q = dot(kt[s, t, hs, at], d_s)
                d_k = dot(qt[s, t, hs, at], d_s, NT)
                d_v = dot(dot_s[t, hs, at], p.astype(BF16), NT)
                dpt[h * hdim:(h + 1) * hdim, here] = d_q.astype(BF16)
                dpt[hd + h * hdim:hd + (h + 1) * hdim, here] = d_k.astype(BF16)
                dpt[2 * hd + h * hdim:2 * hd + (h + 1) * hdim, here] = d_v.astype(BF16)

    def store_d_o(t, d_o):
        dot_s[t] = d_o
        store_diag(dbd, t, d_o)

    def gate_grad(s, t, gate_sum):
        g = g_s[s, t]
        d_lin = dgt[t] * ot[s, t] * g * (1.0 - g)
        dpt[3 * hd:, pair(t)] = d_lin.astype(BF16)
        return gate_sum + d_lin

    def send_weights(s):
        top = wacc[:4 * hd].reshape(2, chips, 4 * hd // group, ch)
        low = wacc[4 * hd:].reshape(2, chips, hd // group, ch)
        w_send[s] = jnp.concatenate([top, low], axis=2).astype(BF16)
        near_w[s].start()

    def chip_sum_weights(s):
        near_w[s].wait_recv()
        w_mid[s] = (w_send[s, core].astype(F32) + w_half[s].astype(F32)).astype(BF16)
        ex_w[s].start()

    def reduce_weights(s):
        ex_w[s].wait_recv()
        w_part[s] = jnp.sum(w_recv[s].astype(F32), axis=0).astype(BF16)
        ex_wf[s].start()

    def forward_weights(s):
        ex_wf[s].wait_recv()
        near_wf[s].start()

    def send_bias_grad(s):
        for h in range(0, heads, 2):
            some = [db[:, (h + r) * n:(h + r + 1) * n] for r in range(2)]
            some = [(one.T if s == 0 else one).reshape(chips, 2, rows, n) for one in some]
            for c in range(2):
                db_send[s, c, :, h * rows:(h + 2) * rows, :] = jnp.concatenate([one[:, c] for one in some], axis=1).astype(BF16)
        near_db[s].start()

    def chip_sum_bias_grad(s):
        near_db[s].wait_recv()
        db_mid[s] = (db_send[s, core].astype(F32) + db_half[s].astype(F32)).astype(BF16)
        ex_db[s].start()

    def take_bias_grad(s):
        ex_db[s].wait_recv()
        return jnp.sum(db_recv[s].astype(F32), axis=0).astype(BF16)

    def bias_terms(s, d_own):
        return [jnp.concatenate([dot(wsel[s, 2 * t + r], d_own) for r in range(2)], axis=1) for t in range(pairs)]

    def head_weight_grad(s, d_own):
        at16 = lax.broadcasted_iota(jnp.int32, (16, heads * rows), 0)
        at32 = lax.broadcasted_iota(jnp.int32, (16, heads * rows), 1)
        for t in range(pairs):
            rows_of = [dot((at32 == at16 * rows + (2 * t + r)).astype(BF16), d_own) for r in range(2)]
            dbt[:, pair(t)] = jnp.concatenate(rows_of, axis=1).astype(BF16)
        return dot(dbt[...], a_s[0]) if s == 0 else dot(dbt[...], at1[...], NT)

    def norm_bwd(s, t, d_n, sums):
        x_hat = xh[s, t]
        d_hat = d_n * column(s, 0)
        along = jnp.mean(d_hat * x_hat, axis=0, keepdims=True)
        d_in = inv[s, t, 0:1, :] * (d_hat - jnp.mean(d_hat, axis=0, keepdims=True) - x_hat * along)
        return d_in, (sums[0] + d_n * x_hat, sums[1] + d_n)

    def lanes_to_row(value):
        return jnp.sum((value[:, :n] + value[:, n:]).T, axis=0, keepdims=True)

    def send_small(s, sums, wb_sum, gate_sum, b_out_row):
        gain_sum, shift_sum = sums
        sm_send[s, 0:1, :] = lanes_to_row(gain_sum)
        sm_send[s, 1:2, :] = lanes_to_row(shift_sum)
        sm_send[s, 2:3, :] = lanes_to_row(gate_sum)
        sm_send[s, 3:4, :] = b_out_row
        sm_send[s, 4:4 + heads, :] = wb_sum[:heads]
        near_small[s].start()

    def chip_sum_small(s):
        near_small[s].wait_recv()
        sm_mid[s] = sm_send[s] + sm_half[s]
        ex_small[s].start()

    zero_tile = jnp.zeros((ch, two), F32)
    early, late = range(pairs // 2), range(pairs // 2, pairs)

    loads[0].wait()
    for t in range(pairs):
        x = jnp.concatenate([z_ref[2 * t + r].astype(F32).T for r in range(2)], axis=1)
        xt[0, t] = x
        at0[t] = keep_norm(0, t, x)
    pl.semaphore_wait(barrier, group - 1)
    send_bias(0)
    loads[5].wait()
    loads[7].wait()
    prepare_project(0)
    for t in range(pairs):
        project(0, t, at0[t])
    for k in (1, 2):
        loads[k].wait()
    b_out_row1 = jnp.zeros((1, ch), F32)
    for t in range(pairs):
        d_y = jnp.concatenate([dz_ref[2 * t + r].astype(F32) for r in range(2)], axis=0)
        pack(dz_send, t, d_y)
        dzt[t] = d_y.T
        b_out_row1 = b_out_row1 + jnp.sum(d_y, axis=0, keepdims=True)
    mk_send[...] = mask_ref[...].astype(F32).astype(BF16)
    ex_dz.start(part_of(early))
    ex_mask.start()
    fill_rows = (mask_ref[...].astype(F32) - 1.0) * (MASK_FILL * LOG2E)
    for i in range(rows):
        maskb[0, i] = jnp.broadcast_to(fill_rows[i:i + 1, :], (n, n)).T
    logits(0)
    loads[8].wait()
    loads[9].wait()
    prepare_late()
    take_bias0()

    for some in (range(1), range(1, pairs)):
        attend(0, range(2 * some[0], 2 * some[-1] + 2))
        for t in some:
            y = block_out(0, t)
            pack(mid_send, t, y.T)
            xt[1, t] = y.astype(BF16).astype(F32)
        ex_mid.start(part_of(some))
    for t in range(pairs):
        at1[:, pair(t)] = keep_norm(1, t, xt[1, t])
    send_bias(1)
    ex_dz.start(part_of(late))

    db[...] = jnp.zeros((n, wide), F32)
    ex_mask.wait_recv()
    whole = mk_recv[...].astype(F32).reshape(n, n).astype(BF16)
    for i in range(rows):
        pick = (lax.broadcasted_iota(jnp.int32, (n, n), 0) == me * rows + i).astype(BF16)
        maskb[1, i] = (dot(whole, pick) - 1.0) * (MASK_FILL * LOG2E)

    ex_mid.wait_recv()
    unpack(mid_recv)
    for t in range(pairs):
        x = staged(t).T
        xt[1, t] = x
        project(1, t, normalize(1, t, x)[0])
    ex_b1.wait_recv()
    near_b1.start()
    logits(1)
    take_bias1()
    attend(1, range(rows // 2))
    for t in early:
        pack(zo_send, t, block_out(1, t).T)
    ex_zo.start(part_of(early))
    attend(1, range(rows // 2, rows))
    ex_dz.wait_recv()
    unpack(dz_recv)
    for t in range(pairs):
        d_low = staged(t).astype(BF16)
        dlp[pair(t), :] = d_low
        dgt[t] = dot(wo_ref[1], d_low, NT)
    for t in range(pairs):
        store_d_o(t, (dgt[t] * g_s[1, t]).astype(BF16))

    gate_sum1 = zero_tile
    for k, some in enumerate((early, late)):
        attend_bwd(1, range(2 * some[0], 2 * some[-1] + 2))
        if k == 1:
            send_bias_grad(1)
        for t in some:
            gate_sum1 = gate_grad(1, t, gate_sum1)
            pack(dm_send, t, dot(wp_ref[1], dpt[:, pair(t)]).T)
        ex_dm.start(part_of(some))
    for t in late:
        pack(zo_send, t, block_out(1, t).T)
    chip_sum_bias_grad(1)

    def sum_weights(s):
        wacc[:4 * hd] = dot(dpt[...], a_s[s])
        wacc[4 * hd:] = dot(ut[1], dlp[...]) if s == 1 else dot(ut[0], dlt[...], NT)
    sum_weights(1)
    send_weights(1)
    db[...] = jnp.zeros((n, wide), F32)
    chip_sum_weights(1)
    ex_zo.start(part_of(late))

    ex_dm.wait_recv()
    unpack(dm_recv)
    for t in range(pairs):
        dnt[t] = staged(t).T
    d_own1 = take_bias_grad(1)
    terms = bias_terms(1, d_own1)
    sums1, b_out_sum = (zero_tile, zero_tile), zero_tile
    for t in range(pairs):
        d_in, sums1 = norm_bwd(1, t, dnt[t] + terms[t], sums1)
        d_y = d_in + dzt[t]
        dmt[t] = d_y
        d_low = d_y.astype(BF16)
        dlt[:, pair(t)] = d_low
        d_gated = dot(wo_ref[0], d_low)
        dgt[t] = d_gated
        store_d_o(t, (d_gated * g_s[0, t]).astype(BF16))
        b_out_sum = b_out_sum + d_y
    gate_sum0 = zero_tile
    for t in range(pairs):
        gate_sum0 = gate_grad(0, t, gate_sum0)

    attend_bwd(0, range(rows))
    send_bias_grad(0)
    sum_weights(0)
    send_weights(0)
    chip_sum_bias_grad(0)
    for t in range(pairs):
        dnt[t] = dot(wp_ref[0], dpt[:, pair(t)])
    send_small(1, sums1, head_weight_grad(1, d_own1), gate_sum1, b_out_row1)
    b_out_row0 = lanes_to_row(b_out_sum)
    chip_sum_weights(0)
    reduce_weights(1)
    chip_sum_small(1)

    d_own0 = take_bias_grad(0)
    terms = bias_terms(0, d_own0)
    sums0 = (zero_tile, zero_tile)
    for t in range(pairs):
        d_in, sums0 = norm_bwd(0, t, dnt[t] + terms[t], sums0)
        d_x = (d_in + dmt[t]).T.astype(BF16)
        for r in range(2):
            zg_out[2 * t + r] = d_x[r * n:(r + 1) * n]
    send_small(0, sums0, head_weight_grad(0, d_own0), gate_sum0, b_out_row0)
    chip_sum_small(0)
    reduce_weights(0)
    forward_weights(1)
    forward_weights(0)

    for one in [ex_zo] + ex_small + near_wf:
        one.wait_recv()
    for one in [ex_b0, ex_b1, near_b1, ex_mid, ex_dz, ex_mask, ex_zo, ex_dm] + near_db + ex_db + near_small + ex_small + near_w + ex_w + ex_wf + near_wf:
        one.wait_send()


def finish(dims, zo_ref, zg_ref, w_ref, sm_ref,
           zo_out, zg_out, lns_out, lnb_out, wp_out, wb_out, bg_out, wo_out, bo_out, stage):
    rows, n, ch, heads, hd, group = dims
    zg_out[...] = zg_ref[...]
    stage[...] = zo_ref[...].astype(F32).reshape(group * rows * rows, ch)
    for i in range(rows):
        zo_out[i] = stage[pl.ds(i, n, stride=rows), :].astype(BF16)
    cut = 4 * hd // group
    for s in range(2):
        full = w_ref[s].astype(F32).reshape(group, 5 * hd // group, ch)
        wp_out[s] = full[:, :cut].reshape(4 * hd, ch).T
        wo_out[s] = full[:, cut:].reshape(hd, ch)
        total = jnp.sum(sm_ref[s], axis=0)
        for place, ref in enumerate((lns_out, lnb_out, bg_out, bo_out)):
            ref[s:s + 1, :] = total[place:place + 1, :]
        wb_out[s] = total[4:4 + heads]


def solution(mesh):
    axis = 'dap'
    group = mesh.shape[axis]
    row_spec = P(('dp', axis), None, None)
    mask_spec = P(('dp', axis), None)
    grad_spec = P('dp')

    def per_device(z, pair_mask, dz_out, ln_scale, ln_shift, w_proj, w_bias, b_gate, w_out, b_out):
        rows, n, ch = z.shape
        heads = w_bias.shape[-1]
        hd = b_gate.shape[-1]
        pairs, two, wide = rows // 2, 2 * n, heads * n
        piece = (group, rows * rows, ch)
        w_rows = 5 * hd // group

        def vmem(shape, dtype):
            return pltpu.VMEM(shape, dtype)

        w_heads = jnp.swapaxes(w_bias, 1, 2)
        like = [z, z, ln_scale, ln_shift, w_proj, w_heads, b_gate, w_out, b_out]
        out_shape = [jax.ShapeDtypeStruct(a.shape, BF16 if k < 2 else F32) for k, a in enumerate(like)]
        chips = group // 2
        mid_shape = [jax.ShapeDtypeStruct(piece, BF16), jax.ShapeDtypeStruct(z.shape, BF16),
                     jax.ShapeDtypeStruct((2, 2, chips, w_rows, ch), BF16), jax.ShapeDtypeStruct((2, chips, 8, ch), F32)]
        tile = (pairs, ch, two)
        scratch = [
            vmem((2, 4 * hd, ch), BF16), vmem((2, ch, hd), BF16), vmem((2, 16, ch), BF16), vmem((2, 4, ch, n), F32),
            vmem((2,) + tile, F32), vmem((2,) + tile, F32), vmem((2, pairs, 8, two), F32), vmem((2, pairs * two, ch), BF16), vmem(tile, BF16), vmem((ch, pairs * two), BF16),
            vmem((2, pairs, hd, two), BF16), vmem((2, pairs, hd, two), BF16), vmem((2, pairs, hd, two), BF16), vmem((2, pairs, two, 2 * hd), BF16),
            vmem((2, pairs, hd, two), F32), vmem((2, pairs, hd, two), F32), vmem((2, hd, pairs * two), BF16), vmem((rows * 16, n), F32),
            vmem((rows, hd, wide), BF16), vmem((rows, hd, wide), BF16), vmem((pairs, hd, two), BF16), vmem((pairs, hd, two), F32),
            vmem((4 * hd, pairs * two), BF16), vmem(tile, F32), vmem(tile, F32), vmem(tile, F32), vmem((pairs * two, ch), BF16), vmem((ch, pairs * two), BF16),
            vmem((2, rows, n, wide), F32), vmem((n, wide), F32), vmem((n, wide), F32),
            vmem((2, rows, n, n), F32), vmem((group * rows * rows, ch), F32),
            vmem((5 * hd, ch), F32), vmem((2, rows, ch, heads * rows), BF16), vmem((16, pairs * two), BF16),
            vmem((2, heads * rows, n), BF16), vmem((group, heads * rows, n), BF16), vmem((2, chips, heads * rows, n), BF16), vmem(piece, BF16), vmem(piece, BF16), vmem(piece, BF16), vmem(piece, BF16),
            vmem((rows, n), BF16), vmem((group, rows, n), BF16), vmem(piece, BF16), vmem(piece, BF16), vmem(piece, BF16),
            vmem((2, 2, chips, heads * rows, n), BF16), vmem((2, chips, heads * rows, n), BF16), vmem((2, chips, heads * rows, n), BF16), vmem((2, chips, heads * rows, n), BF16),
            vmem((2, 2, chips, w_rows, ch), BF16), vmem((2, chips, w_rows, ch), BF16), vmem((2, chips, w_rows, ch), BF16), vmem((2, chips, w_rows, ch), BF16),
            vmem((2, w_rows, ch), BF16), vmem((2, 8, ch), F32), vmem((2, 8, ch), F32), vmem((2, 8, ch), F32),
            pltpu.SemaphoreType.DMA((24,)), pltpu.SemaphoreType.DMA((24,)),
        ]
        operands = (z, pair_mask, dz_out, ln_scale, ln_shift, w_proj, w_heads, b_gate, w_out, b_out)
        scratch += [vmem(a.shape, a.dtype) for a in operands] + [pltpu.SemaphoreType.DMA((10,))]
        in_vmem = pl.BlockSpec(memory_space=pltpu.VMEM)
        mid = pl.pallas_call(
            functools.partial(kernel, (rows, n, ch, heads, hd, group, axis)),
            out_shape=mid_shape,
            in_specs=[pl.BlockSpec(memory_space=pltpu.HBM)] * 10,
            out_specs=[in_vmem] * 4,
            scratch_shapes=scratch,
            compiler_params=pltpu.CompilerParams(collective_id=0, has_side_effects=True, vmem_limit_bytes=40 * 1024 * 1024),
        )(*[pltpu.with_memory_space_constraint(a, pltpu.HBM) for a in operands])
        out = pl.pallas_call(
            functools.partial(finish, (rows, n, ch, heads, hd, group)),
            out_shape=out_shape,
            in_specs=[in_vmem] * 4,
            out_specs=[in_vmem] * 9,
            scratch_shapes=[vmem((group * rows * rows, ch), F32)],
            compiler_params=pltpu.CompilerParams(vmem_limit_bytes=16 * 1024 * 1024),
        )(*mid)
        return tuple(out[:5]) + (jnp.swapaxes(out[5], 1, 2),) + tuple(out[6:])

    return jax.shard_map(per_device, mesh=mesh, in_specs=(row_spec, mask_spec, row_spec) + (P(),) * 7,
                         out_specs=(row_spec, row_spec) + (grad_spec,) * 7, check_vma=False)
```

```python
import functools

import jax
import jax.numpy as jnp
from jax import lax
from jax.experimental import pallas as pl
from jax.experimental.pallas import tpu as pltpu
from jax.sharding import PartitionSpec as P

EPS = 1e-5
MASK_FILL = 1e9
LOG2E = 1.4426950408889634
F32 = jnp.float32
BF16 = jnp.bfloat16
NN = (((1,), (0,)), ((), ()))
NT = (((1,), (1,)), ((), ()))


def dot(a, b, dims=NN):
    return lax.dot_general(a, b, dims, preferred_element_type=F32)


def far_first(size):
    order = [size // 2]
    for hop in range(size // 2 - 1, 0, -1):
        order += [hop, size - hop]
    return order


class Exchange:
    def __init__(self, group, axis, send, recv, send_sem, recv_sem, same=False):
        self.group, self.axis, self.send, self.recv = group, axis, send, recv
        self.send_sem, self.recv_sem, self.same = send_sem, recv_sem, same

    def start(self, part=None):
        me = lax.axis_index(self.axis)
        for hop in far_first(self.group):
            peer = lax.rem(me + hop, self.group)
            source = self.send if self.same else self.send.at[peer] if part is None else self.send.at[peer, part]
            pltpu.make_async_remote_copy(
                src_ref=source,
                dst_ref=self.recv.at[me] if part is None else self.recv.at[me, part],
                send_sem=self.send_sem,
                recv_sem=self.recv_sem,
                device_id={self.axis: peer},
                device_id_type=pl.DeviceIdType.MESH,
            ).start()
        if part is None:
            self.recv[me] = self.send[...] if self.same else self.send[me]
        else:
            self.recv[me, part] = self.send[me, part]

    def _all(self):
        some = self.recv.at[pl.ds(0, self.group - 1)]
        return pltpu.make_async_remote_copy(
            src_ref=some,
            dst_ref=some,
            send_sem=self.send_sem,
            recv_sem=self.recv_sem,
            device_id={self.axis: lax.axis_index(self.axis)},
            device_id_type=pl.DeviceIdType.MESH,
        )

    def wait_recv(self):
        self._all().wait_recv()

    def wait_send(self):
        self._all().wait_send()


class ChipExchange:
    def __init__(self, chips, axis, send, recv, send_sem, recv_sem, same=False):
        self.chips, self.axis, self.send, self.recv = chips, axis, send, recv
        self.send_sem, self.recv_sem, self.same = send_sem, recv_sem, same

    def start(self):
        me = lax.axis_index(self.axis)
        chip, core = me // 2, me % 2
        for hop in far_first(self.chips):
            to = lax.rem(chip + hop, self.chips)
            pltpu.make_async_remote_copy(
                src_ref=self.send if self.same else self.send.at[to],
                dst_ref=self.recv.at[chip],
                send_sem=self.send_sem,
                recv_sem=self.recv_sem,
                device_id={self.axis: 2 * to + core},
                device_id_type=pl.DeviceIdType.MESH,
            ).start()
        self.recv[chip] = self.send[...] if self.same else self.send[chip]

    def _all(self):
        some = self.recv.at[pl.ds(0, self.chips - 1)]
        return pltpu.make_async_remote_copy(
            src_ref=some,
            dst_ref=some,
            send_sem=self.send_sem,
            recv_sem=self.recv_sem,
            device_id={self.axis: lax.axis_index(self.axis)},
            device_id_type=pl.DeviceIdType.MESH,
        )

    def wait_recv(self):
        self._all().wait_recv()

    def wait_send(self):
        self._all().wait_send()


def kernel(dims, *refs):
    rows, n, ch, heads, hd, group, axis = dims
    hdim = hd // heads
    scale = hdim ** -0.5
    pairs = rows // 2
    two = 2 * n
    wide = heads * n
    chips = group // 2
    operands = refs[:10]
    local = refs[-11:-1]
    (z_ref, mask_ref, dz_ref, lns_ref, lnb_ref, wp_ref, wb_ref, bg_ref, wo_ref, bo_ref) = local
    load_sems, refs = refs[-1], refs[10:-11]
    (zo_recv, zg_out, w_full, sm_recv,
     wpt, wot, wbt, col,
     xt, xh, inv, a_s, at0, at1, qt, kt, vt, kv, g_s, ot, ut, btmp, qbd, dbd, dot_s, dgt, dpt, dnt, dzt, dmt, dlp, dlt, pf, bias, db, maskb, stage,
     wacc, wsel, dbt,
     b_send, b_recv, b1_recv, mid_send, mid_recv, dz_send, dz_recv, mk_send, mk_recv, zo_send, dm_send, dm_recv,
     db_send, db_half, db_mid, db_recv, w_send, w_half, w_mid, w_recv, w_part, sm_send, sm_half, sm_mid,
     send_sems, recv_sems) = refs
    me = lax.axis_index(axis)
    core = me % 2
    barrier = pltpu.get_barrier_semaphore()
    for hop in far_first(group):
        pl.semaphore_signal(barrier, inc=1, device_id={axis: lax.rem(me + hop, group)},
                            device_id_type=pl.DeviceIdType.MESH)
    loads = [pltpu.make_async_copy(src, dst, load_sems.at[k]) for k, (src, dst) in enumerate(zip(operands, local))]
    for k in (3, 4, 6, 0, 5, 7, 1, 2, 8, 9):
        loads[k].start()

    def exchange(slot, send, recv, same=False):
        return Exchange(group, axis, send, recv, send_sems.at[slot], recv_sems.at[slot], same)

    def chip_exchange(slot, send, recv, same=False):
        return ChipExchange(chips, axis, send, recv, send_sems.at[slot], recv_sems.at[slot], same)

    def to_sibling(slot, send, recv):
        return pltpu.make_async_remote_copy(src_ref=send, dst_ref=recv, send_sem=send_sems.at[slot], recv_sem=recv_sems.at[slot],
                                            device_id={axis: me + 1 - 2 * core}, device_id_type=pl.DeviceIdType.MESH)

    ex_b0 = exchange(0, b_send.at[0], b_recv, True)
    ex_b1 = chip_exchange(1, b_send.at[1], b1_recv.at[core], True)
    near_b1 = to_sibling(19, b1_recv.at[core], b1_recv.at[core])
    ex_mid = exchange(2, mid_send, mid_recv)
    ex_dz = exchange(3, dz_send, dz_recv)
    ex_mask = exchange(4, mk_send, mk_recv, True)
    ex_zo = exchange(5, zo_send, zo_recv)
    ex_dm = exchange(6, dm_send, dm_recv)
    near_db = [to_sibling(7 + s, db_send.at[s, 1 - core], db_half.at[s]) for s in range(2)]
    ex_db = [chip_exchange((20, 23)[s], db_mid.at[s], db_recv.at[s]) for s in range(2)]
    near_small = [to_sibling(9 + s, sm_send.at[s], sm_half.at[s]) for s in range(2)]
    ex_small = [chip_exchange(21 + s, sm_mid.at[s], sm_recv.at[s], True) for s in range(2)]
    per = hd // group
    sets = [(1, pl.ds(0, 5 * per)), (0, pl.ds(0, 3 * per)), (0, pl.ds(3 * per, 2 * per))]
    near_w = [to_sibling(11 + k, w_send.at[s, 1 - core, :, at], w_half.at[s, :, at]) for k, (s, at) in enumerate(sets)]
    ex_w = [chip_exchange(14 + k, w_mid.at[s, :, at], w_recv.at[s, :, at]) for k, (s, at) in enumerate(sets)]
    ex_wf = [chip_exchange(24 + k, w_part.at[s, at], w_full.at[s, core, :, at], True) for k, (s, at) in enumerate(sets)]
    near_wf = [to_sibling((17, 18, 27)[k], w_full.at[s, core, :, at], w_full.at[s, core, :, at]) for k, (s, at) in enumerate(sets)]

    def zero_diag(i, carry):
        qbd[i] = jnp.zeros((hd, wide), BF16)
        dbd[i] = jnp.zeros((hd, wide), BF16)
        return carry
    lax.fori_loop(0, rows, zero_diag, 0)
    for k in (3, 4, 6):
        loads[k].wait()
    head_pick = (lax.broadcasted_iota(jnp.int32, (16, heads), 0) == lax.broadcasted_iota(jnp.int32, (16, heads), 1)).astype(BF16)
    eye = (lax.broadcasted_iota(jnp.int32, (ch, ch), 0) == lax.broadcasted_iota(jnp.int32, (ch, ch), 1)).astype(BF16)

    def to_column(s, place):
        ref = (lns_ref, lnb_ref, bg_ref, bo_ref)[place]
        col[s, place] = jnp.broadcast_to(ref[s:s + 1, :], (n, ch)).T

    def prepare_norm(s):
        wbt[s] = dot(head_pick, wb_ref[s]).astype(BF16)
        to_column(s, 0)
        to_column(s, 1)
    prepare_norm(0)

    def prepare_project(s):
        wpt[s] = wp_ref[s].T
        to_column(s, 2)

    def prepare_late():
        prepare_norm(1)
        prepare_project(1)
        to_column(0, 3)
        to_column(1, 3)
        at16 = lax.broadcasted_iota(jnp.int32, (16, heads * rows), 0)
        at32 = lax.broadcasted_iota(jnp.int32, (16, heads * rows), 1)
        for s in range(2):
            wot[s] = wo_ref[s].T
            w_heads = dot(eye, wbt[s], NT).astype(BF16)
            for i in range(rows):
                wsel[s, i] = dot(w_heads, ((at32 == at16 * rows + i) & (at16 < heads)).astype(BF16)).astype(BF16)

    def column(s, place):
        one = col[s, place]
        return jnp.concatenate([one, one], axis=1)

    def store_diag(ref, t, value):
        for r in range(2):
            for h in range(heads):
                ref[2 * t + r, h * hdim:(h + 1) * hdim, h * n:(h + 1) * n] = value[h * hdim:(h + 1) * hdim, r * n:(r + 1) * n]

    def staged(t):
        return jnp.concatenate([stage[pl.ds(2 * t + r, n, stride=rows), :] for r in range(2)], axis=0)

    def unpack(recv):
        stage[...] = recv[...].astype(F32).reshape(group * rows * rows, ch)

    def pack(send, t, value):
        parts = [value[r * n:(r + 1) * n].reshape(group, n // group, ch) for r in range(2)]
        send[:, pl.ds(pl.multiple_of(t * 16, 16), 16), :] = jnp.concatenate(parts, axis=1).astype(BF16)

    def pair(t):
        return slice(t * two, (t + 1) * two)

    def part_of(some):
        return pl.ds(2 * some[0] * rows, 2 * len(some) * rows)

    def normalize(s, t, x):
        centred = x - jnp.mean(x, axis=0, keepdims=True)
        inv_std = lax.rsqrt(jnp.mean(centred * centred, axis=0, keepdims=True) + EPS)
        x_hat = centred * inv_std
        return (x_hat * column(s, 0) + column(s, 1)).astype(BF16), x_hat, inv_std

    def keep_norm(s, t, x):
        a_t, x_hat, inv_std = normalize(s, t, x)
        xh[s, t] = x_hat
        inv[s, t] = jnp.broadcast_to(inv_std, (8, two))
        b_t = dot(wbt[s], a_t)
        btmp[pl.ds(pl.multiple_of(t * 32, 32), 32), :] = jnp.concatenate([b_t[:, :n], b_t[:, n:]], axis=0)
        return a_t

    def project(s, t, a_t):
        a = a_t.T
        a_s[s, pair(t), :] = a
        p = dot(wpt[s], a_t).astype(BF16)
        qt[s, t] = p[:hd]
        kt[s, t] = p[hd:2 * hd]
        vt[s, t] = p[2 * hd:3 * hd]
        store_diag(qbd, t, p[:hd])
        g = jax.nn.sigmoid(p[3 * hd:].astype(F32) + column(s, 2))
        g_s[s, t] = g
        kv[s, t] = dot(a, wp_ref[s, :, hd:3 * hd]).astype(BF16)
        return g

    def send_bias(s):
        for h in range(0, heads, 2):
            some = [btmp[pl.ds(h + r, rows, stride=16), :] for r in range(2)]
            b_send[s, h * rows:(h + 2) * rows, :] = jnp.concatenate(some, axis=0).astype(BF16)
        (ex_b0, ex_b1)[s].start()

    def take_bias0():
        ex_b0.wait_recv()
        got = b_recv[...].astype(F32).reshape(group, heads, rows, n)
        for h in range(heads):
            bias[:, h * n:(h + 1) * n] = got[:, h].reshape(n, n).T * LOG2E

    def take_bias1():
        near_b1.wait_recv()
        for c in range(2):
            got = b1_recv[c].astype(F32) * LOG2E
            for chip in range(chips):
                for h in range(heads):
                    at = (2 * chip + c) * rows
                    bias[at:at + rows, h * n:(h + 1) * n] = got[chip, h * rows:(h + 1) * rows]

    def logits(s):
        for i in range(rows):
            t, r = divmod(i, 2)
            fill = maskb[s, i]
            raw = dot(kv[s, t, r * n:(r + 1) * n, :hd], qbd[i])
            for h in range(heads):
                pf[s, i, :, h * n:(h + 1) * n] = raw[:, h * n:(h + 1) * n] * (scale * LOG2E) + fill

    def attend(s, some):
        for i in some:
            t, r = divmod(i, 2)
            for h in range(heads):
                cols = slice(h * n, (h + 1) * n)
                x = pf[s, i, :, cols] + bias[:, cols]
                e = jnp.exp2(x - jnp.max(x, axis=0, keepdims=True))
                p = e * (1.0 / jnp.sum(e, axis=0, keepdims=True))
                pf[s, i, :, cols] = p
                hs = slice(h * hdim, (h + 1) * hdim)
                ot[s, t, hs, r * n:(r + 1) * n] = dot(vt[s, t, hs, r * n:(r + 1) * n], p.astype(BF16))

    def block_out(s, t):
        u = (ot[s, t] * g_s[s, t]).astype(BF16)
        ut[s, :, pair(t)] = u
        return xt[s, t] + dot(wot[s], u) + column(s, 3)

    def attend_bwd(s, some):
        def d_probs(i):
            t, r = divmod(i, 2)
            return dot(kv[s, t, r * n:(r + 1) * n, hd:], dbd[i])
        ahead = d_probs(some[0])
        for k, i in enumerate(some):
            t, r = divmod(i, 2)
            d_p = ahead
            if k + 1 < len(some):
                ahead = d_probs(some[k + 1])
            at = slice(r * n, (r + 1) * n)
            here = slice(i * n, (i + 1) * n)
            for h in range(heads):
                cols = slice(h * n, (h + 1) * n)
                p = pf[s, i, :, cols]
                d_ph = d_p[:, cols]
                d_l = p * (d_ph - jnp.sum(d_ph * p, axis=0, keepdims=True))
                db[:, cols] += d_l
                d_s = (d_l * scale).astype(BF16)
                hs = slice(h * hdim, (h + 1) * hdim)
                d_q = dot(kt[s, t, hs, at], d_s)
                d_k = dot(qt[s, t, hs, at], d_s, NT)
                d_v = dot(dot_s[t, hs, at], p.astype(BF16), NT)
                dpt[h * hdim:(h + 1) * hdim, here] = d_q.astype(BF16)
                dpt[hd + h * hdim:hd + (h + 1) * hdim, here] = d_k.astype(BF16)
                dpt[2 * hd + h * hdim:2 * hd + (h + 1) * hdim, here] = d_v.astype(BF16)

    def store_d_o(t, d_o):
        dot_s[t] = d_o
        store_diag(dbd, t, d_o)

    def gate_grad(s, t, gate_sum):
        g = g_s[s, t]
        d_lin = dgt[t] * ot[s, t] * g * (1.0 - g)
        dpt[3 * hd:, pair(t)] = d_lin.astype(BF16)
        return gate_sum + d_lin

    def send_weights(k):
        s, at = sets[k]
        parts = [(0, 3 * hd), (3 * hd, hd), (4 * hd, hd)]
        for low, size in (parts, parts[:1], parts[1:])[k]:
            w_send[s, :, :, pl.ds(low // group, size // group), :] = wacc[low:low + size].reshape(2, chips, size // group, ch).astype(BF16)
        near_w[k].start()

    def chip_sum_weights(k):
        s, at = sets[k]
        near_w[k].wait_recv()
        w_mid[s, :, at, :] = (w_send[s, core, :, at, :].astype(F32) + w_half[s, :, at, :].astype(F32)).astype(BF16)
        ex_w[k].start()

    def reduce_weights(k):
        s, at = sets[k]
        ex_w[k].wait_recv()
        w_part[s, at, :] = jnp.sum(w_recv[s, :, at, :].astype(F32), axis=0).astype(BF16)
        ex_wf[k].start()

    def forward_weights(k):
        ex_wf[k].wait_recv()
        near_wf[k].start()

    def send_bias_grad(s):
        for h in range(0, heads, 2):
            some = [db[:, (h + r) * n:(h + r + 1) * n] for r in range(2)]
            some = [(one.T if s == 0 else one).reshape(chips, 2, rows, n) for one in some]
            for c in range(2):
                db_send[s, c, :, h * rows:(h + 2) * rows, :] = jnp.concatenate([one[:, c] for one in some], axis=1).astype(BF16)
        near_db[s].start()

    def chip_sum_bias_grad(s):
        near_db[s].wait_recv()
        db_mid[s] = (db_send[s, core].astype(F32) + db_half[s].astype(F32)).astype(BF16)
        ex_db[s].start()

    def take_bias_grad(s):
        ex_db[s].wait_recv()
        return jnp.sum(db_recv[s].astype(F32), axis=0).astype(BF16)

    def bias_terms(s, d_own):
        return [jnp.concatenate([dot(wsel[s, 2 * t + r], d_own) for r in range(2)], axis=1) for t in range(pairs)]

    def head_weight_grad(s, d_own):
        at16 = lax.broadcasted_iota(jnp.int32, (16, heads * rows), 0)
        at32 = lax.broadcasted_iota(jnp.int32, (16, heads * rows), 1)
        for t in range(pairs):
            rows_of = [dot((at32 == at16 * rows + (2 * t + r)).astype(BF16), d_own) for r in range(2)]
            dbt[:, pair(t)] = jnp.concatenate(rows_of, axis=1).astype(BF16)
        return dot(dbt[...], a_s[0]) if s == 0 else dot(dbt[...], at1[...], NT)

    def norm_bwd(s, t, d_n, sums):
        x_hat = xh[s, t]
        d_hat = d_n * column(s, 0)
        along = jnp.mean(d_hat * x_hat, axis=0, keepdims=True)
        d_in = inv[s, t, 0:1, :] * (d_hat - jnp.mean(d_hat, axis=0, keepdims=True) - x_hat * along)
        return d_in, (sums[0] + d_n * x_hat, sums[1] + d_n)

    def lanes_to_row(value):
        return jnp.sum((value[:, :n] + value[:, n:]).T, axis=0, keepdims=True)

    def send_small(s, sums, wb_sum, gate_sum, b_out_row):
        gain_sum, shift_sum = sums
        sm_send[s, 0:1, :] = lanes_to_row(gain_sum)
        sm_send[s, 1:2, :] = lanes_to_row(shift_sum)
        sm_send[s, 2:3, :] = lanes_to_row(gate_sum)
        sm_send[s, 3:4, :] = b_out_row
        sm_send[s, 4:4 + heads, :] = wb_sum[:heads]
        near_small[s].start()

    def chip_sum_small(s):
        near_small[s].wait_recv()
        sm_mid[s] = sm_send[s] + sm_half[s]
        ex_small[s].start()

    zero_tile = jnp.zeros((ch, two), F32)
    early, late = range(pairs // 2), range(pairs // 2, pairs)

    loads[0].wait()
    for t in range(pairs):
        x = jnp.concatenate([z_ref[2 * t + r].astype(F32).T for r in range(2)], axis=1)
        xt[0, t] = x
        at0[t] = keep_norm(0, t, x)
    pl.semaphore_wait(barrier, group - 1)
    send_bias(0)
    loads[5].wait()
    loads[7].wait()
    prepare_project(0)
    for t in range(pairs):
        project(0, t, at0[t])
    for k in (1, 2):
        loads[k].wait()
    b_out_row1 = jnp.zeros((1, ch), F32)
    for t in range(pairs):
        d_y = jnp.concatenate([dz_ref[2 * t + r].astype(F32) for r in range(2)], axis=0)
        pack(dz_send, t, d_y)
        dzt[t] = d_y.T
        b_out_row1 = b_out_row1 + jnp.sum(d_y, axis=0, keepdims=True)
    mk_send[...] = mask_ref[...].astype(F32).astype(BF16)
    ex_dz.start(part_of(early))
    ex_mask.start()
    fill_rows = (mask_ref[...].astype(F32) - 1.0) * (MASK_FILL * LOG2E)
    for i in range(rows):
        maskb[0, i] = jnp.broadcast_to(fill_rows[i:i + 1, :], (n, n)).T
    logits(0)
    loads[8].wait()
    loads[9].wait()
    prepare_late()
    take_bias0()

    for some in (range(1), range(1, pairs)):
        attend(0, range(2 * some[0], 2 * some[-1] + 2))
        for t in some:
            y = block_out(0, t)
            pack(mid_send, t, y.T)
            xt[1, t] = y.astype(BF16).astype(F32)
        ex_mid.start(part_of(some))
    for t in range(pairs):
        at1[:, pair(t)] = keep_norm(1, t, xt[1, t])
    send_bias(1)
    ex_dz.start(part_of(late))

    db[...] = jnp.zeros((n, wide), F32)
    ex_mask.wait_recv()
    whole = mk_recv[...].astype(F32).reshape(n, n).astype(BF16)
    for i in range(rows):
        pick = (lax.broadcasted_iota(jnp.int32, (n, n), 0) == me * rows + i).astype(BF16)
        maskb[1, i] = (dot(whole, pick) - 1.0) * (MASK_FILL * LOG2E)

    ex_mid.wait_recv()
    unpack(mid_recv)
    for t in range(pairs):
        x = staged(t).T
        xt[1, t] = x
        project(1, t, normalize(1, t, x)[0])
    ex_b1.wait_recv()
    near_b1.start()
    logits(1)
    take_bias1()
    attend(1, range(rows // 2))
    for t in early:
        pack(zo_send, t, block_out(1, t).T)
    ex_zo.start(part_of(early))
    attend(1, range(rows // 2, rows))
    ex_dz.wait_recv()
    unpack(dz_recv)
    for t in range(pairs):
        d_low = staged(t).astype(BF16)
        dlp[pair(t), :] = d_low
        dgt[t] = dot(wo_ref[1], d_low, NT)
    for t in range(pairs):
        store_d_o(t, (dgt[t] * g_s[1, t]).astype(BF16))

    gate_sum1 = zero_tile
    for k, some in enumerate((early, late)):
        attend_bwd(1, range(2 * some[0], 2 * some[-1] + 2))
        if k == 1:
            send_bias_grad(1)
        for t in some:
            gate_sum1 = gate_grad(1, t, gate_sum1)
            pack(dm_send, t, dot(wp_ref[1], dpt[:, pair(t)]).T)
        ex_dm.start(part_of(some))
    for t in late:
        pack(zo_send, t, block_out(1, t).T)
    chip_sum_bias_grad(1)

    wacc[:4 * hd] = dot(dpt[...], a_s[1])
    wacc[4 * hd:] = dot(ut[1], dlp[...])
    send_weights(0)
    db[...] = jnp.zeros((n, wide), F32)
    chip_sum_weights(0)
    ex_zo.start(part_of(late))

    ex_dm.wait_recv()
    unpack(dm_recv)
    for t in range(pairs):
        dnt[t] = staged(t).T
    d_own1 = take_bias_grad(1)
    terms = bias_terms(1, d_own1)
    sums1, b_out_sum = (zero_tile, zero_tile), zero_tile
    for t in range(pairs):
        d_in, sums1 = norm_bwd(1, t, dnt[t] + terms[t], sums1)
        d_y = d_in + dzt[t]
        dmt[t] = d_y
        d_low = d_y.astype(BF16)
        dlt[:, pair(t)] = d_low
        d_gated = dot(wo_ref[0], d_low)
        dgt[t] = d_gated
        store_d_o(t, (d_gated * g_s[0, t]).astype(BF16))
        b_out_sum = b_out_sum + d_y
    gate_sum0 = zero_tile
    for t in range(pairs):
        gate_sum0 = gate_grad(0, t, gate_sum0)
    wacc[3 * hd:4 * hd] = dot(dpt[3 * hd:], a_s[0])
    wacc[4 * hd:] = dot(ut[0], dlt[...], NT)
    send_weights(2)

    attend_bwd(0, range(rows))
    send_bias_grad(0)
    wacc[:3 * hd] = dot(dpt[:3 * hd], a_s[0])
    send_weights(1)
    chip_sum_bias_grad(0)
    chip_sum_weights(2)
    for t in range(pairs):
        dnt[t] = dot(wp_ref[0], dpt[:, pair(t)])
    send_small(1, sums1, head_weight_grad(1, d_own1), gate_sum1, b_out_row1)
    b_out_row0 = lanes_to_row(b_out_sum)
    chip_sum_weights(1)
    reduce_weights(0)
    chip_sum_small(1)

    d_own0 = take_bias_grad(0)
    terms = bias_terms(0, d_own0)
    sums0 = (zero_tile, zero_tile)
    for t in range(pairs):
        d_in, sums0 = norm_bwd(0, t, dnt[t] + terms[t], sums0)
        d_x = (d_in + dmt[t]).T.astype(BF16)
        for r in range(2):
            zg_out[2 * t + r] = d_x[r * n:(r + 1) * n]
    send_small(0, sums0, head_weight_grad(0, d_own0), gate_sum0, b_out_row0)
    reduce_weights(2)
    chip_sum_small(0)
    reduce_weights(1)
    forward_weights(0)
    forward_weights(2)
    forward_weights(1)

    for one in [ex_zo] + ex_small + near_wf:
        one.wait_recv()
    for one in [ex_b0, ex_b1, near_b1, ex_mid, ex_dz, ex_mask, ex_zo, ex_dm] + near_db + ex_db + near_small + ex_small + near_w + ex_w + ex_wf + near_wf:
        one.wait_send()


def finish(dims, zo_ref, zg_ref, w_ref, sm_ref,
           zo_out, zg_out, lns_out, lnb_out, wp_out, wb_out, bg_out, wo_out, bo_out, stage):
    rows, n, ch, heads, hd, group = dims
    zg_out[...] = zg_ref[...]
    stage[...] = zo_ref[...].astype(F32).reshape(group * rows * rows, ch)
    for i in range(rows):
        zo_out[i] = stage[pl.ds(i, n, stride=rows), :].astype(BF16)
    per = hd // group
    for s in range(2):
        full = w_ref[s].astype(F32).reshape(group, 5 * hd // group, ch)
        wp_out[s, :, :3 * hd] = full[:, :3 * per].reshape(3 * hd, ch).T
        wp_out[s, :, 3 * hd:] = full[:, 3 * per:4 * per].reshape(hd, ch).T
        wo_out[s] = full[:, 4 * per:].reshape(hd, ch)
        total = jnp.sum(sm_ref[s], axis=0)
        for place, ref in enumerate((lns_out, lnb_out, bg_out, bo_out)):
            ref[s:s + 1, :] = total[place:place + 1, :]
        wb_out[s] = total[4:4 + heads]


def solution(mesh):
    axis = 'dap'
    group = mesh.shape[axis]
    row_spec = P(('dp', axis), None, None)
    mask_spec = P(('dp', axis), None)
    grad_spec = P('dp')

    def per_device(z, pair_mask, dz_out, ln_scale, ln_shift, w_proj, w_bias, b_gate, w_out, b_out):
        rows, n, ch = z.shape
        heads = w_bias.shape[-1]
        hd = b_gate.shape[-1]
        pairs, two, wide = rows // 2, 2 * n, heads * n
        piece = (group, rows * rows, ch)
        w_rows = 5 * hd // group

        def vmem(shape, dtype):
            return pltpu.VMEM(shape, dtype)

        w_heads = jnp.swapaxes(w_bias, 1, 2)
        like = [z, z, ln_scale, ln_shift, w_proj, w_heads, b_gate, w_out, b_out]
        out_shape = [jax.ShapeDtypeStruct(a.shape, BF16 if k < 2 else F32) for k, a in enumerate(like)]
        chips = group // 2
        mid_shape = [jax.ShapeDtypeStruct(piece, BF16), jax.ShapeDtypeStruct(z.shape, BF16),
                     jax.ShapeDtypeStruct((2, 2, chips, w_rows, ch), BF16), jax.ShapeDtypeStruct((2, chips, 8, ch), F32)]
        tile = (pairs, ch, two)
        scratch = [
            vmem((2, 4 * hd, ch), BF16), vmem((2, ch, hd), BF16), vmem((2, 16, ch), BF16), vmem((2, 4, ch, n), F32),
            vmem((2,) + tile, F32), vmem((2,) + tile, F32), vmem((2, pairs, 8, two), F32), vmem((2, pairs * two, ch), BF16), vmem(tile, BF16), vmem((ch, pairs * two), BF16),
            vmem((2, pairs, hd, two), BF16), vmem((2, pairs, hd, two), BF16), vmem((2, pairs, hd, two), BF16), vmem((2, pairs, two, 2 * hd), BF16),
            vmem((2, pairs, hd, two), F32), vmem((2, pairs, hd, two), F32), vmem((2, hd, pairs * two), BF16), vmem((rows * 16, n), F32),
            vmem((rows, hd, wide), BF16), vmem((rows, hd, wide), BF16), vmem((pairs, hd, two), BF16), vmem((pairs, hd, two), F32),
            vmem((4 * hd, pairs * two), BF16), vmem(tile, F32), vmem(tile, F32), vmem(tile, F32), vmem((pairs * two, ch), BF16), vmem((ch, pairs * two), BF16),
            vmem((2, rows, n, wide), F32), vmem((n, wide), F32), vmem((n, wide), F32),
            vmem((2, rows, n, n), F32), vmem((group * rows * rows, ch), F32),
            vmem((5 * hd, ch), F32), vmem((2, rows, ch, heads * rows), BF16), vmem((16, pairs * two), BF16),
            vmem((2, heads * rows, n), BF16), vmem((group, heads * rows, n), BF16), vmem((2, chips, heads * rows, n), BF16), vmem(piece, BF16), vmem(piece, BF16), vmem(piece, BF16), vmem(piece, BF16),
            vmem((rows, n), BF16), vmem((group, rows, n), BF16), vmem(piece, BF16), vmem(piece, BF16), vmem(piece, BF16),
            vmem((2, 2, chips, heads * rows, n), BF16), vmem((2, chips, heads * rows, n), BF16), vmem((2, chips, heads * rows, n), BF16), vmem((2, chips, heads * rows, n), BF16),
            vmem((2, 2, chips, w_rows, ch), BF16), vmem((2, chips, w_rows, ch), BF16), vmem((2, chips, w_rows, ch), BF16), vmem((2, chips, w_rows, ch), BF16),
            vmem((2, w_rows, ch), BF16), vmem((2, 8, ch), F32), vmem((2, 8, ch), F32), vmem((2, 8, ch), F32),
            pltpu.SemaphoreType.DMA((28,)), pltpu.SemaphoreType.DMA((28,)),
        ]
        operands = (z, pair_mask, dz_out, ln_scale, ln_shift, w_proj, w_heads, b_gate, w_out, b_out)
        scratch += [vmem(a.shape, a.dtype) for a in operands] + [pltpu.SemaphoreType.DMA((10,))]
        in_vmem = pl.BlockSpec(memory_space=pltpu.VMEM)
        mid = pl.pallas_call(
            functools.partial(kernel, (rows, n, ch, heads, hd, group, axis)),
            out_shape=mid_shape,
            in_specs=[pl.BlockSpec(memory_space=pltpu.HBM)] * 10,
            out_specs=[in_vmem] * 4,
            scratch_shapes=scratch,
            compiler_params=pltpu.CompilerParams(collective_id=0, has_side_effects=True, vmem_limit_bytes=40 * 1024 * 1024),
        )(*[pltpu.with_memory_space_constraint(a, pltpu.HBM) for a in operands])
        out = pl.pallas_call(
            functools.partial(finish, (rows, n, ch, heads, hd, group)),
            out_shape=out_shape,
            in_specs=[in_vmem] * 4,
            out_specs=[in_vmem] * 9,
            scratch_shapes=[vmem((group * rows * rows, ch), F32)],
            compiler_params=pltpu.CompilerParams(vmem_limit_bytes=16 * 1024 * 1024),
        )(*mid)
        return tuple(out[:5]) + (jnp.swapaxes(out[5], 1, 2),) + tuple(out[6:])

    return jax.shard_map(per_device, mesh=mesh, in_specs=(row_spec, mask_spec, row_spec) + (P(),) * 7,
                         out_specs=(row_spec, row_spec) + (grad_spec,) * 7, check_vma=False)
```

```python
import functools

import jax
import jax.numpy as jnp
from jax import lax
from jax.experimental import pallas as pl
from jax.experimental.pallas import tpu as pltpu
from jax.sharding import PartitionSpec as P

EPS = 1e-5
MASK_FILL = 1e9
LOG2E = 1.4426950408889634
F32 = jnp.float32
BF16 = jnp.bfloat16
NN = (((1,), (0,)), ((), ()))
NT = (((1,), (1,)), ((), ()))


def dot(a, b, dims=NN):
    return lax.dot_general(a, b, dims, preferred_element_type=F32)


def far_first(size):
    order = [size // 2]
    for hop in range(size // 2 - 1, 0, -1):
        order += [hop, size - hop]
    return order


class Exchange:
    def __init__(self, group, axis, send, recv, send_sem, recv_sem, same=False):
        self.group, self.axis, self.send, self.recv = group, axis, send, recv
        self.send_sem, self.recv_sem, self.same = send_sem, recv_sem, same

    def start(self, part=None):
        me = lax.axis_index(self.axis)
        for hop in far_first(self.group):
            peer = lax.rem(me + hop, self.group)
            source = self.send if self.same else self.send.at[peer] if part is None else self.send.at[peer, part]
            pltpu.make_async_remote_copy(
                src_ref=source,
                dst_ref=self.recv.at[me] if part is None else self.recv.at[me, part],
                send_sem=self.send_sem,
                recv_sem=self.recv_sem,
                device_id={self.axis: peer},
                device_id_type=pl.DeviceIdType.MESH,
            ).start()
        if part is None:
            self.recv[me] = self.send[...] if self.same else self.send[me]
        else:
            self.recv[me, part] = self.send[me, part]

    def _all(self):
        some = self.recv.at[pl.ds(0, self.group - 1)]
        return pltpu.make_async_remote_copy(
            src_ref=some,
            dst_ref=some,
            send_sem=self.send_sem,
            recv_sem=self.recv_sem,
            device_id={self.axis: lax.axis_index(self.axis)},
            device_id_type=pl.DeviceIdType.MESH,
        )

    def wait_recv(self):
        self._all().wait_recv()

    def wait_send(self):
        self._all().wait_send()


class ChipExchange:
    def __init__(self, chips, axis, send, recv, send_sem, recv_sem, same=False):
        self.chips, self.axis, self.send, self.recv = chips, axis, send, recv
        self.send_sem, self.recv_sem, self.same = send_sem, recv_sem, same

    def start(self):
        me = lax.axis_index(self.axis)
        chip, core = me // 2, me % 2
        for hop in far_first(self.chips):
            to = lax.rem(chip + hop, self.chips)
            pltpu.make_async_remote_copy(
                src_ref=self.send if self.same else self.send.at[to],
                dst_ref=self.recv.at[chip],
                send_sem=self.send_sem,
                recv_sem=self.recv_sem,
                device_id={self.axis: 2 * to + core},
                device_id_type=pl.DeviceIdType.MESH,
            ).start()
        self.recv[chip] = self.send[...] if self.same else self.send[chip]

    def _all(self):
        some = self.recv.at[pl.ds(0, self.chips - 1)]
        return pltpu.make_async_remote_copy(
            src_ref=some,
            dst_ref=some,
            send_sem=self.send_sem,
            recv_sem=self.recv_sem,
            device_id={self.axis: lax.axis_index(self.axis)},
            device_id_type=pl.DeviceIdType.MESH,
        )

    def wait_recv(self):
        self._all().wait_recv()

    def wait_send(self):
        self._all().wait_send()


def kernel(dims, *refs):
    rows, n, ch, heads, hd, group, axis = dims
    hdim = hd // heads
    scale = hdim ** -0.5
    pairs = rows // 2
    two = 2 * n
    wide = heads * n
    chips = group // 2
    operands = refs[:10]
    local = refs[-11:-1]
    (z_ref, mask_ref, dz_ref, lns_ref, lnb_ref, wp_ref, wb_ref, bg_ref, wo_ref, bo_ref) = local
    load_sems, refs = refs[-1], refs[10:-11]
    (zo_recv, zg_out, w_full, sm_recv,
     wpt, wot, wbt, col,
     xt, xh, inv, a_s, at0, at1, qt, kt, vt, kv, g_s, ot, ut, btmp, qbd, dbd, dot_s, dgt, dpt, dnt, dzt, dmt, dlp, dlt, pf, bias, db, maskb, stage,
     wacc, wsel, dbt,
     b_send, b_recv, b1_recv, mid_send, mid_recv, dz_send, dz_recv, mk_send, mk_recv, zo_send, dm_send, dm_recv,
     db_send, db_half, db_mid, db_recv, w_send, w_half, w_mid, w_recv, w_part, sm_send, sm_half, sm_mid,
     send_sems, recv_sems) = refs
    me = lax.axis_index(axis)
    core = me % 2
    barrier = pltpu.get_barrier_semaphore()
    for hop in far_first(group):
        pl.semaphore_signal(barrier, inc=1, device_id={axis: lax.rem(me + hop, group)},
                            device_id_type=pl.DeviceIdType.MESH)
    loads = [pltpu.make_async_copy(src, dst, load_sems.at[k]) for k, (src, dst) in enumerate(zip(operands, local))]
    for k in (3, 4, 6, 0, 5, 7, 1, 2, 8, 9):
        loads[k].start()

    def exchange(slot, send, recv, same=False):
        return Exchange(group, axis, send, recv, send_sems.at[slot], recv_sems.at[slot], same)

    def chip_exchange(slot, send, recv, same=False):
        return ChipExchange(chips, axis, send, recv, send_sems.at[slot], recv_sems.at[slot], same)

    def to_sibling(slot, send, recv):
        return pltpu.make_async_remote_copy(src_ref=send, dst_ref=recv, send_sem=send_sems.at[slot], recv_sem=recv_sems.at[slot],
                                            device_id={axis: me + 1 - 2 * core}, device_id_type=pl.DeviceIdType.MESH)

    ex_b0 = exchange(0, b_send.at[0], b_recv, True)
    ex_b1 = chip_exchange(1, b_send.at[1], b1_recv.at[core], True)
    near_b1 = to_sibling(19, b1_recv.at[core], b1_recv.at[core])
    ex_mid = exchange(2, mid_send, mid_recv)
    ex_dz = exchange(3, dz_send, dz_recv)
    ex_mask = exchange(4, mk_send, mk_recv, True)
    ex_zo = exchange(5, zo_send, zo_recv)
    ex_dm = exchange(6, dm_send, dm_recv)
    near_db = [to_sibling(7 + s, db_send.at[s, 1 - core], db_half.at[s]) for s in range(2)]
    ex_db = [chip_exchange((20, 23)[s], db_mid.at[s], db_recv.at[s]) for s in range(2)]
    near_small = [to_sibling(9 + s, sm_send.at[s], sm_half.at[s]) for s in range(2)]
    ex_small = [chip_exchange(21 + s, sm_mid.at[s], sm_recv.at[s], True) for s in range(2)]
    near_w = [to_sibling(11 + s, w_send.at[s, 1 - core], w_half.at[s]) for s in range(2)]
    ex_w = [chip_exchange(13 + s, w_mid.at[s], w_recv.at[s]) for s in range(2)]
    ex_wf = [chip_exchange(15 + s, w_part.at[s], w_full.at[s, core], True) for s in range(2)]
    near_wf = [to_sibling(17 + s, w_full.at[s, core], w_full.at[s, core]) for s in range(2)]

    def zero_diag(i, carry):
        qbd[i] = jnp.zeros((hd, wide), BF16)
        dbd[i] = jnp.zeros((hd, wide), BF16)
        return carry
    lax.fori_loop(0, rows, zero_diag, 0)
    for k in (3, 4, 6):
        loads[k].wait()
    head_pick = (lax.broadcasted_iota(jnp.int32, (16, heads), 0) == lax.broadcasted_iota(jnp.int32, (16, heads), 1)).astype(BF16)
    eye = (lax.broadcasted_iota(jnp.int32, (ch, ch), 0) == lax.broadcasted_iota(jnp.int32, (ch, ch), 1)).astype(BF16)

    def to_column(s, place):
        ref = (lns_ref, lnb_ref, bg_ref, bo_ref)[place]
        col[s, place] = jnp.broadcast_to(ref[s:s + 1, :], (n, ch)).T

    def prepare_norm(s):
        wbt[s] = dot(head_pick, wb_ref[s]).astype(BF16)
        to_column(s, 0)
        to_column(s, 1)
    prepare_norm(0)

    def prepare_project(s):
        wpt[s] = wp_ref[s].T
        to_column(s, 2)

    def prepare_late():
        prepare_norm(1)
        prepare_project(1)
        to_column(0, 3)
        to_column(1, 3)
        at16 = lax.broadcasted_iota(jnp.int32, (16, heads * rows), 0)
        at32 = lax.broadcasted_iota(jnp.int32, (16, heads * rows), 1)
        for s in range(2):
            wot[s] = wo_ref[s].T
            w_heads = dot(eye, wbt[s], NT).astype(BF16)
            for i in range(rows):
                wsel[s, i] = dot(w_heads, ((at32 == at16 * rows + i) & (at16 < heads)).astype(BF16)).astype(BF16)

    def column(s, place):
        one = col[s, place]
        return jnp.concatenate([one, one], axis=1)

    def store_diag(ref, t, value):
        for r in range(2):
            for h in range(heads):
                ref[2 * t + r, h * hdim:(h + 1) * hdim, h * n:(h + 1) * n] = value[h * hdim:(h + 1) * hdim, r * n:(r + 1) * n]

    def staged(t):
        return jnp.concatenate([stage[pl.ds(2 * t + r, n, stride=rows), :] for r in range(2)], axis=0)

    def unpack(recv):
        stage[...] = recv[...].astype(F32).reshape(group * rows * rows, ch)

    def pack(send, t, value):
        parts = [value[r * n:(r + 1) * n].reshape(group, n // group, ch) for r in range(2)]
        send[:, pl.ds(pl.multiple_of(t * 16, 16), 16), :] = jnp.concatenate(parts, axis=1).astype(BF16)

    def pair(t):
        return slice(t * two, (t + 1) * two)

    def part_of(some):
        return pl.ds(2 * some[0] * rows, 2 * len(some) * rows)

    def normalize(s, t, x):
        centred = x - jnp.mean(x, axis=0, keepdims=True)
        inv_std = lax.rsqrt(jnp.mean(centred * centred, axis=0, keepdims=True) + EPS)
        x_hat = centred * inv_std
        return (x_hat * column(s, 0) + column(s, 1)).astype(BF16), x_hat, inv_std

    def keep_norm(s, t, x):
        a_t, x_hat, inv_std = normalize(s, t, x)
        xh[s, t] = x_hat
        inv[s, t] = jnp.broadcast_to(inv_std, (8, two))
        b_t = dot(wbt[s], a_t)
        btmp[pl.ds(pl.multiple_of(t * 32, 32), 32), :] = jnp.concatenate([b_t[:, :n], b_t[:, n:]], axis=0)
        return a_t

    def project(s, t, a_t):
        a = a_t.T
        a_s[s, pair(t), :] = a
        p = dot(wpt[s], a_t).astype(BF16)
        qt[s, t] = p[:hd]
        kt[s, t] = p[hd:2 * hd]
        vt[s, t] = p[2 * hd:3 * hd]
        store_diag(qbd, t, p[:hd])
        g = jax.nn.sigmoid(p[3 * hd:].astype(F32) + column(s, 2))
        g_s[s, t] = g
        kv[s, t] = dot(a, wp_ref[s, :, hd:3 * hd]).astype(BF16)
        return g

    def send_bias(s):
        for h in range(0, heads, 2):
            some = [btmp[pl.ds(h + r, rows, stride=16), :] for r in range(2)]
            b_send[s, h * rows:(h + 2) * rows, :] = jnp.concatenate(some, axis=0).astype(BF16)
        (ex_b0, ex_b1)[s].start()

    def take_bias0():
        ex_b0.wait_recv()
        got = b_recv[...].astype(F32).reshape(group, heads, rows, n)
        for h in range(heads):
            bias[:, h * n:(h + 1) * n] = got[:, h].reshape(n, n).T * LOG2E

    def take_bias1():
        near_b1.wait_recv()
        for c in range(2):
            got = b1_recv[c].astype(F32) * LOG2E
            for chip in range(chips):
                for h in range(heads):
                    at = (2 * chip + c) * rows
                    bias[at:at + rows, h * n:(h + 1) * n] = got[chip, h * rows:(h + 1) * rows]

    def logits(s):
        for i in range(rows):
            t, r = divmod(i, 2)
            fill = maskb[s, i]
            raw = dot(kv[s, t, r * n:(r + 1) * n, :hd], qbd[i])
            for h in range(heads):
                pf[s, i, :, h * n:(h + 1) * n] = raw[:, h * n:(h + 1) * n] * (scale * LOG2E) + fill

    def attend(s, some):
        for i in some:
            t, r = divmod(i, 2)
            for h in range(heads):
                cols = slice(h * n, (h + 1) * n)
                x = pf[s, i, :, cols] + bias[:, cols]
                e = jnp.exp2(x - jnp.max(x, axis=0, keepdims=True))
                p = e * (1.0 / jnp.sum(e, axis=0, keepdims=True))
                pf[s, i, :, cols] = p
                hs = slice(h * hdim, (h + 1) * hdim)
                ot[s, t, hs, r * n:(r + 1) * n] = dot(vt[s, t, hs, r * n:(r + 1) * n], p.astype(BF16))

    def block_out(s, t):
        u = (ot[s, t] * g_s[s, t]).astype(BF16)
        ut[s, :, pair(t)] = u
        return xt[s, t] + dot(wot[s], u) + column(s, 3)

    def attend_bwd(s, some):
        def d_probs(i):
            t, r = divmod(i, 2)
            return dot(kv[s, t, r * n:(r + 1) * n, hd:], dbd[i])
        ahead = d_probs(some[0])
        for k, i in enumerate(some):
            t, r = divmod(i, 2)
            d_p = ahead
            if k + 1 < len(some):
                ahead = d_probs(some[k + 1])
            at = slice(r * n, (r + 1) * n)
            here = slice(i * n, (i + 1) * n)
            for h in range(heads):
                cols = slice(h * n, (h + 1) * n)
                p = pf[s, i, :, cols]
                d_ph = d_p[:, cols]
                d_l = p * (d_ph - jnp.sum(d_ph * p, axis=0, keepdims=True))
                db[:, cols] += d_l
                d_s = (d_l * scale).astype(BF16)
                hs = slice(h * hdim, (h + 1) * hdim)
                d_q = dot(kt[s, t, hs, at], d_s)
                d_k = dot(qt[s, t, hs, at], d_s, NT)
                d_v = dot(dot_s[t, hs, at], p.astype(BF16), NT)
                dpt[h * hdim:(h + 1) * hdim, here] = d_q.astype(BF16)
                dpt[hd + h * hdim:hd + (h + 1) * hdim, here] = d_k.astype(BF16)
                dpt[2 * hd + h * hdim:2 * hd + (h + 1) * hdim, here] = d_v.astype(BF16)

    def store_d_o(t, d_o):
        dot_s[t] = d_o
        store_diag(dbd, t, d_o)

    def gate_grad(s, t, gate_sum):
        g = g_s[s, t]
        d_lin = dgt[t] * ot[s, t] * g * (1.0 - g)
        dpt[3 * hd:, pair(t)] = d_lin.astype(BF16)
        return gate_sum + d_lin

    def send_weights(s):
        top = wacc[:4 * hd].reshape(2, chips, 4 * hd // group, ch)
        low = wacc[4 * hd:].reshape(2, chips, hd // group, ch)
        w_send[s] = jnp.concatenate([top, low], axis=2).astype(BF16)
        near_w[s].start()

    def chip_sum_weights(s):
        near_w[s].wait_recv()
        w_mid[s] = (w_send[s, core].astype(F32) + w_half[s].astype(F32)).astype(BF16)
        ex_w[s].start()

    def reduce_weights(s):
        ex_w[s].wait_recv()
        w_part[s] = jnp.sum(w_recv[s].astype(F32), axis=0).astype(BF16)
        ex_wf[s].start()

    def forward_weights(s):
        ex_wf[s].wait_recv()
        near_wf[s].start()

    def send_bias_grad(s):
        for h in range(0, heads, 2):
            some = [db[:, (h + r) * n:(h + r + 1) * n] for r in range(2)]
            some = [(one.T if s == 0 else one).reshape(chips, 2, rows, n) for one in some]
            for c in range(2):
                db_send[s, c, :, h * rows:(h + 2) * rows, :] = jnp.concatenate([one[:, c] for one in some], axis=1).astype(BF16)
        near_db[s].start()

    def chip_sum_bias_grad(s):
        near_db[s].wait_recv()
        db_mid[s] = (db_send[s, core].astype(F32) + db_half[s].astype(F32)).astype(BF16)
        ex_db[s].start()

    def take_bias_grad(s):
        ex_db[s].wait_recv()
        return jnp.sum(db_recv[s].astype(F32), axis=0).astype(BF16)

    def bias_terms(s, d_own):
        return [jnp.concatenate([dot(wsel[s, 2 * t + r], d_own) for r in range(2)], axis=1) for t in range(pairs)]

    def head_weight_grad(s, d_own):
        at16 = lax.broadcasted_iota(jnp.int32, (16, heads * rows), 0)
        at32 = lax.broadcasted_iota(jnp.int32, (16, heads * rows), 1)
        for t in range(pairs):
            rows_of = [dot((at32 == at16 * rows + (2 * t + r)).astype(BF16), d_own) for r in range(2)]
            dbt[:, pair(t)] = jnp.concatenate(rows_of, axis=1).astype(BF16)
        return dot(dbt[...], a_s[0]) if s == 0 else dot(dbt[...], at1[...], NT)

    def norm_bwd(s, t, d_n, sums):
        x_hat = xh[s, t]
        d_hat = d_n * column(s, 0)
        along = jnp.mean(d_hat * x_hat, axis=0, keepdims=True)
        d_in = inv[s, t, 0:1, :] * (d_hat - jnp.mean(d_hat, axis=0, keepdims=True) - x_hat * along)
        return d_in, (sums[0] + d_n * x_hat, sums[1] + d_n)

    def lanes_to_row(value):
        return jnp.sum((value[:, :n] + value[:, n:]).T, axis=0, keepdims=True)

    def send_small(s, sums, wb_sum, gate_sum, b_out_row):
        gain_sum, shift_sum = sums
        sm_send[s, 0:1, :] = lanes_to_row(gain_sum)
        sm_send[s, 1:2, :] = lanes_to_row(shift_sum)
        sm_send[s, 2:3, :] = lanes_to_row(gate_sum)
        sm_send[s, 3:4, :] = b_out_row
        sm_send[s, 4:4 + heads, :] = wb_sum[:heads]
        near_small[s].start()

    def chip_sum_small(s):
        near_small[s].wait_recv()
        sm_mid[s] = sm_send[s] + sm_half[s]
        ex_small[s].start()

    zero_tile = jnp.zeros((ch, two), F32)
    early, late = range(pairs // 2), range(pairs // 2, pairs)

    loads[0].wait()
    for t in range(pairs):
        x = jnp.concatenate([z_ref[2 * t + r].astype(F32).T for r in range(2)], axis=1)
        xt[0, t] = x
        at0[t] = keep_norm(0, t, x)
    pl.semaphore_wait(barrier, group - 1)
    send_bias(0)
    loads[5].wait()
    loads[7].wait()
    prepare_project(0)
    for t in range(pairs):
        project(0, t, at0[t])
    for k in (1, 2):
        loads[k].wait()
    b_out_row1 = jnp.zeros((1, ch), F32)
    for t in range(pairs):
        d_y = jnp.concatenate([dz_ref[2 * t + r].astype(F32) for r in range(2)], axis=0)
        pack(dz_send, t, d_y)
        dzt[t] = d_y.T
        b_out_row1 = b_out_row1 + jnp.sum(d_y, axis=0, keepdims=True)
    mk_send[...] = mask_ref[...].astype(F32).astype(BF16)
    fill_rows = (mask_ref[...].astype(F32) - 1.0) * (MASK_FILL * LOG2E)
    for i in range(rows):
        maskb[0, i] = jnp.broadcast_to(fill_rows[i:i + 1, :], (n, n)).T
    logits(0)
    loads[8].wait()
    loads[9].wait()
    prepare_late()
    ex_dz.start(part_of(early))
    ex_mask.start()
    take_bias0()

    for some in (range(1), range(1, pairs)):
        attend(0, range(2 * some[0], 2 * some[-1] + 2))
        for t in some:
            y = block_out(0, t)
            pack(mid_send, t, y.T)
            xt[1, t] = y.astype(BF16).astype(F32)
        ex_mid.start(part_of(some))
    for t in range(pairs):
        at1[:, pair(t)] = keep_norm(1, t, xt[1, t])
    send_bias(1)
    ex_dz.start(part_of(late))

    db[...] = jnp.zeros((n, wide), F32)
    ex_mask.wait_recv()
    whole = mk_recv[...].astype(F32).reshape(n, n).astype(BF16)
    for i in range(rows):
        pick = (lax.broadcasted_iota(jnp.int32, (n, n), 0) == me * rows + i).astype(BF16)
        maskb[1, i] = (dot(whole, pick) - 1.0) * (MASK_FILL * LOG2E)

    ex_mid.wait_recv()
    unpack(mid_recv)
    for t in range(pairs):
        x = staged(t).T
        xt[1, t] = x
        project(1, t, normalize(1, t, x)[0])
    ex_b1.wait_recv()
    near_b1.start()
    logits(1)
    take_bias1()
    attend(1, range(rows // 2))
    for t in early:
        pack(zo_send, t, block_out(1, t).T)
    ex_zo.start(part_of(early))
    attend(1, range(rows // 2, rows))
    ex_dz.wait_recv()
    unpack(dz_recv)
    for t in range(pairs):
        d_low = staged(t).astype(BF16)
        dlp[pair(t), :] = d_low
        dgt[t] = dot(wo_ref[1], d_low, NT)
    for t in range(pairs):
        store_d_o(t, (dgt[t] * g_s[1, t]).astype(BF16))

    gate_sum1 = zero_tile
    for k, some in enumerate((early, late)):
        attend_bwd(1, range(2 * some[0], 2 * some[-1] + 2))
        if k == 1:
            send_bias_grad(1)
        for t in some:
            gate_sum1 = gate_grad(1, t, gate_sum1)
            pack(dm_send, t, dot(wp_ref[1], dpt[:, pair(t)]).T)
        ex_dm.start(part_of(some))
    for t in late:
        pack(zo_send, t, block_out(1, t).T)
    chip_sum_bias_grad(1)

    def sum_weights(s):
        wacc[:4 * hd] = dot(dpt[...], a_s[s])
        wacc[4 * hd:] = dot(ut[1], dlp[...]) if s == 1 else dot(ut[0], dlt[...], NT)
    sum_weights(1)
    send_weights(1)
    db[...] = jnp.zeros((n, wide), F32)
    chip_sum_weights(1)
    ex_zo.start(part_of(late))

    ex_dm.wait_recv()
    unpack(dm_recv)
    for t in range(pairs):
        dnt[t] = staged(t).T
    d_own1 = take_bias_grad(1)
    terms = bias_terms(1, d_own1)
    sums1, b_out_sum = (zero_tile, zero_tile), zero_tile
    for t in range(pairs):
        d_in, sums1 = norm_bwd(1, t, dnt[t] + terms[t], sums1)
        d_y = d_in + dzt[t]
        dmt[t] = d_y
        d_low = d_y.astype(BF16)
        dlt[:, pair(t)] = d_low
        d_gated = dot(wo_ref[0], d_low)
        dgt[t] = d_gated
        store_d_o(t, (d_gated * g_s[0, t]).astype(BF16))
        b_out_sum = b_out_sum + d_y
    gate_sum0 = zero_tile
    for t in range(pairs):
        gate_sum0 = gate_grad(0, t, gate_sum0)

    attend_bwd(0, range(rows))
    send_bias_grad(0)
    sum_weights(0)
    send_weights(0)
    chip_sum_bias_grad(0)
    for t in range(pairs):
        dnt[t] = dot(wp_ref[0], dpt[:, pair(t)])
    send_small(1, sums1, head_weight_grad(1, d_own1), gate_sum1, b_out_row1)
    b_out_row0 = lanes_to_row(b_out_sum)
    chip_sum_weights(0)
    reduce_weights(1)
    chip_sum_small(1)

    d_own0 = take_bias_grad(0)
    terms = bias_terms(0, d_own0)
    sums0 = (zero_tile, zero_tile)
    for t in range(pairs):
        d_in, sums0 = norm_bwd(0, t, dnt[t] + terms[t], sums0)
        d_x = (d_in + dmt[t]).T.astype(BF16)
        for r in range(2):
            zg_out[2 * t + r] = d_x[r * n:(r + 1) * n]
    send_small(0, sums0, head_weight_grad(0, d_own0), gate_sum0, b_out_row0)
    chip_sum_small(0)
    reduce_weights(0)
    forward_weights(1)
    forward_weights(0)

    for one in [ex_zo] + ex_small + near_wf:
        one.wait_recv()
    for one in [ex_b0, ex_b1, near_b1, ex_mid, ex_dz, ex_mask, ex_zo, ex_dm] + near_db + ex_db + near_small + ex_small + near_w + ex_w + ex_wf + near_wf:
        one.wait_send()


def finish(dims, zo_ref, zg_ref, w_ref, sm_ref,
           zo_out, zg_out, lns_out, lnb_out, wp_out, wb_out, bg_out, wo_out, bo_out, stage):
    rows, n, ch, heads, hd, group = dims
    zg_out[...] = zg_ref[...]
    stage[...] = zo_ref[...].astype(F32).reshape(group * rows * rows, ch)
    for i in range(rows):
        zo_out[i] = stage[pl.ds(i, n, stride=rows), :].astype(BF16)
    cut = 4 * hd // group
    for s in range(2):
        full = w_ref[s].astype(F32).reshape(group, 5 * hd // group, ch)
        wp_out[s] = full[:, :cut].reshape(4 * hd, ch).T
        wo_out[s] = full[:, cut:].reshape(hd, ch)
        total = jnp.sum(sm_ref[s], axis=0)
        for place, ref in enumerate((lns_out, lnb_out, bg_out, bo_out)):
            ref[s:s + 1, :] = total[place:place + 1, :]
        wb_out[s] = total[4:4 + heads]


def solution(mesh):
    axis = 'dap'
    group = mesh.shape[axis]
    row_spec = P(('dp', axis), None, None)
    mask_spec = P(('dp', axis), None)
    grad_spec = P('dp')

    def per_device(z, pair_mask, dz_out, ln_scale, ln_shift, w_proj, w_bias, b_gate, w_out, b_out):
        rows, n, ch = z.shape
        heads = w_bias.shape[-1]
        hd = b_gate.shape[-1]
        pairs, two, wide = rows // 2, 2 * n, heads * n
        piece = (group, rows * rows, ch)
        w_rows = 5 * hd // group

        def vmem(shape, dtype):
            return pltpu.VMEM(shape, dtype)

        w_heads = jnp.swapaxes(w_bias, 1, 2)
        like = [z, z, ln_scale, ln_shift, w_proj, w_heads, b_gate, w_out, b_out]
        out_shape = [jax.ShapeDtypeStruct(a.shape, BF16 if k < 2 else F32) for k, a in enumerate(like)]
        chips = group // 2
        mid_shape = [jax.ShapeDtypeStruct(piece, BF16), jax.ShapeDtypeStruct(z.shape, BF16),
                     jax.ShapeDtypeStruct((2, 2, chips, w_rows, ch), BF16), jax.ShapeDtypeStruct((2, chips, 8, ch), F32)]
        tile = (pairs, ch, two)
        scratch = [
            vmem((2, 4 * hd, ch), BF16), vmem((2, ch, hd), BF16), vmem((2, 16, ch), BF16), vmem((2, 4, ch, n), F32),
            vmem((2,) + tile, F32), vmem((2,) + tile, F32), vmem((2, pairs, 8, two), F32), vmem((2, pairs * two, ch), BF16), vmem(tile, BF16), vmem((ch, pairs * two), BF16),
            vmem((2, pairs, hd, two), BF16), vmem((2, pairs, hd, two), BF16), vmem((2, pairs, hd, two), BF16), vmem((2, pairs, two, 2 * hd), BF16),
            vmem((2, pairs, hd, two), F32), vmem((2, pairs, hd, two), F32), vmem((2, hd, pairs * two), BF16), vmem((rows * 16, n), F32),
            vmem((rows, hd, wide), BF16), vmem((rows, hd, wide), BF16), vmem((pairs, hd, two), BF16), vmem((pairs, hd, two), F32),
            vmem((4 * hd, pairs * two), BF16), vmem(tile, F32), vmem(tile, F32), vmem(tile, F32), vmem((pairs * two, ch), BF16), vmem((ch, pairs * two), BF16),
            vmem((2, rows, n, wide), F32), vmem((n, wide), F32), vmem((n, wide), F32),
            vmem((2, rows, n, n), F32), vmem((group * rows * rows, ch), F32),
            vmem((5 * hd, ch), F32), vmem((2, rows, ch, heads * rows), BF16), vmem((16, pairs * two), BF16),
            vmem((2, heads * rows, n), BF16), vmem((group, heads * rows, n), BF16), vmem((2, chips, heads * rows, n), BF16), vmem(piece, BF16), vmem(piece, BF16), vmem(piece, BF16), vmem(piece, BF16),
            vmem((rows, n), BF16), vmem((group, rows, n), BF16), vmem(piece, BF16), vmem(piece, BF16), vmem(piece, BF16),
            vmem((2, 2, chips, heads * rows, n), BF16), vmem((2, chips, heads * rows, n), BF16), vmem((2, chips, heads * rows, n), BF16), vmem((2, chips, heads * rows, n), BF16),
            vmem((2, 2, chips, w_rows, ch), BF16), vmem((2, chips, w_rows, ch), BF16), vmem((2, chips, w_rows, ch), BF16), vmem((2, chips, w_rows, ch), BF16),
            vmem((2, w_rows, ch), BF16), vmem((2, 8, ch), F32), vmem((2, 8, ch), F32), vmem((2, 8, ch), F32),
            pltpu.SemaphoreType.DMA((24,)), pltpu.SemaphoreType.DMA((24,)),
        ]
        operands = (z, pair_mask, dz_out, ln_scale, ln_shift, w_proj, w_heads, b_gate, w_out, b_out)
        scratch += [vmem(a.shape, a.dtype) for a in operands] + [pltpu.SemaphoreType.DMA((10,))]
        in_vmem = pl.BlockSpec(memory_space=pltpu.VMEM)
        mid = pl.pallas_call(
            functools.partial(kernel, (rows, n, ch, heads, hd, group, axis)),
            out_shape=mid_shape,
            in_specs=[pl.BlockSpec(memory_space=pltpu.HBM)] * 10,
            out_specs=[in_vmem] * 4,
            scratch_shapes=scratch,
            compiler_params=pltpu.CompilerParams(collective_id=0, has_side_effects=True, vmem_limit_bytes=40 * 1024 * 1024),
        )(*[pltpu.with_memory_space_constraint(a, pltpu.HBM) for a in operands])
        out = pl.pallas_call(
            functools.partial(finish, (rows, n, ch, heads, hd, group)),
            out_shape=out_shape,
            in_specs=[in_vmem] * 4,
            out_specs=[in_vmem] * 9,
            scratch_shapes=[vmem((group * rows * rows, ch), F32)],
            compiler_params=pltpu.CompilerParams(vmem_limit_bytes=16 * 1024 * 1024),
        )(*mid)
        return tuple(out[:5]) + (jnp.swapaxes(out[5], 1, 2),) + tuple(out[6:])

    return jax.shard_map(per_device, mesh=mesh, in_specs=(row_spec, mask_spec, row_spec) + (P(),) * 7,
                         out_specs=(row_spec, row_spec) + (grad_spec,) * 7, check_vma=False)
```
